256 devices in a mesh: seq: 256 (over y, z, x, core).
Axes of the slice: x: 4, y: 4, z: 8, core: 2. Of those that a mesh axis runs over, the one named last changes fastest.
Arguments:
- queries: bfloat16 [16, 8192], P(None, 'seq'), may hold values from -1000 to 1000
- span_keys: bfloat16 [16, 1024], P(None, 'seq'), may hold values from -6 to 6
- span_values: bfloat16 [16, 1024], P(None, 'seq'), may hold values from -6 to 6
- positions: int32 [3, 16], replicated, may hold values from 0 to 8191, as said below
- span_segments: int32 [16], replicated, may hold values from 0 to 3, as said below
- cache_keys: bfloat16 [131072, 1024], P('seq'), may hold values from -6 to 6
- cache_values: bfloat16 [131072, 1024], P('seq'), may hold values from -6 to 6
- cache_segments: int32 [131072], P('seq'), may hold values from 0 to 3
Outputs:
- attended: bfloat16 [16, 8192], replicated
The draws below stay inside these ranges and needn't reach their ends.
Inputs may be any that keep to these rules, and one draw needn't show every extreme that they name: `positions`: row 0 holds time ids; rows 1 and 2 hold height and width ids, which are below 64. `span_segments`: never falling; every request 0 to 3 has one run of rows, and every run starts at an even row.
All inputs are finite; a program needn't handle non-finite values.
Results may differ from the reference program's by a relative error of at most 0.0054.
Values may be sent and summed in bfloat16 or wider, within the bound.
No kernel may reach another device: no remote copies, remote signals or barrier semaphores. Data moves between devices by JAX's collectives and lax.ppermute only.
A program may use at most 64 MiB of HBM per device.

```python
import jax
import jax.numpy as jnp
from jax import lax

H = 64
KVH = 8
HD = 128
REQS = 4
QROWS = 16
KV_DEV = 512
TOKENS = 131072
N_SEQ = 256


def position_table(key):
    base = jax.random.fold_in(key, 23)
    first, second = jax.random.split(base)
    times = jax.random.randint(first, (1, QROWS), 0, 8192)
    places = jax.random.randint(second, (2, QROWS), 0, 64)
    return jnp.concatenate([times, places], axis=0).astype(jnp.int32)


def span_segment_table(key):
    base = jax.random.fold_in(key, 37)
    order = jax.random.permutation(base, QROWS // 2 - 1) + 1
    starts = 2 * order[:REQS - 1]
    rows = jnp.arange(QROWS, dtype=jnp.int32)
    return jnp.sum((rows[:, None] >= starts[None, :]).astype(jnp.int32), axis=1).astype(jnp.int32)


def cache_segment_table(key):
    base = jax.random.fold_in(key, 53)
    return jax.random.randint(base, (TOKENS,), 0, REQS).astype(jnp.int32)


def span_pair(key):
    base = jax.random.fold_in(key, 11)
    parts = jax.random.split(base, 3)
    group = H // KVH
    keys = jnp.clip(jax.random.normal(parts[0], (QROWS, KVH, HD), jnp.float32), -6.0, 6.0)
    noise = jnp.clip(jax.random.normal(parts[1], (QROWS, KVH, group, HD), jnp.float32), -6.0, 6.0)
    pull = jax.random.uniform(parts[2], (QROWS, KVH, group, 1), jnp.float32, 0.9, 1.6)
    queries = 3.0 * noise + pull * keys[:, :, None, :]
    queries = jnp.clip(queries, -1000.0, 1000.0)
    keys = jnp.clip(keys, -6.0, 6.0)
    return (queries.reshape(QROWS, H * HD), keys.reshape(QROWS, KVH * HD))


def draw_queries(key, part):
    return span_pair(key)[0].astype(jnp.bfloat16)


def draw_span_keys(key, part):
    return span_pair(key)[1].astype(jnp.bfloat16)


def draw_positions(key, part):
    return position_table(key)


def draw_span_segments(key, part):
    return span_segment_table(key)


def draw_cache_segments(key, part):
    return cache_segment_table(key)


def draw_cache_keys(key, part):
    base = jax.random.fold_in(key, 71)
    parts = jax.random.split(base, 1)
    cache = jnp.clip(jax.random.normal(parts[0], (TOKENS, KVH, HD), jnp.float32), -6.0, 6.0)
    return jnp.clip(cache, -6.0, 6.0).reshape(TOKENS, KVH * HD).astype(jnp.bfloat16)


def level_of(own_key, extent, cuts, least, largest):
    gain, own = 1.0, jax.random.fold_in(own_key, 6)
    for dim, blocks in cuts:
        steps = jnp.exp(jax.random.uniform(jax.random.fold_in(own, dim), (blocks,), jnp.float32, least / len(cuts), largest / len(cuts)))
        gain = gain * jnp.repeat(steps, extent[dim] // blocks).reshape([-1 if axis == dim else 1 for axis in range(len(extent))])
    return gain


def centred(key, shape, spread, reach, cuts=(), held_as=jnp.bfloat16):
    entries = spread * jax.random.normal(key, shape, jnp.float32)
    if cuts:
        entries = entries * level_of(key, shape, cuts, -0.22, 0.18)
    return jnp.clip(entries, -reach, reach).astype(held_as)


def setup_inputs(seed: int = 0) -> dict:
    streams_of = jax.random.split(jax.random.key(seed), 9)
    return {
        "queries": draw_queries(jax.random.fold_in(streams_of[8], 71), 0),
        "span_keys": draw_span_keys(jax.random.fold_in(streams_of[8], 71), 0),
        "span_values": centred(streams_of[2], (QROWS, KVH * HD), 1.0, 6.0, ((1, 256),)),
        "positions": draw_positions(jax.random.fold_in(streams_of[8], 71), 0),
        "span_segments": draw_span_segments(jax.random.fold_in(streams_of[8], 71), 0),
        "cache_keys": draw_cache_keys(jax.random.fold_in(streams_of[8], 71), 0),
        "cache_values": centred(streams_of[6], (TOKENS, KVH * HD), 1.0, 6.0, ((0, 256),)),
        "cache_segments": draw_cache_segments(jax.random.fold_in(streams_of[8], 71), 0),
    }


def rope_tables(positions, head_dim):
    half = head_dim // 2
    index = jnp.arange(half, dtype=jnp.int32)
    inverse = jnp.power(jnp.float32(1000000.0), -2.0 * index.astype(jnp.float32) / head_dim)
    section = jnp.where(index < head_dim // 8, 0, jnp.where(index < 5 * head_dim // 16, 1, 2))
    chosen = jnp.where(section[None, :] == 0, positions[0][:, None],
                       jnp.where(section[None, :] == 1, positions[1][:, None], positions[2][:, None]))
    angle = chosen.astype(jnp.float32) * inverse[None, :]
    return jnp.cos(angle), jnp.sin(angle)


def rotate(values, cosines, sines):
    half = values.shape[-1] // 2
    first = values[..., :half]
    second = values[..., half:]
    cosine = cosines[:, None, :]
    sine = sines[:, None, :]
    return jnp.concatenate([first * cosine - second * sine, second * cosine + first * sine], axis=-1)


def head_state(q_rot, keys, values, visible):
    rows, kv_heads, group, head_dim = q_rot.shape
    scale = 1.0 / (head_dim ** 0.5)
    outs, peaks, totals = [], [], []
    for head in range(kv_heads):
        block = q_rot[:, head].reshape(rows * group, head_dim)
        key_cols = keys[:, head * head_dim:(head + 1) * head_dim]
        value_cols = values[:, head * head_dim:(head + 1) * head_dim]
        scores = lax.dot_general(block, key_cols, (((1,), (1,)), ((), ())),
                                 preferred_element_type=jnp.float32) * scale
        scores = scores.reshape(rows, group, -1)
        mask = visible[:, None, :]
        peak = jnp.max(jnp.where(mask, scores, jnp.float32(-1e30)), axis=-1)
        weights = jnp.where(mask, jnp.exp(scores - peak[..., None]), jnp.float32(0.0))
        total = jnp.sum(weights, axis=-1)
        out = jnp.dot(weights.astype(jnp.bfloat16).reshape(rows * group, -1), value_cols,
                      preferred_element_type=jnp.float32)
        outs.append(out.reshape(rows, group, head_dim))
        peaks.append(peak)
        totals.append(total)
    out_all = jnp.stack(outs, axis=1).reshape(rows * kv_heads * group, head_dim)
    peak_all = jnp.stack(peaks, axis=1).reshape(rows * kv_heads * group)
    total_all = jnp.stack(totals, axis=1).reshape(rows * kv_heads * group)
    return out_all, peak_all, total_all


def combine(left, right):
    out_a, peak_a, total_a = left
    out_b, peak_b, total_b = right
    peak = jnp.maximum(peak_a, peak_b)
    factor_a = jnp.exp(peak_a - peak)
    factor_b = jnp.exp(peak_b - peak)
    return (out_a * factor_a[:, None] + out_b * factor_b[:, None], peak,
            total_a * factor_a + total_b * factor_b)


def reference(queries, span_keys, span_values, positions, span_segments, cache_keys, cache_values, cache_segments):
    group = H // KVH
    cosines, sines = rope_tables(positions, HD)
    q_rot = rotate(queries.astype(jnp.float32).reshape(QROWS, H, HD), cosines, sines).astype(jnp.bfloat16)
    q_rot = q_rot.reshape(QROWS, KVH, group, HD)
    k_rot = rotate(span_keys.astype(jnp.float32).reshape(QROWS, KVH, HD), cosines, sines)
    k_rot = k_rot.astype(jnp.bfloat16).reshape(QROWS, KVH * HD)
    index = jnp.arange(QROWS, dtype=jnp.int32)
    own_visible = (span_segments[:, None] == span_segments[None, :]) & (index[None, :] <= index[:, None])
    span_state = head_state(q_rot, k_rot, span_values, own_visible)

    key_blocks = cache_keys.reshape(N_SEQ, KV_DEV, KVH * HD)
    value_blocks = cache_values.reshape(N_SEQ, KV_DEV, KVH * HD)
    segment_blocks = cache_segments.reshape(N_SEQ, KV_DEV)

    def step(carry, block):
        keys, values, segments = block
        visible = span_segments[:, None] == segments[None, :]
        return combine(carry, head_state(q_rot, keys, values, visible)), None

    start = (jnp.zeros((QROWS * H, HD), jnp.float32), jnp.full((QROWS * H,), -1e30, jnp.float32),
             jnp.zeros((QROWS * H,), jnp.float32))
    cache_state, _ = lax.scan(step, start, (key_blocks, value_blocks, segment_blocks))
    merged_out, _, merged_total = combine(cache_state, span_state)
    return (merged_out / merged_total[:, None]).astype(jnp.bfloat16).reshape(QROWS, H * HD)
```

```python
import functools

import jax
import jax.numpy as jnp
from jax import lax
from jax.experimental import pallas as pl
from jax.experimental.pallas import tpu as pltpu
from jax.sharding import Mesh
from jax.sharding import PartitionSpec as P

H = 64
KVH = 8
HD = 128
ROWS = 16
ALL = ("y", "z", "x", "c")
NEAR = ("y", "x", "c")
LOG2E = 1.4426950408889634
NONE = -1e30
HIDDEN = -2e30
F32 = jnp.float32
BF16 = jnp.bfloat16
VMEM = pl.BlockSpec(memory_space=pltpu.VMEM)
SMEM = pl.BlockSpec(memory_space=pltpu.SMEM)
NT = (((1,), (1,)), ((), ()))


def call(body, name, out_shape, *args, specs=None, scratch=()):
    return pl.pallas_call(
        body,
        name=name,
        out_shape=out_shape,
        in_specs=specs or [VMEM] * len(args),
        out_specs=jax.tree.map(lambda _: VMEM, out_shape),
        scratch_shapes=scratch,
    )(*args)


def lanes(shape):
    return lax.broadcasted_iota(jnp.int32, shape, len(shape) - 1)


def move(value, by):
    by %= value.shape[-1]
    return pltpu.roll(value, by, value.ndim - 1) if by else value


def exchange(tiles, axes):
    return lax.all_to_all(tiles, axes, 0, 0, tiled=True)


def rope_tables(positions):
    half = HD // 2
    index = jnp.arange(half, dtype=jnp.int32)
    inverse = jnp.power(jnp.float32(1000000.0), -2.0 * index.astype(jnp.float32) / HD)
    section = jnp.where(index < HD // 8, 0, jnp.where(index < 5 * HD // 16, 1, 2))
    chosen = jnp.where(
        section[None, :] == 0,
        positions[0][:, None],
        jnp.where(section[None, :] == 1, positions[1][:, None], positions[2][:, None]),
    )
    angle = chosen.astype(jnp.float32) * inverse[None, :]
    cosine, sine = (jnp.cos(angle), jnp.sin(angle))
    return jnp.stack(
        [jnp.concatenate([cosine, cosine], 1), jnp.concatenate([sine, sine], 1)], axis=0
    )


def pack_body(q_ref, k_ref, v_ref, out_ref):
    fill = jnp.zeros((ROWS, 128 - 40), F32)
    tile = jnp.concatenate(
        [q_ref[...].astype(F32), k_ref[...].astype(F32), v_ref[...].astype(F32), fill], axis=1
    ).astype(BF16)
    for d in range(out_ref.shape[0]):
        out_ref[d] = tile


def regroup_body(in_ref, out_ref):
    lane = lanes((ROWS, 128))
    tiles = [in_ref[s].astype(F32) for s in range(16)]
    rows = []
    for m in range(4):
        dense = tiles[4 * m]
        for i in range(1, 4):
            dense = jnp.where(lane < 32 * i, dense, move(tiles[4 * m + i], 32 * i))
        rows.append(dense.astype(BF16))
    kv = jnp.zeros((ROWS, 128), F32)
    for s in range(16):
        z, c = divmod(s, 2)
        at = (z % 4) * 32 + (z // 4) * 8 + c * 4
        kv = jnp.where((lane >= at) & (lane < at + 4), move(tiles[s], at - 32), kv)
        kv = jnp.where((lane >= at + 16) & (lane < at + 20), move(tiles[s], at + 16 - 36), kv)
    rows.append(kv.astype(BF16))
    for d in range(out_ref.shape[0]):
        for n, r in enumerate(rows):
            out_ref[d, n * ROWS : (n + 1) * ROWS, :] = r


def turn_body(v_ref, out_ref):
    for g in range(KVH):
        out_ref[g] = v_ref[:, g * HD : (g + 1) * HD].T


def split_pair(value):
    high = value.astype(BF16).astype(F32)
    return high, (value - high).astype(BF16).astype(F32)


def state_rows(peak, total):
    row = lax.broadcasted_iota(jnp.int32, (8, 128), 0)
    parts = (*split_pair(peak), *split_pair(total))
    tile = jnp.zeros((8, 128), F32)
    for n, part in enumerate(parts):
        tile = jnp.where(row == n, part, tile)
    return tile.astype(BF16)


def attend_body(own_ref, in_ref, rope_ref, bias_ref, span_bias_ref, k_ref, vt_ref, out_ref, q_ref):
    lane = lanes((ROWS, 128))
    cosine, sine = rope_ref[0], rope_ref[1]
    signed = jnp.where(lane < 64, -sine, sine)
    for y in range(4):
        for m in range(4):
            for p in range(2):
                a = in_ref[y * 4 + 2 * p, m * ROWS : (m + 1) * ROWS, :].astype(F32)
                b = in_ref[y * 4 + 2 * p + 1, m * ROWS : (m + 1) * ROWS, :].astype(F32)
                a, b = a * cosine - b * sine, b * cosine + a * sine
                for n in range(2):
                    head = y * 16 + 4 * m + 2 * n + p
                    if n == 0:
                        whole = jnp.where(lane < 64, a, move(b, 64))
                    else:
                        whole = jnp.where(lane < 64, move(a, 64), b)
                    q_ref[head * ROWS : (head + 1) * ROWS, :] = whole.astype(BF16)
    factor = LOG2E / HD**0.5
    for g in range(KVH):
        y, upper = divmod(g, 2)
        found = []
        for kind in (upper, 2 + upper):
            value = jnp.zeros((ROWS, 128), F32)
            for x in range(4):
                tile = in_ref[y * 4 + x, 4 * ROWS : 5 * ROWS, :].astype(F32)
                value = jnp.where((lane // 8) % 4 == x, move(tile, 8 * (x - kind)), value)
            found.append(value)
        span_k = (found[0] * cosine + move(found[0], 64) * signed).astype(BF16)
        span_v = found[1].astype(BF16)
        q = q_ref[g * 128 : (g + 1) * 128, :]
        k = k_ref[:, g * HD : (g + 1) * HD]
        absent = jnp.where(own_ref[0] == g, 0.0, HIDDEN)
        s = lax.dot_general(k, q, NT, preferred_element_type=F32) * factor + bias_ref[...]
        t = lax.dot_general(span_k, q, NT, preferred_element_type=F32) * factor
        t = t + (span_bias_ref[...] + absent)
        peak = jnp.maximum(
            jnp.maximum(jnp.max(s, axis=0, keepdims=True), jnp.max(t, axis=0, keepdims=True)),
            NONE,
        )
        high, low = split_pair(peak)
        peak = high + low
        s = jnp.exp2(s - peak)
        t = jnp.exp2(t - peak)
        total = jnp.sum(s, axis=0, keepdims=True) + jnp.sum(t, axis=0, keepdims=True)
        out = jnp.dot(vt_ref[g], s.astype(BF16), preferred_element_type=F32)
        out = out + lax.dot_general(
            span_v, t.astype(BF16), (((0,), (0,)), ((), ())), preferred_element_type=F32
        )
        out = out.astype(BF16)
        state = state_rows(peak, total)
        for n in range(4):
            out_ref[g * 4 + n, 0:32, :] = out[n * 32 : (n + 1) * 32]
            out_ref[g * 4 + n, 32:40, :] = state


def merged(in_ref):
    count = in_ref.shape[0]
    peaks, totals = [], []
    for n in range(count):
        state = in_ref[n, 32:40, :].astype(F32)
        peaks.append(state[0:1] + state[1:2])
        totals.append(state[2:3] + state[3:4])
    peak = functools.reduce(jnp.maximum, peaks)
    out = jnp.zeros((32, 128), F32)
    total = jnp.zeros((1, 128), F32)
    for n in range(count):
        factor = jnp.exp2(peaks[n] - peak)
        out = out + in_ref[n, 0:32, :].astype(F32) * factor
        total = total + totals[n] * factor
    return out, peak, total


def merge_body(in_ref, out_ref):
    out, peak, total = merged(in_ref)
    out = out.astype(BF16)
    state = state_rows(peak, total)
    for d in range(out_ref.shape[0]):
        out_ref[d, 0:32, :] = out
        out_ref[d, 32:40, :] = state


def finish_body(in_ref, out_ref):
    out, _, total = merged(in_ref)
    out = (out / total).astype(BF16)
    for d in range(out_ref.shape[0]):
        out_ref[d] = out


def place_body(in_ref, out_ref):
    eye = jnp.where(
        lax.broadcasted_iota(jnp.int32, (128, 128), 0) == lanes((128, 128)), 1.0, 0.0
    ).astype(BF16)
    for g in range(KVH):
        block = in_ref[g * 4 : (g + 1) * 4].reshape(128, 128)
        block = lax.dot_general(eye, block, NT, preferred_element_type=F32).astype(BF16)
        for i in range(8):
            at = (g * 8 + i) * HD
            out_ref[:, at : at + HD] = block[i * ROWS : (i + 1) * ROWS]


def per_device(
    queries,
    span_keys,
    span_values,
    positions,
    span_segments,
    cache_keys,
    cache_values,
    cache_segments,
):
    shape = jax.ShapeDtypeStruct
    tiles = call(pack_body, "pack", shape((16, ROWS, 128), BF16), queries, span_keys, span_values)
    tiles = exchange(tiles, ("z", "c"))
    tiles = call(regroup_body, "regroup", shape((16, 5 * ROWS, 128), BF16), tiles)
    tiles = exchange(tiles, ("y", "x"))

    rope = rope_tables(positions)
    turned = call(turn_body, "turn", shape((KVH, HD, 512), BF16), cache_values)
    columns = jnp.tile(span_segments, 8)[None, :]
    bias = jnp.where(cache_segments[:, None] == columns, 0.0, HIDDEN).astype(F32)
    index = jnp.arange(ROWS, dtype=jnp.int32)
    seen = (span_segments[:, None] == span_segments[None, :]) & (index[:, None] <= index[None, :])
    span_bias = jnp.tile(jnp.where(seen, 0.0, HIDDEN).astype(F32), (1, 8))
    own = lax.axis_index(ALL).astype(jnp.int32).reshape(1)

    parts = call(
        attend_body,
        "attend",
        shape((32, 40, 128), BF16),
        own,
        tiles,
        rope,
        bias,
        span_bias,
        cache_keys,
        turned,
        specs=[SMEM] + [VMEM] * 6,
        scratch=[pltpu.VMEM((H * ROWS, HD), BF16)],
    )
    parts = exchange(parts, NEAR)
    parts = call(merge_body, "merge", shape((8, 40, 128), BF16), parts)
    parts = exchange(parts, ("z",))
    whole = call(finish_body, "finish", shape((32, 32, 128), BF16), parts)
    whole = exchange(whole, NEAR)
    return call(place_body, "place", shape((ROWS, H * HD), BF16), whole)


def solution(mesh):
    split = Mesh(mesh.devices.reshape(4, 8, 4, 2), ALL)
    return jax.shard_map(
        per_device,
        mesh=split,
        in_specs=(
            P(None, ALL),
            P(None, ALL),
            P(None, ALL),
            P(),
            P(),
            P(ALL, None),
            P(ALL, None),
            P(ALL),
        ),
        out_specs=P(),
        check_vma=False,
    )
```

```python
import functools

import jax
import jax.numpy as jnp
from jax import lax
from jax.experimental import pallas as pl
from jax.experimental.pallas import tpu as pltpu
from jax.sharding import Mesh
from jax.sharding import PartitionSpec as P

H = 64
KVH = 8
HD = 128
ROWS = 16
ALL = ("y", "z", "x", "c")
NEAR = ("y", "x", "c")
LOG2E = 1.4426950408889634
NONE = -1e30
HIDDEN = -2e30
F32 = jnp.float32
BF16 = jnp.bfloat16
VMEM = pl.BlockSpec(memory_space=pltpu.VMEM)
SMEM = pl.BlockSpec(memory_space=pltpu.SMEM)
NT = (((1,), (1,)), ((), ()))


def call(body, name, out_shape, *args, specs=None, scratch=(), limit=8 << 20):
    return pl.pallas_call(
        body,
        name=name,
        out_shape=out_shape,
        in_specs=specs or [VMEM] * len(args),
        out_specs=jax.tree.map(lambda _: VMEM, out_shape),
        scratch_shapes=scratch,
        compiler_params=pltpu.CompilerParams(vmem_limit_bytes=limit),
    )(*args)


def lanes(shape):
    return lax.broadcasted_iota(jnp.int32, shape, len(shape) - 1)


def move(value, by):
    by %= value.shape[-1]
    return pltpu.roll(value, by, value.ndim - 1) if by else value


def exchange(tiles, axes):
    return lax.all_to_all(tiles, axes, 0, 0, tiled=True)


def rope_tables(positions):
    half = HD // 2
    index = jnp.arange(half, dtype=jnp.int32)
    inverse = jnp.power(jnp.float32(1000000.0), -2.0 * index.astype(jnp.float32) / HD)
    section = jnp.where(index < HD // 8, 0, jnp.where(index < 5 * HD // 16, 1, 2))
    chosen = jnp.where(
        section[None, :] == 0,
        positions[0][:, None],
        jnp.where(section[None, :] == 1, positions[1][:, None], positions[2][:, None]),
    )
    angle = chosen.astype(jnp.float32) * inverse[None, :]
    cosine, sine = (jnp.cos(angle), jnp.sin(angle))
    return jnp.stack(
        [jnp.concatenate([cosine, cosine], 1), jnp.concatenate([sine, sine], 1)], axis=0
    )


def pack_body(q_ref, k_ref, v_ref, out_ref):
    def spread(count, at):
        shape = (count, 128)
        hit = lanes(shape) == lax.broadcasted_iota(jnp.int32, shape, 0) + at
        return jnp.where(hit, 1.0, 0.0).astype(BF16)

    tile = jnp.dot(q_ref[...], spread(32, 0), preferred_element_type=F32)
    for ref, at in ((k_ref, 32), (v_ref, 36)):
        tile = tile + lax.dot_general(
            ref[...], spread(4, at), (((0,), (0,)), ((), ())), preferred_element_type=F32
        )
    tile = tile.astype(BF16)
    for d in range(out_ref.shape[0]):
        out_ref[d] = tile


def regroup_body(in_ref, out_ref):
    lane = lanes((ROWS, 128))
    tiles = [in_ref[s].astype(F32) for s in range(16)]
    rows = []
    for m in range(4):
        dense = tiles[4 * m]
        for i in range(1, 4):
            dense = jnp.where(lane < 32 * i, dense, move(tiles[4 * m + i], 32 * i))
        rows.append(dense.astype(BF16))
    kv = jnp.zeros((ROWS, 128), F32)
    for s in range(16):
        z, c = divmod(s, 2)
        at = (z % 4) * 32 + (z // 4) * 8 + c * 4
        kv = jnp.where((lane >= at) & (lane < at + 4), move(tiles[s], at - 32), kv)
        kv = jnp.where((lane >= at + 16) & (lane < at + 20), move(tiles[s], at + 16 - 36), kv)
    rows.append(kv.astype(BF16))
    for d in range(out_ref.shape[0]):
        for n, r in enumerate(rows):
            out_ref[d, n * ROWS : (n + 1) * ROWS, :] = r


def turn_body(v_ref, out_ref):
    for g in range(KVH):
        out_ref[g] = v_ref[:, g * HD : (g + 1) * HD].T


def split_pair(value):
    high = value.astype(BF16).astype(F32)
    return high, (value - high).astype(BF16).astype(F32)


def state_rows(peak, total):
    row = lax.broadcasted_iota(jnp.int32, (8, 128), 0)
    parts = (*split_pair(peak), *split_pair(total))
    tile = jnp.zeros((8, 128), F32)
    for n, part in enumerate(parts):
        tile = jnp.where(row == n, part, tile)
    return tile.astype(BF16)


def attend_body(own_ref, in_ref, rope_ref, bias_ref, span_bias_ref, k_ref, vt_ref, out_ref, q_ref):
    lane = lanes((ROWS, 128))
    cosine, sine = rope_ref[0], rope_ref[1]
    signed = jnp.where(lane < 64, -sine, sine)
    for y in range(4):
        for m in range(4):
            for p in range(2):
                a = in_ref[y * 4 + 2 * p, m * ROWS : (m + 1) * ROWS, :].astype(F32)
                b = in_ref[y * 4 + 2 * p + 1, m * ROWS : (m + 1) * ROWS, :].astype(F32)
                a, b = a * cosine - b * sine, b * cosine + a * sine
                for n in range(2):
                    head = y * 16 + 4 * m + 2 * n + p
                    if n == 0:
                        whole = jnp.where(lane < 64, a, move(b, 64))
                    else:
                        whole = jnp.where(lane < 64, move(a, 64), b)
                    q_ref[head * ROWS : (head + 1) * ROWS, :] = whole.astype(BF16)
    factor = LOG2E / HD**0.5
    for g in range(KVH):
        y, upper = divmod(g, 2)
        found = []
        for kind in (upper, 2 + upper):
            value = jnp.zeros((ROWS, 128), F32)
            for x in range(4):
                tile = in_ref[y * 4 + x, 4 * ROWS : 5 * ROWS, :].astype(F32)
                value = jnp.where((lane // 8) % 4 == x, move(tile, 8 * (x - kind)), value)
            found.append(value)
        span_k = (found[0] * cosine + move(found[0], 64) * signed).astype(BF16)
        span_v = found[1].astype(BF16)
        q = q_ref[g * 128 : (g + 1) * 128, :]
        k = k_ref[:, g * HD : (g + 1) * HD]
        absent = jnp.where(own_ref[0] == g, 0.0, HIDDEN)
        s = lax.dot_general(k, q, NT, preferred_element_type=F32) * factor + bias_ref[...]
        t = lax.dot_general(span_k, q, NT, preferred_element_type=F32) * factor
        t = t + (span_bias_ref[...] + absent)
        peak = jnp.maximum(
            jnp.maximum(jnp.max(s, axis=0, keepdims=True), jnp.max(t, axis=0, keepdims=True)),
            NONE,
        )
        high, low = split_pair(peak)
        peak = high + low
        s = jnp.exp2(s - peak)
        t = jnp.exp2(t - peak)
        total = jnp.sum(s, axis=0, keepdims=True) + jnp.sum(t, axis=0, keepdims=True)
        out = jnp.dot(vt_ref[g], s.astype(BF16), preferred_element_type=F32)
        out = out + lax.dot_general(
            span_v, t.astype(BF16), (((0,), (0,)), ((), ())), preferred_element_type=F32
        )
        out = out.astype(BF16)
        state = state_rows(peak, total)
        for n in range(4):
            out_ref[g * 4 + n, 0:32, :] = out[n * 32 : (n + 1) * 32]
            out_ref[g * 4 + n, 32:40, :] = state


def merged(in_ref):
    count = in_ref.shape[0]
    peaks, totals = [], []
    for n in range(count):
        state = in_ref[n, 32:40, :].astype(F32)
        peaks.append(state[0:1] + state[1:2])
        totals.append(state[2:3] + state[3:4])
    peak = functools.reduce(jnp.maximum, peaks)
    out = jnp.zeros((32, 128), F32)
    total = jnp.zeros((1, 128), F32)
    for n in range(count):
        factor = jnp.exp2(peaks[n] - peak)
        out = out + in_ref[n, 0:32, :].astype(F32) * factor
        total = total + totals[n] * factor
    return out, peak, total


def merge_body(in_ref, out_ref):
    out, peak, total = merged(in_ref)
    out = out.astype(BF16)
    state = state_rows(peak, total)
    for d in range(out_ref.shape[0]):
        out_ref[d, 0:32, :] = out
        out_ref[d, 32:40, :] = state


def finish_body(in_ref, out_ref):
    out, _, total = merged(in_ref)
    out = (out / total).astype(BF16)
    for d in range(out_ref.shape[0]):
        out_ref[d] = out


def place_body(in_ref, out_ref):
    eye = jnp.where(
        lax.broadcasted_iota(jnp.int32, (128, 128), 0) == lanes((128, 128)), 1.0, 0.0
    ).astype(BF16)
    for g in range(KVH):
        block = in_ref[g * 4 : (g + 1) * 4].reshape(128, 128)
        block = lax.dot_general(eye, block, NT, preferred_element_type=F32).astype(BF16)
        for i in range(8):
            at = (g * 8 + i) * HD
            out_ref[:, at : at + HD] = block[i * ROWS : (i + 1) * ROWS]


def per_device(
    queries,
    span_keys,
    span_values,
    positions,
    span_segments,
    cache_keys,
    cache_values,
    cache_segments,
):
    shape = jax.ShapeDtypeStruct
    tiles = call(pack_body, "pack", shape((16, ROWS, 128), BF16), queries, span_keys.T, span_values.T)
    tiles = exchange(tiles, ("z", "c"))
    tiles = call(regroup_body, "regroup", shape((16, 5 * ROWS, 128), BF16), tiles)
    tiles, cache_values, cache_segments, span_segments = lax.optimization_barrier(
        (tiles, cache_values, cache_segments, span_segments)
    )
    tiles = exchange(tiles, ("y", "x"))

    rope = rope_tables(positions)
    turned = call(turn_body, "turn", shape((KVH, HD, 512), BF16), cache_values)
    columns = jnp.tile(span_segments, 8)[None, :]
    bias = jnp.where(cache_segments[:, None] == columns, 0.0, HIDDEN).astype(F32)
    index = jnp.arange(ROWS, dtype=jnp.int32)
    seen = (span_segments[:, None] == span_segments[None, :]) & (index[:, None] <= index[None, :])
    span_bias = jnp.tile(jnp.where(seen, 0.0, HIDDEN).astype(F32), (1, 8))
    own = lax.axis_index(ALL).astype(jnp.int32).reshape(1)

    parts = call(
        attend_body,
        "attend",
        shape((32, 40, 128), BF16),
        own,
        tiles,
        rope,
        bias,
        span_bias,
        cache_keys,
        turned,
        specs=[SMEM] + [VMEM] * 6,
        scratch=[pltpu.VMEM((H * ROWS, HD), BF16)],
    )
    parts = exchange(parts, NEAR)
    parts = call(merge_body, "merge", shape((8, 40, 128), BF16), parts)
    parts = exchange(parts, ("z",))
    whole = call(finish_body, "finish", shape((32, 32, 128), BF16), parts)
    whole = exchange(whole, NEAR)
    return call(place_body, "place", shape((ROWS, H * HD), BF16), whole)


def solution(mesh):
    split = Mesh(mesh.devices.reshape(4, 8, 4, 2), ALL)
    return jax.shard_map(
        per_device,
        mesh=split,
        in_specs=(
            P(None, ALL),
            P(None, ALL),
            P(None, ALL),
            P(),
            P(),
            P(ALL, None),
            P(ALL, None),
            P(ALL),
        ),
        out_specs=P(),
        check_vma=False,
    )
```

```python
import functools

import jax
import jax.numpy as jnp
from jax import lax
from jax.experimental import pallas as pl
from jax.experimental.pallas import tpu as pltpu
from jax.sharding import Mesh
from jax.sharding import PartitionSpec as P

H = 64
HD = 128
ROWS = 16
ALL = ("y", "z", "x", "c")
CHIPS = ("y", "z", "x")
PLANE = ("y", "x")
LOG2E = 1.4426950408889634
NONE = -1e30
HIDDEN = -2e30
F32 = jnp.float32
BF16 = jnp.bfloat16
VMEM = pl.BlockSpec(memory_space=pltpu.VMEM)
HBM = pl.BlockSpec(memory_space=pltpu.HBM)
NT = (((1,), (1,)), ((), ()))


def call(body, out_shape, *args, specs=None, scratch=(), limit=8 << 20):
    return pl.pallas_call(
        body,
        out_shape=out_shape,
        in_specs=specs or [VMEM] * len(args),
        out_specs=jax.tree.map(lambda _: VMEM, out_shape),
        scratch_shapes=scratch,
        compiler_params=pltpu.CompilerParams(vmem_limit_bytes=limit),
    )(*args)


def lanes(shape):
    return lax.broadcasted_iota(jnp.int32, shape, len(shape) - 1)


def move(value, by):
    by %= value.shape[-1]
    return pltpu.roll(value, by, value.ndim - 1) if by else value


def exchange(tiles, axes):
    return lax.all_to_all(tiles, axes, 0, 0, tiled=True)


def swap(value):
    return lax.ppermute(value, "c", ((0, 1), (1, 0)))


def rows_of(shape):
    return lax.broadcasted_iota(jnp.int32, shape, 0)


TN = (((0,), (0,)), ((), ()))


def dot(a, b, dims):
    return lax.dot_general(a, b, dims, preferred_element_type=F32)


def where_one(hit):
    return jnp.where(hit, 1.0, 0.0).astype(BF16)


def fetch(sources, targets, sems):
    return [pltpu.make_async_copy(a, b, sems.at[n]) for n, (a, b) in enumerate(zip(sources, targets))]


def pack_body(*refs):
    sources, (keep_ref, send_ref, pos_ref, seg_ref) = refs[:6], refs[6:10]
    q_ref, k_ref, v_ref, s_ref, sems = refs[10:]
    copies = fetch(sources, (q_ref, k_ref, v_ref, s_ref, pos_ref, seg_ref), sems)
    for copy in copies:
        copy.start()
    for copy in copies:
        copy.wait()
    c = lax.axis_index("c")

    def spread(count, at):
        return where_one(lanes((count, 128)) == rows_of((count, 128)) + at)

    q = jnp.dot(q_ref[...], spread(32, c * 32), preferred_element_type=F32)
    kv = jnp.zeros((8, 128), F32)
    for ref, at in ((k_ref, 64), (v_ref, 96)):
        kv = kv + dot(ref[...], spread(4, at + c * 4), TN)[0:8]
        kv = kv + dot(ref[...], spread(4, at + 16 + c * 4), TN)[8:16]
    low, high = q[0:8] + kv, q[8:16] + kv
    first = c == 0
    segments = s_ref[...].astype(F32).astype(BF16)
    for ref, tile in (
        (keep_ref, jnp.where(first, low, high)),
        (send_ref, jnp.where(first, high, low)),
    ):
        ref[0:8, :] = tile.astype(BF16)
        ref[8:12, :] = segments
        ref[12:16, :] = jnp.zeros((4, 128), BF16)


def spread_body(keep_ref, came_ref, out_ref):
    lane = lanes((8, 128))
    mine = jnp.where(lane < 64, lane // 32, (lane // 4) % 2) == lax.axis_index("c")
    tile = jnp.where(mine, keep_ref[0:8, :].astype(F32), came_ref[0:8, :].astype(F32)).astype(BF16)
    for d in range(out_ref.shape[0]):
        out_ref[d] = tile


def turn(angle):
    quarter = jnp.floor(angle * 0.6366197723675814 + 0.5)
    rest = angle - quarter * 1.5703125
    rest = rest - quarter * 4.837512969970703e-4
    rest = rest - quarter * 7.549789948768648e-8
    square = rest * rest
    sine = -1.9515295891e-4 * square + 8.3321608736e-3
    sine = (sine * square - 1.6666654611e-1) * square * rest + rest
    cosine = 2.443315711809948e-5 * square - 1.388731625493765e-3
    cosine = (cosine * square + 4.166664568298827e-2) * square * square - 0.5 * square + 1.0
    which = quarter.astype(jnp.int32) % 4
    odd = which % 2 == 1
    cosine, sine = jnp.where(odd, sine, cosine), jnp.where(odd, cosine, sine)
    cosine = jnp.where((which == 1) | (which == 2), -cosine, cosine)
    sine = jnp.where(which >= 2, -sine, sine)
    return cosine, sine


def rope_tables(positions):
    shape = (3, 128)
    index = lanes(shape) % 64
    section = jnp.where(index < 16, 0, jnp.where(index < 40, 1, 2))
    chosen = where_one(section == rows_of(shape))
    high = positions // 64
    low = positions - high * 64
    position = 64.0 * dot(high.astype(F32).astype(BF16), chosen, TN)
    position = position + dot(low.astype(F32).astype(BF16), chosen, TN)
    index = lanes((ROWS, 128)) % 64
    inverse = jnp.ones((ROWS, 128), F32)
    for bit in range(6):
        step = 1000000.0 ** (-2.0 * 2**bit / HD)
        inverse = jnp.where((index // 2**bit) % 2 == 1, inverse * step, inverse)
    cosine, sine = turn(position * inverse)
    return cosine, jnp.where(lanes((ROWS, 128)) < 64, -sine, sine)


def rotate(value, cosine, sine):
    return value * cosine + move(value, 64) * sine


def split_pair(value):
    high = value.astype(BF16).astype(F32)
    return high, (value - high).astype(BF16).astype(F32)


def state_rows(peak, total):
    row = rows_of((8, 128))
    parts = (*split_pair(peak), *split_pair(total))
    tile = jnp.zeros((8, 128), F32)
    for n, part in enumerate(parts):
        tile = jnp.where(row == n, part, tile)
    return tile.astype(BF16)


def attend_body(
    in_ref, keep_ref, came_ref, pos_ref, seg_ref, k2_ref, v2_ref, k_hbm, v_hbm,
    out_ref, q_ref, rope_ref, bias_ref, k_ref, v_ref, sems,
):
    copies = fetch((k_hbm, v_hbm), (k_ref, v_ref), sems)
    for copy in copies:
        copy.start()
    c = lax.axis_index("c")
    y0 = lax.axis_index("y")
    duty = (lax.axis_index("z") == 0) & (lax.axis_index("x") == 0)
    lane = lanes((8, 128))
    cosine, sine = rope_tables(pos_ref[...])
    rope_ref[0] = cosine
    rope_ref[1] = sine
    half = pl.ds(pl.multiple_of(c * 8, 8), 8)
    half_cosine, half_sine = rope_ref[0, half, :], rope_ref[1, half, :]

    for y in range(4):
        q_ref[y] = jnp.zeros((128, 256), BF16)
        for z in range(8):
            upper = z // 4
            for p in range(2):
                n = (y * 8 + z) * 4 + 2 * p
                a, b = in_ref[n].astype(F32), in_ref[n + 1].astype(F32)
                whole = jnp.where(lane < 64, a, move(b, 64))
                at = upper * 64 + ((z % 4) * 2 + p) * 8
                q_ref[y, at : at + 8, upper * 128 : (upper + 1) * 128] = rotate(
                    whole, half_cosine, half_sine
                ).astype(BF16)

    found = []
    for kind in range(2):
        for upper in range(2):
            parts = []
            for late in range(2):
                value = jnp.zeros((8, 128), F32)
                for z in range(4):
                    for x in range(4):
                        tile = in_ref[(y0 * 8 + upper * 4 + z) * 4 + x].astype(F32)
                        at = z * 32 + x * 8
                        value = jnp.where(
                            (lane >= at) & (lane < at + 8),
                            move(tile, at - 64 - kind * 32 - late * 16),
                            value,
                        )
                parts.append(value)
            found.append(jnp.concatenate(parts, axis=0))
    span_k = jnp.concatenate([rotate(f, cosine, sine) for f in found[:2]], axis=1).astype(BF16)
    span_v = jnp.concatenate(found[2:], axis=1).astype(BF16)

    row_of_lane = c * 8 + lanes((ROWS, 128)) % 8
    pick = where_one(rows_of((ROWS, 128)) == row_of_lane)
    kinds = where_one(rows_of((8, ROWS)) == seg_ref[...])
    wanted = dot(kinds, pick, (((1,), (0,)), ((), ()))).astype(BF16)
    for n, ref in enumerate((keep_ref, came_ref)):
        for part in range(4):
            held = ref[8 + part : 9 + part, :].astype(F32)
            have = where_one(rows_of((8, 128)).astype(F32) == held)
            at = n * 512 + part * 128
            bias_ref[at : at + 128, :] = (dot(have, wanted, TN) - 1.0) * -HIDDEN
    seen = dot(kinds, wanted, TN) * jnp.where(rows_of((ROWS, 128)) <= row_of_lane, 1.0, 0.0)
    span_bias = (seen - 1.0) * -HIDDEN

    for copy in copies:
        copy.wait()
    factor = LOG2E / HD**0.5
    span_s = dot(span_k, q_ref[y0], NT) * factor + span_bias
    for y in range(4):
        q = q_ref[y]
        at = slice(y * 256, (y + 1) * 256)
        absent = jnp.where(duty & (y0 == y), 0.0, HIDDEN)
        scores = [
            dot(ref[:, at], q, NT) * factor + bias_ref[n * 512 : (n + 1) * 512, :]
            for n, ref in enumerate((k_ref, k2_ref))
        ]
        scores.append(span_s + absent)
        peak = functools.reduce(
            jnp.maximum, [jnp.max(s, axis=0, keepdims=True) for s in scores], jnp.float32(NONE)
        )
        high, low = split_pair(peak)
        peak = high + low
        weights = [jnp.exp2(s - peak) for s in scores]
        total = sum(jnp.sum(w, axis=0, keepdims=True) for w in weights)
        out = dot(v_ref[:, at].T, weights[0].astype(BF16), (((1,), (0,)), ((), ())))
        out = out + dot(v2_ref[:, at].T, weights[1].astype(BF16), (((1,), (0,)), ((), ())))
        out = out + dot(span_v, weights[2].astype(BF16), TN)
        out = jnp.where(lanes((128, 128)) < 64, out[:128], out[128:]).astype(BF16)
        state = state_rows(peak, total)
        for n in range(4):
            out_ref[y * 4 + n, 0:32, :] = out[n * 32 : (n + 1) * 32]
            out_ref[y * 4 + n, 32:40, :] = state


def merged(in_ref):
    count = in_ref.shape[0]
    peaks, totals = [], []
    for n in range(count):
        state = in_ref[n, 32:40, :].astype(F32)
        peaks.append(state[0:1] + state[1:2])
        totals.append(state[2:3] + state[3:4])
    peak = functools.reduce(jnp.maximum, peaks)
    out = jnp.zeros((32, 128), F32)
    total = jnp.zeros((1, 128), F32)
    for n in range(count):
        factor = jnp.exp2(peaks[n] - peak)
        out = out + in_ref[n, 0:32, :].astype(F32) * factor
        total = total + totals[n] * factor
    return out, peak, total


def merge_body(in_ref, out_ref):
    out, peak, total = merged(in_ref)
    out = out.astype(BF16)
    state = state_rows(peak, total)
    for d in range(out_ref.shape[0]):
        out_ref[d, 0:32, :] = out
        out_ref[d, 32:40, :] = state


def finish_body(in_ref, out_ref):
    out, _, total = merged(in_ref)
    out = (out / total).astype(BF16)
    for d in range(out_ref.shape[0]):
        out_ref[d] = out


def turned(in_ref, store):
    eye = where_one(rows_of((128, 128)) == lanes((128, 128)))
    for y in range(4):
        block = dot(eye, in_ref[y * 4 : (y + 1) * 4].reshape(128, 128), NT).astype(BF16)
        for i in range(16):
            store((y * 16 + i) * HD, block[i * 8 : (i + 1) * 8])


def half_body(in_ref, out_ref):
    def store(at, piece):
        out_ref[:, at : at + HD] = piece

    turned(in_ref, store)


def place_body(in_ref, own_ref, out_ref):
    c = lax.axis_index("c")
    out_ref[pl.ds(pl.multiple_of(c * 8, 8), 8), :] = own_ref[...]
    rows = pl.ds(pl.multiple_of((1 - c) * 8, 8), 8)

    def store(at, piece):
        out_ref[rows, at : at + HD] = piece

    turned(in_ref, store)


def per_device(
    queries,
    span_keys,
    span_values,
    positions,
    span_segments,
    cache_keys,
    cache_values,
    cache_segments,
):
    shape = jax.ShapeDtypeStruct
    tile = shape((16, 128), BF16)
    keep, send, positions, span_segments = call(
        pack_body,
        (tile, tile, shape((3, ROWS), jnp.int32), shape((1, ROWS), jnp.int32)),
        queries,
        span_keys.T,
        span_values.T,
        cache_segments.reshape(4, 128),
        positions,
        span_segments.reshape(1, ROWS),
        specs=[HBM] * 6,
        scratch=[
            pltpu.VMEM((ROWS, 32), BF16),
            pltpu.VMEM((4, ROWS), BF16),
            pltpu.VMEM((4, ROWS), BF16),
            pltpu.VMEM((4, 128), jnp.int32),
            pltpu.SemaphoreType.DMA((6,)),
        ],
    )
    came = swap(send)
    came, cache_keys, cache_values = lax.optimization_barrier((came, cache_keys, cache_values))
    other_keys = swap(cache_keys)
    other_values = swap(cache_values)
    tiles = call(spread_body, shape((128, 8, 128), BF16), keep, came)
    tiles = exchange(tiles, CHIPS)
    parts = call(
        attend_body,
        shape((16, 40, 128), BF16),
        tiles,
        keep,
        came,
        positions,
        span_segments,
        other_keys,
        other_values,
        cache_keys,
        cache_values,
        specs=[VMEM] * 7 + [HBM] * 2,
        scratch=[
            pltpu.VMEM((4, 128, 256), BF16),
            pltpu.VMEM((2, ROWS, 128), F32),
            pltpu.VMEM((1024, 128), F32),
            pltpu.VMEM((512, 1024), BF16),
            pltpu.VMEM((512, 1024), BF16),
            pltpu.SemaphoreType.DMA((2,)),
        ],
        limit=12 << 20,
    )
    parts = exchange(parts, PLANE)
    parts = call(merge_body, shape((8, 40, 128), BF16), parts)
    parts = exchange(parts, ("z",))
    whole = call(finish_body, shape((16, 32, 128), BF16), parts)
    whole = exchange(whole, PLANE)
    other = swap(whole)
    own = call(half_body, shape((8, H * HD), BF16), whole)
    return call(place_body, shape((ROWS, H * HD), BF16), other, own)


def solution(mesh):
    split = Mesh(mesh.devices.reshape(4, 8, 4, 2), ALL)
    return jax.shard_map(
        per_device,
        mesh=split,
        in_specs=(
            P(None, ALL),
            P(None, ALL),
            P(None, ALL),
            P(),
            P(),
            P(ALL, None),
            P(ALL, None),
            P(ALL),
        ),
        out_specs=P(),
        check_vma=False,
    )
```

```python
import functools

import jax
import jax.numpy as jnp
from jax import lax
from jax.experimental import pallas as pl
from jax.experimental.pallas import tpu as pltpu
from jax.sharding import Mesh
from jax.sharding import PartitionSpec as P

H = 64
KVH = 8
HD = 128
ROWS = 16
ALL = ("y", "z", "x", "c")
CHIPS = ("y", "z", "x")
PLANE = ("y", "x")
LOG2E = 1.4426950408889634
NONE = -1e30
HIDDEN = -2e30
F32 = jnp.float32
BF16 = jnp.bfloat16
VMEM = pl.BlockSpec(memory_space=pltpu.VMEM)
NT = (((1,), (1,)), ((), ()))


def call(body, name, out_shape, *args, specs=None, scratch=(), limit=8 << 20):
    return pl.pallas_call(
        body,
        name=name,
        out_shape=out_shape,
        in_specs=specs or [VMEM] * len(args),
        out_specs=jax.tree.map(lambda _: VMEM, out_shape),
        scratch_shapes=scratch,
        compiler_params=pltpu.CompilerParams(vmem_limit_bytes=limit),
    )(*args)


def lanes(shape):
    return lax.broadcasted_iota(jnp.int32, shape, len(shape) - 1)


def move(value, by):
    by %= value.shape[-1]
    return pltpu.roll(value, by, value.ndim - 1) if by else value


def exchange(tiles, axes):
    return lax.all_to_all(tiles, axes, 0, 0, tiled=True)


def swap(value):
    return lax.ppermute(value, "c", ((0, 1), (1, 0)))


def rows_of(shape):
    return lax.broadcasted_iota(jnp.int32, shape, 0)


TN = (((0,), (0,)), ((), ()))
NN = (((1,), (0,)), ((), ()))


def dot(a, b, dims):
    return lax.dot_general(a, b, dims, preferred_element_type=F32)


def where_one(hit):
    return jnp.where(hit, 1.0, 0.0).astype(BF16)


def pack_body(q_ref, k_ref, v_ref, out_ref):
    def spread(count, at):
        return where_one(lanes((count, 128)) == rows_of((count, 128)) + at)

    tile = jnp.zeros((8, 128), F32)
    for late in range(2):
        part = dot(q_ref[...], spread(32, late * 32), NN)
        for ref, at in ((k_ref, 64), (v_ref, 96)):
            part = part + dot(ref[...], spread(4, at + late * 16), TN)
        tile = tile + part[late * 8 : (late + 1) * 8]
    tile = tile.astype(BF16)
    for d in range(out_ref.shape[0]):
        out_ref[d] = tile


def turn(angle):
    quarter = jnp.floor(angle * 0.6366197723675814 + 0.5)
    rest = angle - quarter * 1.5703125
    rest = rest - quarter * 4.837512969970703e-4
    rest = rest - quarter * 7.549789948768648e-8
    square = rest * rest
    sine = -1.9515295891e-4 * square + 8.3321608736e-3
    sine = (sine * square - 1.6666654611e-1) * square * rest + rest
    cosine = 2.443315711809948e-5 * square - 1.388731625493765e-3
    cosine = (cosine * square + 4.166664568298827e-2) * square * square - 0.5 * square + 1.0
    which = quarter.astype(jnp.int32) % 4
    odd = which % 2 == 1
    cosine, sine = jnp.where(odd, sine, cosine), jnp.where(odd, cosine, sine)
    cosine = jnp.where((which == 1) | (which == 2), -cosine, cosine)
    sine = jnp.where(which >= 2, -sine, sine)
    return cosine, sine


def rope_tables(positions, index):
    section = jnp.where(index < 16, 0, jnp.where(index < 40, 1, 2))
    high = positions // 64
    position = jnp.zeros(index.shape, F32)
    for scale, part in ((64.0, high), (1.0, positions - high * 64)):
        chosen = dot(part.astype(F32).astype(BF16), where_one(rows_of((3, 3 * 128)) == lanes((3, 3 * 128)) // 128), TN)
        picked = chosen[:, 256:]
        for n in range(2):
            picked = jnp.where(section == n, chosen[:, n * 128 : (n + 1) * 128], picked)
        position = position + scale * picked
    inverse = jnp.ones(index.shape, F32)
    for bit in range(6):
        step = 1000000.0 ** (-2.0 * 2**bit / HD)
        inverse = jnp.where((index // 2**bit) % 2 == 1, inverse * step, inverse)
    return turn(position * inverse)


def rotate(value, cosine, sine):
    return value * cosine + move(value, 64) * sine


def split_pair(value):
    high = value.astype(BF16).astype(F32)
    return high, (value - high).astype(BF16).astype(F32)


def state_rows(peak, total):
    row = rows_of((8, 128))
    parts = (*split_pair(peak), *split_pair(total))
    tile = jnp.zeros((8, 128), F32)
    for n, part in enumerate(parts):
        tile = jnp.where(row == n, part, tile)
    return tile.astype(BF16)


def ready_body(in_ref, pos_ref, seg_ref, held_ref, v_ref, q_ref, vt_ref, bias_ref, table_ref):
    c = lax.axis_index("c")
    lane = lanes((ROWS, 128))
    for n in range(2):
        own = n == 0
        cosine, sine = rope_tables(pos_ref[...], lane % 32 + jnp.where(own, c, 1 - c) * 32)
        late = (lane // 32) % 2 == 1
        cosine = jnp.where(late[:8], cosine[8:], cosine[:8])
        sine = jnp.where(late[:8], sine[8:], sine[:8])
        table_ref[2 * n] = cosine
        table_ref[2 * n + 1] = jnp.where(lane[:8] < 64, -sine, sine)
    cosine, sine = rope_tables(pos_ref[...], lane % 64)
    table_ref[4], table_ref[5] = cosine[:8], cosine[8:]
    sine = jnp.where(lane < 64, -sine, sine)
    table_ref[6], table_ref[7] = sine[:8], sine[8:]
    rotate_pairs(in_ref, q_ref, table_ref[0], table_ref[1])
    for g in range(KVH):
        vt_ref[g] = v_ref[:, g * HD : (g + 1) * HD].T
    pick = where_one(rows_of((ROWS, 128)) == lane % ROWS)
    kinds = where_one(rows_of((8, ROWS)) == seg_ref[...])
    wanted = dot(kinds, pick, NN).astype(BF16)
    for part in range(4):
        have = where_one(rows_of((8, 128)) == held_ref[part : part + 1, :])
        bias_ref[part * 128 : (part + 1) * 128, :] = (dot(have, wanted, TN) - 1.0) * -HIDDEN
    seen = dot(kinds, wanted, TN) * jnp.where(rows_of((ROWS, 128)) <= lane % ROWS, 1.0, 0.0)
    bias_ref[512:, :] = (seen - 1.0) * -HIDDEN


def rotate_pairs(in_ref, out_ref, cosine, sine):
    lane = lanes((8, 128))
    for n in range(64):
        a, b = in_ref[2 * n].astype(F32), in_ref[2 * n + 1].astype(F32)
        out_ref[n] = rotate(jnp.where(lane < 64, a, move(b, 64)), cosine, sine)


def join_body(own_ref, in_ref, table_ref, q_ref, other_ref):
    c = lax.axis_index("c")
    rotate_pairs(in_ref, other_ref, table_ref[2], table_ref[3])
    lane = lanes((8, 128))
    first = c == 0
    near = lane % 64 < 32
    for n in range(64):
        own, other = own_ref[n], other_ref[n]
        low, high = jnp.where(first, own, other), jnp.where(first, other, own)
        z, p = (n // 2) % 8, n % 2
        head = (n // 16) * 16 + z * 2 + p
        q_ref[head * 16 : head * 16 + 8, :] = jnp.where(near, low, move(high, 32)).astype(BF16)
        q_ref[head * 16 + 8 : head * 16 + 16, :] = jnp.where(near, move(low, -32), high).astype(BF16)


def attend(q, k, vt, bias, span):
    factor = LOG2E / HD**0.5
    scores = [dot(k, q, NT) * factor + bias]
    if span is not None:
        scores.append(dot(span[0], q, NT) * factor + span[2])
    peak = functools.reduce(
        jnp.maximum, [jnp.max(s, axis=0, keepdims=True) for s in scores], jnp.float32(NONE)
    )
    high, low = split_pair(peak)
    peak = high + low
    weights = [jnp.exp2(s - peak) for s in scores]
    total = sum(jnp.sum(w, axis=0, keepdims=True) for w in weights)
    out = dot(vt, weights[0].astype(BF16), NN)
    if span is not None:
        out = out + dot(span[1], weights[1].astype(BF16), TN)
    return out.astype(BF16), state_rows(peak, total)


def emit(out_ref, i, result):
    for n in range(4):
        out_ref[i * 4 + n, 0:32, :] = result[0][n * 32 : (n + 1) * 32]
        out_ref[i * 4 + n, 32:40, :] = result[1]


def heads_at(base, i):
    return pl.ds(pl.multiple_of((base + i) * 128, 128), 128)


def first_body(q_ref, k_ref, vt_ref, bias_ref, out_ref):
    base = (1 - lax.axis_index("c")) * 4
    for i in range(4):
        at = heads_at(base, i)
        emit(out_ref, i, attend(q_ref[at, :], k_ref[:, at], vt_ref[base + i], bias_ref[0:512, :], None))


def second_body(q_ref, k_ref, vt_ref, bias_ref, in_ref, came_ref, table_ref, out_ref):
    c, y = lax.axis_index("c"), lax.axis_index("y")
    base = c * 4
    lane = lanes((8, 128))
    duty = (lax.axis_index("z") == 0) & (lax.axis_index("x") == 0)
    g = base + y
    start = (g // 2) * 32 + (g % 2) * 16
    found = []
    for kind in range(2):
        parts = []
        for late in range(2):
            value = jnp.zeros((8, 128), F32)
            for n in range(16):
                own, came = in_ref[start + n].astype(F32), came_ref[start + n].astype(F32)
                pair = (jnp.where(c == 0, own, came), jnp.where(c == 0, came, own))
                for core in range(2):
                    at = n * 8 + core * 4
                    value = jnp.where(
                        (lane >= at) & (lane < at + 4),
                        move(pair[core], at - 64 - kind * 32 - late * 16),
                        value,
                    )
            parts.append(value)
        if kind == 0:
            parts = [rotate(v, table_ref[4 + n], table_ref[6 + n]) for n, v in enumerate(parts)]
        found.append(jnp.concatenate(parts, axis=0).astype(BF16))
    for i in range(4):
        at = heads_at(base, i)
        absent = jnp.where(duty & (y == i), 0.0, HIDDEN)
        span = (found[0], found[1], bias_ref[512:, :] + absent)
        emit(out_ref, i, attend(q_ref[at, :], k_ref[:, at], vt_ref[base + i], bias_ref[0:512, :], span))


def couple_body(own_ref, came_ref, out_ref):
    for n in range(16):
        out, peak, total = merged([own_ref.at[n], came_ref.at[n]])
        out_ref[n, 0:32, :] = out.astype(BF16)
        out_ref[n, 32:40, :] = state_rows(peak, total)


def merged(refs):
    peaks, totals = [], []
    for ref in refs:
        state = ref[32:40, :].astype(F32)
        peaks.append(state[0:1] + state[1:2])
        totals.append(state[2:3] + state[3:4])
    peak = functools.reduce(jnp.maximum, peaks)
    out = jnp.zeros((32, 128), F32)
    total = jnp.zeros((1, 128), F32)
    for n, ref in enumerate(refs):
        factor = jnp.exp2(peaks[n] - peak)
        out = out + ref[0:32, :].astype(F32) * factor
        total = total + totals[n] * factor
    return out, peak, total


def merge_body(in_ref, out_ref):
    out, peak, total = merged([in_ref.at[n] for n in range(in_ref.shape[0])])
    out = out.astype(BF16)
    state = state_rows(peak, total)
    for d in range(out_ref.shape[0]):
        out_ref[d, 0:32, :] = out
        out_ref[d, 32:40, :] = state


def finish_body(in_ref, out_ref):
    out, _, total = merged([in_ref.at[n] for n in range(in_ref.shape[0])])
    out = (out / total).astype(BF16)
    for d in range(out_ref.shape[0]):
        out_ref[d] = out


def turned(in_ref, store):
    eye = where_one(rows_of((128, 128)) == lanes((128, 128)))
    for g in range(4):
        block = dot(eye, in_ref[g * 4 : (g + 1) * 4].reshape(128, 128), NT).astype(BF16)
        for i in range(8):
            store((g * 8 + i) * HD, block[i * ROWS : (i + 1) * ROWS])


def half_body(in_ref, out_ref):
    def store(at, piece):
        out_ref[:, at : at + HD] = piece

    turned(in_ref, store)


def place_body(in_ref, own_ref, out_ref):
    c = lax.axis_index("c")
    half = H * HD // 2
    out_ref[:, pl.ds(pl.multiple_of(c * half, half), half)] = own_ref[...]

    def store(at, piece):
        out_ref[:, pl.ds(pl.multiple_of((1 - c) * half + at, HD), HD)] = piece

    turned(in_ref, store)


def per_device(
    queries,
    span_keys,
    span_values,
    positions,
    span_segments,
    cache_keys,
    cache_values,
    cache_segments,
):
    shape = jax.ShapeDtypeStruct
    tiles = call(
        pack_body, "pack", shape((128, 8, 128), BF16), queries, span_keys.T, span_values.T
    )
    tiles = exchange(tiles, CHIPS)
    came = swap(tiles)
    own, turned_values, bias, tables = call(
        ready_body,
        "ready",
        (
            shape((64, 8, 128), F32),
            shape((KVH, HD, 512), BF16),
            shape((512 + ROWS, 128), F32),
            shape((8, 8, 128), F32),
        ),
        tiles,
        positions,
        span_segments.reshape(1, ROWS),
        cache_segments.reshape(4, 128),
        cache_values,
    )
    q = call(
        join_body,
        "join",
        shape((H * ROWS, HD), BF16),
        own,
        came,
        tables,
        scratch=[pltpu.VMEM((64, 8, 128), F32)],
    )
    message = shape((16, 40, 128), BF16)
    parts = call(first_body, "first", message, q, cache_keys, turned_values, bias)
    other = swap(parts)
    parts = call(
        second_body, "second", message, q, cache_keys, turned_values, bias, tiles, came, tables
    )
    parts = call(couple_body, "couple", message, parts, other)
    parts = exchange(parts, PLANE)
    parts = call(merge_body, "merge", shape((8, 40, 128), BF16), parts)
    parts = exchange(parts, ("z",))
    whole = call(finish_body, "finish", shape((16, 32, 128), BF16), parts)
    whole = exchange(whole, PLANE)
    other = swap(whole)
    own = call(half_body, "half", shape((ROWS, H * HD // 2), BF16), whole)
    return call(place_body, "place", shape((ROWS, H * HD), BF16), other, own)


def solution(mesh):
    split = Mesh(mesh.devices.reshape(4, 8, 4, 2), ALL)
    return jax.shard_map(
        per_device,
        mesh=split,
        in_specs=(
            P(None, ALL),
            P(None, ALL),
            P(None, ALL),
            P(),
            P(),
            P(ALL, None),
            P(ALL, None),
            P(ALL),
        ),
        out_specs=P(),
        check_vma=False,
    )
```

```python
import functools

import jax
import jax.numpy as jnp
from jax import lax
from jax.experimental import pallas as pl
from jax.experimental.pallas import tpu as pltpu
from jax.sharding import Mesh
from jax.sharding import PartitionSpec as P

H = 64
KVH = 8
HD = 128
ROWS = 16
ALL = ("y", "z", "x", "c")
CHIPS = ("y", "z", "x")
PLANE = ("y", "x")
LOG2E = 1.4426950408889634
NONE = -1e30
HIDDEN = -2e30
F32 = jnp.float32
BF16 = jnp.bfloat16
VMEM = pl.BlockSpec(memory_space=pltpu.VMEM)
NT = (((1,), (1,)), ((), ()))


def call(body, name, out_shape, *args, specs=None, scratch=(), limit=8 << 20):
    return pl.pallas_call(
        body,
        name=name,
        out_shape=out_shape,
        in_specs=specs or [VMEM] * len(args),
        out_specs=jax.tree.map(lambda _: VMEM, out_shape),
        scratch_shapes=scratch,
        compiler_params=pltpu.CompilerParams(vmem_limit_bytes=limit),
    )(*args)


def lanes(shape):
    return lax.broadcasted_iota(jnp.int32, shape, len(shape) - 1)


def move(value, by):
    by %= value.shape[-1]
    return pltpu.roll(value, by, value.ndim - 1) if by else value


def exchange(tiles, axes):
    return lax.all_to_all(tiles, axes, 0, 0, tiled=True)


def swap(value):
    return lax.ppermute(value, "c", ((0, 1), (1, 0)))


def rows_of(shape):
    return lax.broadcasted_iota(jnp.int32, shape, 0)


TN = (((0,), (0,)), ((), ()))
NN = (((1,), (0,)), ((), ()))


def dot(a, b, dims):
    return lax.dot_general(a, b, dims, preferred_element_type=F32)


def where_one(hit):
    return jnp.where(hit, 1.0, 0.0).astype(BF16)


def pack_body(q_ref, k_ref, v_ref, *rest):
    out_ref = rest[-1]
    turn = (lax.axis_index("x") % 2) * 64

    def spread(count, at):
        return where_one(lanes((count, 128)) == rows_of((count, 128)) + (at + turn) % 128)

    tile = jnp.zeros((8, 128), F32)
    for late in range(2):
        part = dot(q_ref[...], spread(32, late * 32), NN)
        for ref, at in ((k_ref, 64), (v_ref, 96)):
            part = part + dot(ref[...], spread(4, at + late * 16), TN)
        tile = tile + part[late * 8 : (late + 1) * 8]
    tile = tile.astype(BF16)
    for d in range(out_ref.shape[0]):
        out_ref[d] = tile


def turn(angle):
    quarter = jnp.floor(angle * 0.6366197723675814 + 0.5)
    rest = angle - quarter * 1.5703125
    rest = rest - quarter * 4.837512969970703e-4
    rest = rest - quarter * 7.549789948768648e-8
    square = rest * rest
    sine = -1.9515295891e-4 * square + 8.3321608736e-3
    sine = (sine * square - 1.6666654611e-1) * square * rest + rest
    cosine = 2.443315711809948e-5 * square - 1.388731625493765e-3
    cosine = (cosine * square + 4.166664568298827e-2) * square * square - 0.5 * square + 1.0
    which = quarter.astype(jnp.int32) % 4
    odd = which % 2 == 1
    cosine, sine = jnp.where(odd, sine, cosine), jnp.where(odd, cosine, sine)
    cosine = jnp.where((which == 1) | (which == 2), -cosine, cosine)
    sine = jnp.where(which >= 2, -sine, sine)
    return cosine, sine


def rope_tables(positions, index):
    section = jnp.where(index < 16, 0, jnp.where(index < 40, 1, 2))
    high = positions // 64
    position = jnp.zeros(index.shape, F32)
    for scale, part in ((64.0, high), (1.0, positions - high * 64)):
        chosen = dot(part.astype(F32).astype(BF16), where_one(rows_of((3, 3 * 128)) == lanes((3, 3 * 128)) // 128), TN)
        picked = chosen[:, 256:]
        for n in range(2):
            picked = jnp.where(section == n, chosen[:, n * 128 : (n + 1) * 128], picked)
        position = position + scale * picked
    inverse = jnp.ones(index.shape, F32)
    for bit in range(6):
        step = 1000000.0 ** (-2.0 * 2**bit / HD)
        inverse = jnp.where((index // 2**bit) % 2 == 1, inverse * step, inverse)
    return turn(position * inverse)


def rotate(value, cosine, sine):
    return value * cosine + move(value, 64) * sine


def split_pair(value):
    high = value.astype(BF16).astype(F32)
    return high, (value - high).astype(BF16).astype(F32)


def state_rows(peak, total):
    row = rows_of((8, 128))
    parts = (*split_pair(peak), *split_pair(total))
    tile = jnp.zeros((8, 128), F32)
    for n, part in enumerate(parts):
        tile = jnp.where(row == n, part, tile)
    return tile.astype(BF16)


def ready_body(pos_ref, seg_ref, held_ref, v_ref, vt_ref, bias_ref, table_ref):
    lane = lanes((ROWS, 128))
    cosine, sine = rope_tables(pos_ref[...], lane % 64)
    table_ref[0] = cosine
    table_ref[1] = jnp.where(lane < 64, -sine, sine)
    for g in range(KVH):
        vt_ref[g] = v_ref[:, g * HD : (g + 1) * HD].T
    pick = where_one(rows_of((ROWS, 128)) == lane % ROWS)
    kinds = where_one(rows_of((8, ROWS)) == seg_ref[...])
    wanted = dot(kinds, pick, NN).astype(BF16)
    for part in range(4):
        have = where_one(rows_of((8, 128)) == held_ref[part : part + 1, :])
        bias_ref[part * 128 : (part + 1) * 128, :] = (dot(have, wanted, TN) - 1.0) * -HIDDEN
    seen = dot(kinds, wanted, TN) * jnp.where(rows_of((ROWS, 128)) <= lane % ROWS, 1.0, 0.0)
    bias_ref[512:, :] = (seen - 1.0) * -HIDDEN


def placing(core):
    row, lane = rows_of((128, 256)), lanes((128, 256))
    at = (row // 64) * 64 + core * 32 + row % 32 + ((row // 32) % 2) * 128
    return where_one(lane == at)


def join(own_ref, came_ref, table_ref, q_ref):
    c = lax.axis_index("c")
    near = lanes((1, 8, 128)) < 64

    def halves(ref):
        tiles = ref[...].astype(F32).reshape(64, 2, 8, 128)
        return jnp.where(near, tiles[:, 0], tiles[:, 1]).reshape(512, 128).astype(BF16)

    whole = dot(halves(own_ref), placing(c), NN) + dot(halves(came_ref), placing(1 - c), NN)
    for late in range(2):
        part = whole[:, late * 128 : (late + 1) * 128]
        at = slice(late * 8, (late + 1) * 8)
        cosine, sine = table_ref[0, at, :], table_ref[1, at, :]
        turned = move(part, 64).reshape(64, 8, 128)
        part = (part.reshape(64, 8, 128) * cosine[None] + turned * sine[None]).astype(BF16)
        for n in range(64):
            z, p = (n // 2) % 8, n % 2
            head = (n // 16) * 16 + z * 2 + p
            q_ref[head * 16 + late * 8 : head * 16 + late * 8 + 8, :] = part[n]


def attend(q, k, vt, bias, span):
    factor = LOG2E / HD**0.5
    scores = [dot(k, q, NT) * factor + bias]
    if span is not None:
        scores.append(dot(span[0], q, NT) * factor + span[2])
    peak = functools.reduce(
        jnp.maximum, [jnp.max(s, axis=0, keepdims=True) for s in scores], jnp.float32(NONE)
    )
    high, low = split_pair(peak)
    peak = high + low
    weights = [jnp.exp2(s - peak) for s in scores]
    total = sum(jnp.sum(w, axis=0, keepdims=True) for w in weights)
    out = dot(vt, weights[0].astype(BF16), NN)
    if span is not None:
        out = out + dot(span[1], weights[1].astype(BF16), TN)
    return out.astype(BF16), state_rows(peak, total)


def emit(out_ref, i, result):
    for n in range(4):
        out_ref[i * 4 + n, 0:32, :] = result[0][n * 32 : (n + 1) * 32]
        out_ref[i * 4 + n, 32:40, :] = result[1]


def heads_at(base, i):
    return pl.ds(pl.multiple_of((base + i) * 128, 128), 128)


def first_body(own_ref, came_ref, table_ref, k_ref, vt_ref, bias_ref, out_ref, q_ref):
    join(own_ref, came_ref, table_ref, q_ref)
    base = (1 - lax.axis_index("c")) * 4
    for i in range(4):
        at = heads_at(base, i)
        emit(out_ref, i, attend(q_ref[at, :], k_ref[:, at], vt_ref[base + i], bias_ref[0:512, :], None))


def second_body(q_ref, k_ref, vt_ref, bias_ref, in_ref, came_ref, table_ref, out_ref):
    c, y = lax.axis_index("c"), lax.axis_index("y")
    base = c * 4
    lane = lanes((8, 128))
    duty = (lax.axis_index("z") == 0) & (lax.axis_index("x") == 0)
    g = base + y
    start = (g // 2) * 32 + (g % 2) * 16
    found = []
    for kind in range(2):
        parts = []
        for late in range(2):
            value = jnp.zeros((8, 128), F32)
            for n in range(16):
                own, came = in_ref[start + n].astype(F32), came_ref[start + n].astype(F32)
                pair = (jnp.where(c == 0, own, came), jnp.where(c == 0, came, own))
                for core in range(2):
                    at = n * 8 + core * 4
                    held = (1 - n % 2) * 64 + kind * 32 + late * 16
                    value = jnp.where(
                        (lane >= at) & (lane < at + 4),
                        move(pair[core], at - held),
                        value,
                    )
            parts.append(value)
        if kind == 0:
            parts = [
                rotate(v, table_ref[0, n * 8 : n * 8 + 8, :], table_ref[1, n * 8 : n * 8 + 8, :])
                for n, v in enumerate(parts)
            ]
        found.append(jnp.concatenate(parts, axis=0).astype(BF16))
    for i in range(4):
        at = heads_at(base, i)
        absent = jnp.where(duty & (y == i), 0.0, HIDDEN)
        span = (found[0], found[1], bias_ref[512:, :] + absent)
        emit(out_ref, i, attend(q_ref[at, :], k_ref[:, at], vt_ref[base + i], bias_ref[0:512, :], span))


def couple_body(own_ref, came_ref, out_ref):
    for n in range(16):
        out, peak, total = merged([own_ref.at[n], came_ref.at[n]])
        out_ref[n, 0:32, :] = out.astype(BF16)
        out_ref[n, 32:40, :] = state_rows(peak, total)


def merged(refs):
    peaks, totals = [], []
    for ref in refs:
        state = ref[32:40, :].astype(F32)
        peaks.append(state[0:1] + state[1:2])
        totals.append(state[2:3] + state[3:4])
    peak = functools.reduce(jnp.maximum, peaks)
    out = jnp.zeros((32, 128), F32)
    total = jnp.zeros((1, 128), F32)
    for n, ref in enumerate(refs):
        factor = jnp.exp2(peaks[n] - peak)
        out = out + ref[0:32, :].astype(F32) * factor
        total = total + totals[n] * factor
    return out, peak, total


def merge_body(in_ref, out_ref):
    out, peak, total = merged([in_ref.at[n] for n in range(in_ref.shape[0])])
    out = out.astype(BF16)
    state = state_rows(peak, total)
    for d in range(out_ref.shape[0]):
        out_ref[d, 0:32, :] = out
        out_ref[d, 32:40, :] = state


def finish_body(in_ref, out_ref):
    out, _, total = merged([in_ref.at[n] for n in range(in_ref.shape[0])])
    out = (out / total).astype(BF16)
    for d in range(out_ref.shape[0]):
        out_ref[d] = out


def turned(in_ref, store):
    eye = where_one(rows_of((128, 128)) == lanes((128, 128)))
    for g in range(4):
        block = dot(eye, in_ref[g * 4 : (g + 1) * 4].reshape(128, 128), NT).astype(BF16)
        for i in range(8):
            store((g * 8 + i) * HD, block[i * ROWS : (i + 1) * ROWS])


def half_body(in_ref, out_ref):
    def store(at, piece):
        out_ref[:, at : at + HD] = piece

    turned(in_ref, store)


def place_body(in_ref, own_ref, out_ref):
    c = lax.axis_index("c")
    half = H * HD // 2
    out_ref[:, pl.ds(pl.multiple_of(c * half, half), half)] = own_ref[...]

    def store(at, piece):
        out_ref[:, pl.ds(pl.multiple_of((1 - c) * half + at, HD), HD)] = piece

    turned(in_ref, store)


def per_device(
    queries,
    span_keys,
    span_values,
    positions,
    span_segments,
    cache_keys,
    cache_values,
    cache_segments,
):
    shape = jax.ShapeDtypeStruct
    span_segments = span_segments.reshape(1, ROWS)
    cache_segments = cache_segments.reshape(4, 128)
    tiles = call(
        pack_body,
        "pack",
        shape((128, 8, 128), BF16),
        queries,
        span_keys.T,
        span_values.T,
        positions,
        span_segments,
        cache_segments,
    )
    tiles = exchange(tiles, CHIPS)
    came = swap(tiles)
    turned_values, bias, tables = call(
        ready_body,
        "ready",
        (
            shape((KVH, HD, 512), BF16),
            shape((512 + ROWS, 128), F32),
            shape((2, ROWS, 128), F32),
        ),
        positions,
        span_segments,
        cache_segments,
        cache_values,
    )
    message = shape((16, 40, 128), BF16)
    parts, q = call(
        first_body,
        "first",
        (message, shape((H * ROWS, HD), BF16)),
        tiles,
        came,
        tables,
        cache_keys,
        turned_values,
        bias,
    )
    other = swap(parts)
    parts = call(
        second_body, "second", message, q, cache_keys, turned_values, bias, tiles, came, tables
    )
    parts = call(couple_body, "couple", message, parts, other)
    parts = exchange(parts, PLANE)
    parts = call(merge_body, "merge", shape((8, 40, 128), BF16), parts)
    parts = exchange(parts, ("z",))
    whole = call(finish_body, "finish", shape((16, 32, 128), BF16), parts)
    whole = exchange(whole, PLANE)
    other = swap(whole)
    own = call(half_body, "half", shape((ROWS, H * HD // 2), BF16), whole)
    return call(place_body, "place", shape((ROWS, H * HD), BF16), other, own)


def solution(mesh):
    split = Mesh(mesh.devices.reshape(4, 8, 4, 2), ALL)
    return jax.shard_map(
        per_device,
        mesh=split,
        in_specs=(
            P(None, ALL),
            P(None, ALL),
            P(None, ALL),
            P(),
            P(),
            P(ALL, None),
            P(ALL, None),
            P(ALL),
        ),
        out_specs=P(),
        check_vma=False,
    )
```

```python
import functools

import jax
import jax.numpy as jnp
from jax import lax
from jax.experimental import pallas as pl
from jax.experimental.pallas import tpu as pltpu
from jax.sharding import Mesh
from jax.sharding import PartitionSpec as P

H = 64
KVH = 8
HD = 128
ROWS = 16
ALL = ("y", "z", "x", "c")
CHIPS = ("y", "z", "x")
PLANE = ("y", "x")
LOG2E = 1.4426950408889634
NONE = -1e30
HIDDEN = -2e30
F32 = jnp.float32
BF16 = jnp.bfloat16
VMEM = pl.BlockSpec(memory_space=pltpu.VMEM)
NT = (((1,), (1,)), ((), ()))

HBM = pl.BlockSpec(memory_space=pltpu.HBM)


def call(body, name, out_shape, *args, specs=None, scratch=(), limit=8 << 20):
    return pl.pallas_call(
        body,
        name=name,
        out_shape=out_shape,
        in_specs=specs or [VMEM] * len(args),
        out_specs=jax.tree.map(lambda _: VMEM, out_shape),
        scratch_shapes=scratch,
        compiler_params=pltpu.CompilerParams(vmem_limit_bytes=limit),
    )(*args)


def lanes(shape):
    return lax.broadcasted_iota(jnp.int32, shape, len(shape) - 1)


def move(value, by):
    by %= value.shape[-1]
    return pltpu.roll(value, by, value.ndim - 1) if by else value


def exchange(tiles, axes):
    return lax.all_to_all(tiles, axes, 0, 0, tiled=True)


def swap(value):
    return lax.ppermute(value, "c", ((0, 1), (1, 0)))


def rows_of(shape):
    return lax.broadcasted_iota(jnp.int32, shape, 0)


TN = (((0,), (0,)), ((), ()))
NN = (((1,), (0,)), ((), ()))


def dot(a, b, dims):
    return lax.dot_general(a, b, dims, preferred_element_type=F32)


def where_one(hit):
    return jnp.where(hit, 1.0, 0.0).astype(BF16)


def pack_body(*refs):
    out_ref, q_ref, k_ref, v_ref, sems = refs[6], *refs[10:]
    copies = [
        pltpu.make_async_copy(source, target, sems.at[n])
        for n, (source, target) in enumerate(zip(refs[:6], (q_ref, k_ref, v_ref, *refs[7:10])))
    ]
    for copy in copies:
        copy.start()
    for copy in copies:
        copy.wait()
    turn = (lax.axis_index("x") % 2) * 64

    def spread(count, at):
        return where_one(lanes((count, 128)) == rows_of((count, 128)) + (at + turn) % 128)

    tile = jnp.zeros((8, 128), F32)
    for late in range(2):
        part = dot(q_ref[...], spread(32, late * 32), NN)
        for ref, at in ((k_ref, 64), (v_ref, 96)):
            part = part + dot(ref[...], spread(4, at + late * 16), TN)
        tile = tile + part[late * 8 : (late + 1) * 8]
    tile = tile.astype(BF16)
    for d in range(out_ref.shape[0]):
        out_ref[d] = tile


def turn(angle):
    quarter = jnp.floor(angle * 0.6366197723675814 + 0.5)
    rest = angle - quarter * 1.5703125
    rest = rest - quarter * 4.837512969970703e-4
    rest = rest - quarter * 7.549789948768648e-8
    square = rest * rest
    sine = -1.9515295891e-4 * square + 8.3321608736e-3
    sine = (sine * square - 1.6666654611e-1) * square * rest + rest
    cosine = 2.443315711809948e-5 * square - 1.388731625493765e-3
    cosine = (cosine * square + 4.166664568298827e-2) * square * square - 0.5 * square + 1.0
    which = quarter.astype(jnp.int32) % 4
    odd = which % 2 == 1
    cosine, sine = jnp.where(odd, sine, cosine), jnp.where(odd, cosine, sine)
    cosine = jnp.where((which == 1) | (which == 2), -cosine, cosine)
    sine = jnp.where(which >= 2, -sine, sine)
    return cosine, sine


def rope_tables(positions, index):
    section = jnp.where(index < 16, 0, jnp.where(index < 40, 1, 2))
    high = positions // 64
    position = jnp.zeros(index.shape, F32)
    for scale, part in ((64.0, high), (1.0, positions - high * 64)):
        chosen = dot(part.astype(F32).astype(BF16), where_one(rows_of((3, 3 * 128)) == lanes((3, 3 * 128)) // 128), TN)
        picked = chosen[:, 256:]
        for n in range(2):
            picked = jnp.where(section == n, chosen[:, n * 128 : (n + 1) * 128], picked)
        position = position + scale * picked
    inverse = jnp.ones(index.shape, F32)
    for bit in range(6):
        step = 1000000.0 ** (-2.0 * 2**bit / HD)
        inverse = jnp.where((index // 2**bit) % 2 == 1, inverse * step, inverse)
    return turn(position * inverse)


def rotate(value, cosine, sine):
    return value * cosine + move(value, 64) * sine


def split_pair(value):
    high = value.astype(BF16).astype(F32)
    return high, (value - high).astype(BF16).astype(F32)


def state_rows(peak, total):
    row = rows_of((8, 128))
    parts = (*split_pair(peak), *split_pair(total))
    tile = jnp.zeros((8, 128), F32)
    for n, part in enumerate(parts):
        tile = jnp.where(row == n, part, tile)
    return tile.astype(BF16)


def ready_body(pos_ref, seg_ref, held_ref, k_hbm, v_hbm, bias_ref, table_ref, k_ref, vt_ref, v_ref, sems):
    copies = []
    for g in range(KVH):
        at = slice(g * HD, (g + 1) * HD)
        copies.append(pltpu.make_async_copy(v_hbm.at[:, at], v_ref.at[:, at], sems.at[g]))
    copies.append(pltpu.make_async_copy(k_hbm, k_ref, sems.at[KVH]))
    for copy in copies:
        copy.start()
    lane = lanes((ROWS, 128))
    cosine, sine = rope_tables(pos_ref[...], lane % 64)
    table_ref[0] = cosine
    table_ref[1] = jnp.where(lane < 64, -sine, sine)
    pick = where_one(rows_of((ROWS, 128)) == lane % ROWS)
    kinds = where_one(rows_of((8, ROWS)) == seg_ref[...])
    wanted = dot(kinds, pick, NN).astype(BF16)
    for part in range(4):
        have = where_one(rows_of((8, 128)) == held_ref[part : part + 1, :])
        bias_ref[part * 128 : (part + 1) * 128, :] = (dot(have, wanted, TN) - 1.0) * -HIDDEN
    seen = dot(kinds, wanted, TN) * jnp.where(rows_of((ROWS, 128)) <= lane % ROWS, 1.0, 0.0)
    bias_ref[512:, :] = (seen - 1.0) * -HIDDEN
    for g in range(KVH):
        copies[g].wait()
        vt_ref[g] = v_ref[:, g * HD : (g + 1) * HD].T
    copies[KVH].wait()


def placing(core):
    row, lane = rows_of((128, 256)), lanes((128, 256))
    at = (row // 64) * 64 + core * 32 + row % 32 + ((row // 32) % 2) * 128
    return where_one(lane == at)


def join(own_ref, came_ref, table_ref, q_ref):
    c = lax.axis_index("c")
    near = lanes((1, 8, 128)) < 64

    def halves(ref):
        tiles = ref[...].astype(F32).reshape(64, 2, 8, 128)
        return jnp.where(near, tiles[:, 0], tiles[:, 1]).reshape(512, 128).astype(BF16)

    whole = dot(halves(own_ref), placing(c), NN) + dot(halves(came_ref), placing(1 - c), NN)
    for late in range(2):
        part = whole[:, late * 128 : (late + 1) * 128]
        at = slice(late * 8, (late + 1) * 8)
        cosine, sine = table_ref[0, at, :], table_ref[1, at, :]
        turned = move(part, 64).reshape(64, 8, 128)
        part = (part.reshape(64, 8, 128) * cosine[None] + turned * sine[None]).astype(BF16)
        for n in range(64):
            z, p = (n // 2) % 8, n % 2
            head = (n // 16) * 16 + z * 2 + p
            q_ref[head * 16 + late * 8 : head * 16 + late * 8 + 8, :] = part[n]


def attend(q, k, vt, bias, span):
    factor = LOG2E / HD**0.5
    scores = [dot(k, q, NT) * factor + bias]
    if span is not None:
        scores.append(dot(span[0], q, NT) * factor + span[2])
    peak = functools.reduce(
        jnp.maximum, [jnp.max(s, axis=0, keepdims=True) for s in scores], jnp.float32(NONE)
    )
    high, low = split_pair(peak)
    peak = high + low
    weights = [jnp.exp2(s - peak) for s in scores]
    total = sum(jnp.sum(w, axis=0, keepdims=True) for w in weights)
    out = dot(vt, weights[0].astype(BF16), NN)
    if span is not None:
        out = out + dot(span[1], weights[1].astype(BF16), TN)
    return out.astype(BF16), state_rows(peak, total)


def emit(out_ref, i, result):
    for n in range(4):
        out_ref[i * 4 + n, 0:32, :] = result[0][n * 32 : (n + 1) * 32]
        out_ref[i * 4 + n, 32:40, :] = result[1]


def heads_at(base, i):
    return pl.ds(pl.multiple_of((base + i) * 128, 128), 128)


def first_body(own_ref, came_ref, table_ref, k_ref, vt_ref, bias_ref, out_ref, q_ref):
    join(own_ref, came_ref, table_ref, q_ref)
    base = (1 - lax.axis_index("c")) * 4
    for i in range(4):
        at = heads_at(base, i)
        emit(out_ref, i, attend(q_ref[at, :], k_ref[:, at], vt_ref[base + i], bias_ref[0:512, :], None))


def second_body(q_ref, k_ref, vt_ref, bias_ref, in_ref, came_ref, table_ref, out_ref):
    c, y = lax.axis_index("c"), lax.axis_index("y")
    base = c * 4
    lane = lanes((8, 128))
    duty = (lax.axis_index("z") == 0) & (lax.axis_index("x") == 0)
    g = base + y
    start = (g // 2) * 32 + (g % 2) * 16
    found = []
    for kind in range(2):
        parts = []
        for late in range(2):
            value = jnp.zeros((8, 128), F32)
            for n in range(16):
                own, came = in_ref[start + n].astype(F32), came_ref[start + n].astype(F32)
                pair = (jnp.where(c == 0, own, came), jnp.where(c == 0, came, own))
                for core in range(2):
                    at = n * 8 + core * 4
                    held = (1 - n % 2) * 64 + kind * 32 + late * 16
                    value = jnp.where(
                        (lane >= at) & (lane < at + 4),
                        move(pair[core], at - held),
                        value,
                    )
            parts.append(value)
        if kind == 0:
            parts = [
                rotate(v, table_ref[0, n * 8 : n * 8 + 8, :], table_ref[1, n * 8 : n * 8 + 8, :])
                for n, v in enumerate(parts)
            ]
        found.append(jnp.concatenate(parts, axis=0).astype(BF16))
    for i in range(4):
        at = heads_at(base, i)
        absent = jnp.where(duty & (y == i), 0.0, HIDDEN)
        span = (found[0], found[1], bias_ref[512:, :] + absent)
        emit(out_ref, i, attend(q_ref[at, :], k_ref[:, at], vt_ref[base + i], bias_ref[0:512, :], span))


def couple_body(own_ref, came_ref, out_ref):
    for n in range(16):
        out, peak, total = merged([own_ref.at[n], came_ref.at[n]])
        out_ref[n, 0:32, :] = out.astype(BF16)
        out_ref[n, 32:40, :] = state_rows(peak, total)


def merged(refs):
    peaks, totals = [], []
    for ref in refs:
        state = ref[32:40, :].astype(F32)
        peaks.append(state[0:1] + state[1:2])
        totals.append(state[2:3] + state[3:4])
    peak = functools.reduce(jnp.maximum, peaks)
    out = jnp.zeros((32, 128), F32)
    total = jnp.zeros((1, 128), F32)
    for n, ref in enumerate(refs):
        factor = jnp.exp2(peaks[n] - peak)
        out = out + ref[0:32, :].astype(F32) * factor
        total = total + totals[n] * factor
    return out, peak, total


def merge_body(in_ref, out_ref):
    out, peak, total = merged([in_ref.at[n] for n in range(in_ref.shape[0])])
    out = out.astype(BF16)
    state = state_rows(peak, total)
    for d in range(out_ref.shape[0]):
        out_ref[d, 0:32, :] = out
        out_ref[d, 32:40, :] = state


def finish_body(in_ref, out_ref):
    out, _, total = merged([in_ref.at[n] for n in range(in_ref.shape[0])])
    out = (out / total).astype(BF16)
    for d in range(out_ref.shape[0]):
        out_ref[d] = out


def turned(in_ref, store):
    eye = where_one(rows_of((128, 128)) == lanes((128, 128)))
    for g in range(4):
        block = dot(eye, in_ref[g * 4 : (g + 1) * 4].reshape(128, 128), NT).astype(BF16)
        for i in range(8):
            store((g * 8 + i) * HD, block[i * ROWS : (i + 1) * ROWS])


def half_body(in_ref, out_ref):
    def store(at, piece):
        out_ref[:, at : at + HD] = piece

    turned(in_ref, store)


def place_body(in_ref, own_ref, out_ref):
    c = lax.axis_index("c")
    half = H * HD // 2
    out_ref[:, pl.ds(pl.multiple_of(c * half, half), half)] = own_ref[...]

    def store(at, piece):
        out_ref[:, pl.ds(pl.multiple_of((1 - c) * half + at, HD), HD)] = piece

    turned(in_ref, store)


def per_device(
    queries,
    span_keys,
    span_values,
    positions,
    span_segments,
    cache_keys,
    cache_values,
    cache_segments,
):
    shape = jax.ShapeDtypeStruct
    small = (
        queries,
        span_keys.T,
        span_values.T,
        positions,
        span_segments.reshape(1, ROWS),
        cache_segments.reshape(4, 128),
    )
    tiles, positions, span_segments, cache_segments = call(
        pack_body,
        "pack",
        (shape((128, 8, 128), BF16), *(shape(a.shape, a.dtype) for a in small[3:])),
        *(pltpu.with_memory_space_constraint(a, pltpu.HBM) for a in small),
        specs=[HBM] * 6,
        scratch=[pltpu.VMEM(a.shape, a.dtype) for a in small[:3]] + [pltpu.SemaphoreType.DMA((6,))],
    )
    tiles = exchange(tiles, CHIPS)
    came = swap(tiles)
    bias, tables, keys, turned_values = call(
        ready_body,
        "ready",
        (
            shape((512 + ROWS, 128), F32),
            shape((2, ROWS, 128), F32),
            shape((512, KVH * HD), BF16),
            shape((KVH, HD, 512), BF16),
        ),
        positions,
        span_segments,
        cache_segments,
        *(pltpu.with_memory_space_constraint(a, pltpu.HBM) for a in (cache_keys, cache_values)),
        specs=[VMEM] * 3 + [HBM] * 2,
        scratch=[pltpu.VMEM((512, KVH * HD), BF16), pltpu.SemaphoreType.DMA((KVH + 1,))],
    )
    message = shape((16, 40, 128), BF16)
    parts, q = call(
        first_body,
        "first",
        (message, shape((H * ROWS, HD), BF16)),
        tiles,
        came,
        tables,
        keys,
        turned_values,
        bias,
    )
    other = swap(parts)
    parts = call(
        second_body, "second", message, q, keys, turned_values, bias, tiles, came, tables
    )
    parts = call(couple_body, "couple", message, parts, other)
    parts = exchange(parts, PLANE)
    parts = call(merge_body, "merge", shape((8, 40, 128), BF16), parts)
    parts = exchange(parts, ("z",))
    whole = call(finish_body, "finish", shape((16, 32, 128), BF16), parts)
    whole = exchange(whole, PLANE)
    other = swap(whole)
    own = call(half_body, "half", shape((ROWS, H * HD // 2), BF16), whole)
    return call(place_body, "place", shape((ROWS, H * HD), BF16), other, own)


def solution(mesh):
    split = Mesh(mesh.devices.reshape(4, 8, 4, 2), ALL)
    return jax.shard_map(
        per_device,
        mesh=split,
        in_specs=(
            P(None, ALL),
            P(None, ALL),
            P(None, ALL),
            P(),
            P(),
            P(ALL, None),
            P(ALL, None),
            P(ALL),
        ),
        out_specs=P(),
        check_vma=False,
    )
```

```python
import functools

import jax
import jax.numpy as jnp
from jax import lax
from jax.experimental import pallas as pl
from jax.experimental.pallas import tpu as pltpu
from jax.sharding import Mesh
from jax.sharding import PartitionSpec as P

H = 64
KVH = 8
HD = 128
ROWS = 16
ALL = ("y", "z", "x", "c")
CHIPS = ("y", "z", "x")
PLANE = ("y", "x")
LOG2E = 1.4426950408889634
NONE = -1e30
HIDDEN = -2e30
F32 = jnp.float32
BF16 = jnp.bfloat16
VMEM = pl.BlockSpec(memory_space=pltpu.VMEM)
NT = (((1,), (1,)), ((), ()))

HBM = pl.BlockSpec(memory_space=pltpu.HBM)


def call(body, name, out_shape, *args, specs=None, scratch=(), limit=8 << 20):
    return pl.pallas_call(
        body,
        name=name,
        out_shape=out_shape,
        in_specs=specs or [VMEM] * len(args),
        out_specs=jax.tree.map(lambda _: VMEM, out_shape),
        scratch_shapes=scratch,
        compiler_params=pltpu.CompilerParams(vmem_limit_bytes=limit),
    )(*args)


def lanes(shape):
    return lax.broadcasted_iota(jnp.int32, shape, len(shape) - 1)


def move(value, by):
    by %= value.shape[-1]
    return pltpu.roll(value, by, value.ndim - 1) if by else value


def exchange(tiles, axes):
    return lax.all_to_all(tiles, axes, 0, 0, tiled=True)


def swap(value):
    return lax.ppermute(value, "c", ((0, 1), (1, 0)))


def rows_of(shape):
    return lax.broadcasted_iota(jnp.int32, shape, 0)


TN = (((0,), (0,)), ((), ()))
NN = (((1,), (0,)), ((), ()))


def dot(a, b, dims):
    return lax.dot_general(a, b, dims, preferred_element_type=F32)


def where_one(hit):
    return jnp.where(hit, 1.0, 0.0).astype(BF16)


def pack_body(*refs):
    out_ref, q_ref, k_ref, v_ref, sems = refs[7], *refs[12:]
    copies = [
        pltpu.make_async_copy(source, target, sems.at[n])
        for n, (source, target) in enumerate(zip(refs[:7], (q_ref, k_ref, v_ref, *refs[8:12])))
    ]
    for copy in copies:
        copy.start()
    for copy in copies[:6]:
        copy.wait()
    turn = (lax.axis_index("x") % 2) * 64

    def spread(count, at):
        return where_one(lanes((count, 128)) == rows_of((count, 128)) + (at + turn) % 128)

    tile = jnp.zeros((8, 128), F32)
    for late in range(2):
        part = dot(q_ref[...], spread(32, late * 32), NN)
        for ref, at in ((k_ref, 64), (v_ref, 96)):
            part = part + dot(ref[...], spread(4, at + late * 16), TN)
        tile = tile + part[late * 8 : (late + 1) * 8]
    tile = tile.astype(BF16)
    for d in range(out_ref.shape[0]):
        out_ref[d] = tile
    copies[6].wait()


def turn(angle):
    quarter = jnp.floor(angle * 0.6366197723675814 + 0.5)
    rest = angle - quarter * 1.5703125
    rest = rest - quarter * 4.837512969970703e-4
    rest = rest - quarter * 7.549789948768648e-8
    square = rest * rest
    sine = -1.9515295891e-4 * square + 8.3321608736e-3
    sine = (sine * square - 1.6666654611e-1) * square * rest + rest
    cosine = 2.443315711809948e-5 * square - 1.388731625493765e-3
    cosine = (cosine * square + 4.166664568298827e-2) * square * square - 0.5 * square + 1.0
    which = quarter.astype(jnp.int32) % 4
    odd = which % 2 == 1
    cosine, sine = jnp.where(odd, sine, cosine), jnp.where(odd, cosine, sine)
    cosine = jnp.where((which == 1) | (which == 2), -cosine, cosine)
    sine = jnp.where(which >= 2, -sine, sine)
    return cosine, sine


def rope_tables(positions, index):
    section = jnp.where(index < 16, 0, jnp.where(index < 40, 1, 2))
    high = positions // 64
    position = jnp.zeros(index.shape, F32)
    for scale, part in ((64.0, high), (1.0, positions - high * 64)):
        chosen = dot(part.astype(F32).astype(BF16), where_one(rows_of((3, 3 * 128)) == lanes((3, 3 * 128)) // 128), TN)
        picked = chosen[:, 256:]
        for n in range(2):
            picked = jnp.where(section == n, chosen[:, n * 128 : (n + 1) * 128], picked)
        position = position + scale * picked
    inverse = jnp.ones(index.shape, F32)
    for bit in range(6):
        step = 1000000.0 ** (-2.0 * 2**bit / HD)
        inverse = jnp.where((index // 2**bit) % 2 == 1, inverse * step, inverse)
    return turn(position * inverse)


def rotate(value, cosine, sine):
    return value * cosine + move(value, 64) * sine


def split_pair(value):
    high = value.astype(BF16).astype(F32)
    return high, (value - high).astype(BF16).astype(F32)


def state_rows(peak, total):
    row = rows_of((8, 128))
    parts = (*split_pair(peak), *split_pair(total))
    tile = jnp.zeros((8, 128), F32)
    for n, part in enumerate(parts):
        tile = jnp.where(row == n, part, tile)
    return tile.astype(BF16)


def ready_body(pos_ref, seg_ref, held_ref, v_hbm, bias_ref, table_ref, vt_ref, v_ref, sems):
    copies = []
    for g in range(KVH):
        at = slice(g * HD, (g + 1) * HD)
        copies.append(pltpu.make_async_copy(v_hbm.at[:, at], v_ref.at[:, at], sems.at[g]))
    for copy in copies:
        copy.start()
    lane = lanes((ROWS, 128))
    cosine, sine = rope_tables(pos_ref[...], lane % 64)
    table_ref[0] = cosine
    table_ref[1] = jnp.where(lane < 64, -sine, sine)
    pick = where_one(rows_of((ROWS, 128)) == lane % ROWS)
    kinds = where_one(rows_of((8, ROWS)) == seg_ref[...])
    wanted = dot(kinds, pick, NN).astype(BF16)
    for part in range(4):
        have = where_one(rows_of((8, 128)) == held_ref[part : part + 1, :])
        bias_ref[part * 128 : (part + 1) * 128, :] = (dot(have, wanted, TN) - 1.0) * -HIDDEN
    seen = dot(kinds, wanted, TN) * jnp.where(rows_of((ROWS, 128)) <= lane % ROWS, 1.0, 0.0)
    bias_ref[512:, :] = (seen - 1.0) * -HIDDEN
    for g in range(KVH):
        copies[g].wait()
        vt_ref[g] = v_ref[:, g * HD : (g + 1) * HD].T


def placing(core):
    row, lane = rows_of((128, 256)), lanes((128, 256))
    at = (row // 64) * 64 + core * 32 + row % 32 + ((row // 32) % 2) * 128
    return where_one(lane == at)


def join(own_ref, came_ref, table_ref, q_ref):
    c = lax.axis_index("c")
    near = lanes((1, 8, 128)) < 64

    def halves(ref):
        tiles = ref[...].astype(F32).reshape(64, 2, 8, 128)
        return jnp.where(near, tiles[:, 0], tiles[:, 1]).reshape(512, 128).astype(BF16)

    whole = dot(halves(own_ref), placing(c), NN) + dot(halves(came_ref), placing(1 - c), NN)
    for late in range(2):
        part = whole[:, late * 128 : (late + 1) * 128]
        at = slice(late * 8, (late + 1) * 8)
        cosine, sine = table_ref[0, at, :], table_ref[1, at, :]
        turned = move(part, 64).reshape(64, 8, 128)
        part = (part.reshape(64, 8, 128) * cosine[None] + turned * sine[None]).astype(BF16)
        for n in range(64):
            z, p = (n // 2) % 8, n % 2
            head = (n // 16) * 16 + z * 2 + p
            q_ref[head * 16 + late * 8 : head * 16 + late * 8 + 8, :] = part[n]


FACTOR = LOG2E / HD**0.5


def softened(scores):
    peak = jnp.maximum(jnp.max(scores, axis=0, keepdims=True), NONE)
    high, low = split_pair(peak)
    peak = high + low
    weights = jnp.exp2(scores - peak)
    return weights.astype(BF16), peak, jnp.sum(weights, axis=0, keepdims=True)


def heads_at(base, i):
    return pl.ds(pl.multiple_of((base + i) * 128, 128), 128)


def attend(base, q_ref, k_ref, vt_ref, bias_ref, out_ref):
    for pair in ((0, 1), (2, 3)):
        scores = [
            dot(k_ref[:, heads_at(base, i)], q_ref[heads_at(base, i), :], NT) * FACTOR
            + bias_ref[0:512, :]
            for i in pair
        ]
        parts = [softened(s) for s in scores]
        outs = [dot(vt_ref[base + i], w[0], NN) for i, w in zip(pair, parts)]
        for i, out, (_, peak, total) in zip(pair, outs, parts):
            emit(out_ref, i * 4, out.astype(BF16), state_rows(peak, total))


def emit(out_ref, first, out, state):
    for n in range(4):
        out_ref[first + n, 0:32, :] = out[n * 32 : (n + 1) * 32]
        out_ref[first + n, 32:40, :] = state


def first_body(own_ref, came_ref, table_ref, k_ref, vt_ref, bias_ref, out_ref, q_ref):
    join(own_ref, came_ref, table_ref, q_ref)
    attend((1 - lax.axis_index("c")) * 4, q_ref, k_ref, vt_ref, bias_ref, out_ref)


def second_body(q_ref, k_ref, vt_ref, bias_ref, in_ref, came_ref, table_ref, out_ref):
    c, y = lax.axis_index("c"), lax.axis_index("y")
    attend(c * 4, q_ref, k_ref, vt_ref, bias_ref, out_ref)

    @pl.when((lax.axis_index("z") == 0) & (lax.axis_index("x") == 0))
    def _():
        lane = lanes((8, 128))
        g = c * 4 + y
        start = (g // 2) * 32 + (g % 2) * 16
        found = []
        for kind in range(2):
            parts = []
            for late in range(2):
                value = jnp.zeros((8, 128), F32)
                for n in range(16):
                    own, came = in_ref[start + n].astype(F32), came_ref[start + n].astype(F32)
                    pair = (jnp.where(c == 0, own, came), jnp.where(c == 0, came, own))
                    for core in range(2):
                        at = n * 8 + core * 4
                        held = (1 - n % 2) * 64 + kind * 32 + late * 16
                        value = jnp.where(
                            (lane >= at) & (lane < at + 4), move(pair[core], at - held), value
                        )
                parts.append(value)
            if kind == 0:
                parts = [
                    rotate(v, table_ref[0, n * 8 : n * 8 + 8, :], table_ref[1, n * 8 : n * 8 + 8, :])
                    for n, v in enumerate(parts)
                ]
            found.append(jnp.concatenate(parts, axis=0).astype(BF16))
        scores = dot(found[0], q_ref[heads_at(c * 4, y), :], NT) * FACTOR + bias_ref[512:, :]
        weights, peak, total = softened(scores)
        own = dot(found[1], weights, TN)
        for n in range(4):
            tile = out_ref.at[y * 4 + n]
            out, peaks, totals = merge(
                [tile[0:32, :].astype(F32), own[n * 32 : (n + 1) * 32]],
                *zip(state_of(tile, 32), (peak, total)),
            )
            tile[0:32, :] = out.astype(BF16)
            tile[32:40, :] = state_rows(peaks, totals)


def state_of(ref, at):
    state = ref[at : at + 8, :].astype(F32)
    return state[0:1] + state[1:2], state[2:3] + state[3:4]


def merge(outs, peaks, totals):
    peak = functools.reduce(jnp.maximum, peaks)
    factors = [jnp.exp2(p - peak) for p in peaks]
    out = sum(o * f for o, f in zip(outs, factors))
    return out, peak, sum(t * f for t, f in zip(totals, factors))


def merged(refs, at=0):
    outs = [ref[at : at + 32, :].astype(F32) for ref in refs]
    return merge(outs, *zip(*(state_of(ref, at + 32) for ref in refs)))


def tiles_of(ref):
    return [ref.at[n] for n in range(ref.shape[0])]


def couple_body(own_ref, came_ref, out_ref):
    for n in range(16):
        out, peak, total = merged([own_ref.at[n], came_ref.at[n]])
        out_ref[n, 0:32, :] = out.astype(BF16)
        out_ref[n, 32:40, :] = state_rows(peak, total)


def merge_body(in_ref, out_ref):
    out, peak, total = merged(tiles_of(in_ref))
    out_ref[0:32, :] = out.astype(BF16)
    out_ref[32:40, :] = state_rows(peak, total)


def pair_body(own_ref, came_ref, out_ref):
    first = lax.axis_index("c") == 0
    own, came = own_ref[...].astype(F32), came_ref[...].astype(F32)
    tiles = (jnp.where(first, own, came).astype(BF16), jnp.where(first, came, own).astype(BF16))
    for d in range(out_ref.shape[0]):
        for n, tile in enumerate(tiles):
            out_ref[d, n * 40 : (n + 1) * 40, :] = tile


def finish_body(in_ref, out_ref):
    for n in range(2):
        out, _, total = merged(tiles_of(in_ref), n * 40)
        out = (out / total).astype(BF16)
        for d in range(out_ref.shape[0]):
            out_ref[d, n * 32 : (n + 1) * 32, :] = out


def place_body(in_ref, out_ref):
    eye = where_one(rows_of((128, 128)) == lanes((128, 128)))
    for g in range(KVH):
        half, y = divmod(g, 4)
        block = in_ref[y * 4 : (y + 1) * 4, half * 32 : (half + 1) * 32, :].reshape(128, 128)
        block = dot(eye, block, NT).astype(BF16)
        for i in range(8):
            at = (g * 8 + i) * HD
            out_ref[:, at : at + HD] = block[i * ROWS : (i + 1) * ROWS]


def per_device(
    queries,
    span_keys,
    span_values,
    positions,
    span_segments,
    cache_keys,
    cache_values,
    cache_segments,
):
    shape = jax.ShapeDtypeStruct
    small = (
        queries,
        span_keys.T,
        span_values.T,
        positions,
        span_segments.reshape(1, ROWS),
        cache_segments.reshape(4, 128),
        cache_keys,
    )
    tiles, positions, span_segments, cache_segments, keys = call(
        pack_body,
        "pack",
        (shape((128, 8, 128), BF16), *(shape(a.shape, a.dtype) for a in small[3:])),
        *(pltpu.with_memory_space_constraint(a, pltpu.HBM) for a in small),
        specs=[HBM] * 7,
        scratch=[pltpu.VMEM(a.shape, a.dtype) for a in small[:3]] + [pltpu.SemaphoreType.DMA((7,))],
    )
    tiles = exchange(tiles, CHIPS)
    came = swap(tiles)
    bias, tables, turned_values = call(
        ready_body,
        "ready",
        (
            shape((512 + ROWS, 128), F32),
            shape((2, ROWS, 128), F32),
            shape((KVH, HD, 512), BF16),
        ),
        positions,
        span_segments,
        cache_segments,
        pltpu.with_memory_space_constraint(cache_values, pltpu.HBM),
        specs=[VMEM] * 3 + [HBM],
        scratch=[pltpu.VMEM((512, KVH * HD), BF16), pltpu.SemaphoreType.DMA((KVH,))],
    )
    message = shape((16, 40, 128), BF16)
    parts, q = call(
        first_body,
        "first",
        (message, shape((H * ROWS, HD), BF16)),
        tiles,
        came,
        tables,
        keys,
        turned_values,
        bias,
    )
    other = swap(parts)
    parts = call(
        second_body, "second", message, q, keys, turned_values, bias, tiles, came, tables
    )
    parts = call(couple_body, "couple", message, parts, other)
    parts = exchange(parts, PLANE)
    part = call(merge_body, "merge", shape((40, 128), BF16), parts)
    parts = call(pair_body, "pair", shape((8, 80, 128), BF16), part, swap(part))
    parts = exchange(parts, ("z",))
    whole = call(finish_body, "finish", shape((16, 64, 128), BF16), parts)
    whole = exchange(whole, PLANE)
    return call(place_body, "place", shape((ROWS, H * HD), BF16), whole)


def solution(mesh):
    split = Mesh(mesh.devices.reshape(4, 8, 4, 2), ALL)
    return jax.shard_map(
        per_device,
        mesh=split,
        in_specs=(
            P(None, ALL),
            P(None, ALL),
            P(None, ALL),
            P(),
            P(),
            P(ALL, None),
            P(ALL, None),
            P(ALL),
        ),
        out_specs=P(),
        check_vma=False,
    )
```

```python
import functools

import jax
import jax.numpy as jnp
from jax import lax
from jax.experimental import pallas as pl
from jax.experimental.pallas import tpu as pltpu
from jax.sharding import Mesh
from jax.sharding import PartitionSpec as P

H = 64
KVH = 8
HD = 128
ROWS = 16
ALL = ("y", "z", "x", "c")
CHIPS = ("y", "z", "x")
PLANE = ("y", "x")
LOG2E = 1.4426950408889634
NONE = -1e30
HIDDEN = -2e30
F32 = jnp.float32
BF16 = jnp.bfloat16
VMEM = pl.BlockSpec(memory_space=pltpu.VMEM)
NT = (((1,), (1,)), ((), ()))

HBM = pl.BlockSpec(memory_space=pltpu.HBM)


def call(body, name, out_shape, *args, specs=None, scratch=(), limit=8 << 20):
    return pl.pallas_call(
        body,
        name=name,
        out_shape=out_shape,
        in_specs=specs or [VMEM] * len(args),
        out_specs=jax.tree.map(lambda _: VMEM, out_shape),
        scratch_shapes=scratch,
        compiler_params=pltpu.CompilerParams(vmem_limit_bytes=limit),
    )(*args)


def lanes(shape):
    return lax.broadcasted_iota(jnp.int32, shape, len(shape) - 1)


def move(value, by):
    by %= value.shape[-1]
    return pltpu.roll(value, by, value.ndim - 1) if by else value


def exchange(tiles, axes):
    return lax.all_to_all(tiles, axes, 0, 0, tiled=True)


def swap(value):
    return lax.ppermute(value, "c", ((0, 1), (1, 0)))


def stay(value):
    return lax.ppermute(value, "c", ((0, 0), (1, 1)))


def rows_of(shape):
    return lax.broadcasted_iota(jnp.int32, shape, 0)


TN = (((0,), (0,)), ((), ()))
NN = (((1,), (0,)), ((), ()))


def dot(a, b, dims):
    return lax.dot_general(a, b, dims, preferred_element_type=F32)


def where_one(hit):
    return jnp.where(hit, 1.0, 0.0).astype(BF16)


def pack_body(*refs):
    out_ref, q_ref, k_ref, v_ref, sems = refs[6], *refs[10:]
    copies = [
        pltpu.make_async_copy(source, target, sems.at[n])
        for n, (source, target) in enumerate(zip(refs[:6], (q_ref, k_ref, v_ref, *refs[7:10])))
    ]
    for copy in copies:
        copy.start()
    for copy in copies:
        copy.wait()
    turn = (lax.axis_index("x") % 2) * 64

    def spread(count, at):
        return where_one(lanes((count, 128)) == rows_of((count, 128)) + (at + turn) % 128)

    tile = jnp.zeros((8, 128), F32)
    for late in range(2):
        part = dot(q_ref[...], spread(32, late * 32), NN)
        for ref, at in ((k_ref, 64), (v_ref, 96)):
            part = part + dot(ref[...], spread(4, at + late * 16), TN)
        tile = tile + part[late * 8 : (late + 1) * 8]
    tile = tile.astype(BF16)
    for d in range(out_ref.shape[0]):
        out_ref[d] = tile


def turn(angle):
    quarter = jnp.floor(angle * 0.6366197723675814 + 0.5)
    rest = angle - quarter * 1.5703125
    rest = rest - quarter * 4.837512969970703e-4
    rest = rest - quarter * 7.549789948768648e-8
    square = rest * rest
    sine = -1.9515295891e-4 * square + 8.3321608736e-3
    sine = (sine * square - 1.6666654611e-1) * square * rest + rest
    cosine = 2.443315711809948e-5 * square - 1.388731625493765e-3
    cosine = (cosine * square + 4.166664568298827e-2) * square * square - 0.5 * square + 1.0
    which = quarter.astype(jnp.int32) % 4
    odd = which % 2 == 1
    cosine, sine = jnp.where(odd, sine, cosine), jnp.where(odd, cosine, sine)
    cosine = jnp.where((which == 1) | (which == 2), -cosine, cosine)
    sine = jnp.where(which >= 2, -sine, sine)
    return cosine, sine


def rope_tables(positions, index):
    section = jnp.where(index < 16, 0, jnp.where(index < 40, 1, 2))
    high = positions // 64
    position = jnp.zeros(index.shape, F32)
    for scale, part in ((64.0, high), (1.0, positions - high * 64)):
        chosen = dot(part.astype(F32).astype(BF16), where_one(rows_of((3, 3 * 128)) == lanes((3, 3 * 128)) // 128), TN)
        picked = chosen[:, 256:]
        for n in range(2):
            picked = jnp.where(section == n, chosen[:, n * 128 : (n + 1) * 128], picked)
        position = position + scale * picked
    inverse = jnp.ones(index.shape, F32)
    for bit in range(6):
        step = 1000000.0 ** (-2.0 * 2**bit / HD)
        inverse = jnp.where((index // 2**bit) % 2 == 1, inverse * step, inverse)
    return turn(position * inverse)


def rotate(value, cosine, sine):
    return value * cosine + move(value, 64) * sine


def split_pair(value):
    high = value.astype(BF16).astype(F32)
    return high, (value - high).astype(BF16).astype(F32)


def state_rows(peak, total):
    row = rows_of((8, 128))
    parts = (*split_pair(peak), *split_pair(total))
    tile = jnp.zeros((8, 128), F32)
    for n, part in enumerate(parts):
        tile = jnp.where(row == n, part, tile)
    return tile.astype(BF16)


def ready_body(pos_ref, seg_ref, held_ref, v_ref, bias_ref, table_ref, vt_ref):
    lane = lanes((ROWS, 128))
    cosine, sine = rope_tables(pos_ref[...], lane % 64)
    table_ref[0] = cosine
    table_ref[1] = jnp.where(lane < 64, -sine, sine)
    pick = where_one(rows_of((ROWS, 128)) == lane % ROWS)
    kinds = where_one(rows_of((8, ROWS)) == seg_ref[...])
    wanted = dot(kinds, pick, NN).astype(BF16)
    for part in range(4):
        have = where_one(rows_of((8, 128)) == held_ref[part : part + 1, :])
        bias_ref[part * 128 : (part + 1) * 128, :] = (dot(have, wanted, TN) - 1.0) * -HIDDEN
    seen = dot(kinds, wanted, TN) * jnp.where(rows_of((ROWS, 128)) <= lane % ROWS, 1.0, 0.0)
    bias_ref[512:, :] = (seen - 1.0) * -HIDDEN
    for g in range(KVH):
        vt_ref[g] = v_ref[:, g * HD : (g + 1) * HD].T


def placing(core):
    row, lane = rows_of((128, 256)), lanes((128, 256))
    at = (row // 64) * 64 + core * 32 + row % 32 + ((row // 32) % 2) * 128
    return where_one(lane == at)


def join(own_ref, came_ref, table_ref, q_ref):
    c = lax.axis_index("c")
    near = lanes((1, 8, 128)) < 64

    def halves(ref):
        tiles = ref[...].astype(F32).reshape(64, 2, 8, 128)
        return jnp.where(near, tiles[:, 0], tiles[:, 1]).reshape(512, 128).astype(BF16)

    whole = dot(halves(own_ref), placing(c), NN) + dot(halves(came_ref), placing(1 - c), NN)
    for late in range(2):
        part = whole[:, late * 128 : (late + 1) * 128]
        at = slice(late * 8, (late + 1) * 8)
        cosine, sine = table_ref[0, at, :], table_ref[1, at, :]
        turned = move(part, 64).reshape(64, 8, 128)
        part = (part.reshape(64, 8, 128) * cosine[None] + turned * sine[None]).astype(BF16)
        for n in range(64):
            z, p = (n // 2) % 8, n % 2
            head = (n // 16) * 16 + z * 2 + p
            q_ref[head * 16 + late * 8 : head * 16 + late * 8 + 8, :] = part[n]


FACTOR = LOG2E / HD**0.5


def softened(scores):
    peak = jnp.maximum(jnp.max(scores, axis=0, keepdims=True), NONE)
    high, low = split_pair(peak)
    peak = high + low
    weights = jnp.exp2(scores - peak)
    return weights.astype(BF16), peak, jnp.sum(weights, axis=0, keepdims=True)


def heads_at(base, i):
    return pl.ds(pl.multiple_of((base + i) * 128, 128), 128)


def attend(base, q_ref, k_ref, vt_ref, bias_ref, out_ref):
    for pair in ((0, 1), (2, 3)):
        scores = [
            dot(k_ref[:, heads_at(base, i)], q_ref[heads_at(base, i), :], NT) * FACTOR
            + bias_ref[0:512, :]
            for i in pair
        ]
        parts = [softened(s) for s in scores]
        outs = [dot(vt_ref[base + i], w[0], NN) for i, w in zip(pair, parts)]
        for i, out, (_, peak, total) in zip(pair, outs, parts):
            emit(out_ref, i * 4, out.astype(BF16), state_rows(peak, total))


def emit(out_ref, first, out, state):
    for n in range(4):
        out_ref[first + n, 0:32, :] = out[n * 32 : (n + 1) * 32]
        out_ref[first + n, 32:40, :] = state


def first_body(own_ref, came_ref, table_ref, k_ref, vt_ref, bias_ref, out_ref, q_ref):
    join(own_ref, came_ref, table_ref, q_ref)
    attend((1 - lax.axis_index("c")) * 4, q_ref, k_ref, vt_ref, bias_ref, out_ref)


def second_body(q_ref, k_ref, vt_ref, bias_ref, in_ref, came_ref, table_ref, out_ref):
    c, y = lax.axis_index("c"), lax.axis_index("y")
    attend(c * 4, q_ref, k_ref, vt_ref, bias_ref, out_ref)

    @pl.when((lax.axis_index("z") == 0) & (lax.axis_index("x") == 0))
    def _():
        lane = lanes((8, 128))
        g = c * 4 + y
        start = (g // 2) * 32 + (g % 2) * 16
        found = []
        for kind in range(2):
            parts = []
            for late in range(2):
                value = jnp.zeros((8, 128), F32)
                for n in range(16):
                    own, came = in_ref[start + n].astype(F32), came_ref[start + n].astype(F32)
                    pair = (jnp.where(c == 0, own, came), jnp.where(c == 0, came, own))
                    for core in range(2):
                        at = n * 8 + core * 4
                        held = (1 - n % 2) * 64 + kind * 32 + late * 16
                        value = jnp.where(
                            (lane >= at) & (lane < at + 4), move(pair[core], at - held), value
                        )
                parts.append(value)
            if kind == 0:
                parts = [
                    rotate(v, table_ref[0, n * 8 : n * 8 + 8, :], table_ref[1, n * 8 : n * 8 + 8, :])
                    for n, v in enumerate(parts)
                ]
            found.append(jnp.concatenate(parts, axis=0).astype(BF16))
        scores = dot(found[0], q_ref[heads_at(c * 4, y), :], NT) * FACTOR + bias_ref[512:, :]
        weights, peak, total = softened(scores)
        own = dot(found[1], weights, TN)
        for n in range(4):
            tile = out_ref.at[y * 4 + n]
            out, peaks, totals = merge(
                [tile[0:32, :].astype(F32), own[n * 32 : (n + 1) * 32]],
                *zip(state_of(tile), (peak, total)),
            )
            tile[0:32, :] = out.astype(BF16)
            tile[32:40, :] = state_rows(peaks, totals)


def state_of(ref):
    state = ref[32:40, :].astype(F32)
    return state[0:1] + state[1:2], state[2:3] + state[3:4]


def merge(outs, peaks, totals):
    peak = functools.reduce(jnp.maximum, peaks)
    factors = [jnp.exp2(p - peak) for p in peaks]
    out = sum(o * f for o, f in zip(outs, factors))
    return out, peak, sum(t * f for t, f in zip(totals, factors))


def merged(refs):
    outs = [ref[0:32, :].astype(F32) for ref in refs]
    return merge(outs, *zip(*map(state_of, refs)))


def tiles_of(ref):
    return [ref.at[n] for n in range(ref.shape[0])]


def couple_body(own_ref, came_ref, out_ref):
    for n in range(16):
        out, peak, total = merged([own_ref.at[n], came_ref.at[n]])
        out_ref[n, 0:32, :] = out.astype(BF16)
        out_ref[n, 32:40, :] = state_rows(peak, total)


def merge_body(in_ref, out_ref):
    out, peak, total = merged(tiles_of(in_ref))
    out, state = out.astype(BF16), state_rows(peak, total)
    for d in range(out_ref.shape[0]):
        out_ref[d, 0:32, :] = out
        out_ref[d, 32:40, :] = state


def finish_body(in_ref, out_ref):
    out, _, total = merged(tiles_of(in_ref))
    out_ref[...] = (out / total).astype(BF16)


def pair_body(own_ref, came_ref, out_ref):
    first = lax.axis_index("c") == 0
    own, came = own_ref[...].astype(F32), came_ref[...].astype(F32)
    tiles = (jnp.where(first, own, came).astype(BF16), jnp.where(first, came, own).astype(BF16))
    for d in range(out_ref.shape[0]):
        for n, tile in enumerate(tiles):
            out_ref[d, n * 32 : (n + 1) * 32, :] = tile


def place_body(in_ref, out_ref):
    eye = where_one(rows_of((128, 128)) == lanes((128, 128)))
    for g in range(KVH):
        half, y = divmod(g, 4)
        block = in_ref[y * 4 : (y + 1) * 4, half * 32 : (half + 1) * 32, :].reshape(128, 128)
        block = dot(eye, block, NT).astype(BF16)
        for i in range(8):
            at = (g * 8 + i) * HD
            out_ref[:, at : at + HD] = block[i * ROWS : (i + 1) * ROWS]


def per_device(
    queries,
    span_keys,
    span_values,
    positions,
    span_segments,
    cache_keys,
    cache_values,
    cache_segments,
):
    shape = jax.ShapeDtypeStruct
    small = (
        queries,
        span_keys.T,
        span_values.T,
        positions,
        span_segments.reshape(1, ROWS),
        cache_segments.reshape(4, 128),
    )
    tiles, positions, span_segments, cache_segments = call(
        pack_body,
        "pack",
        (shape((128, 8, 128), BF16), *(shape(a.shape, a.dtype) for a in small[3:])),
        *(pltpu.with_memory_space_constraint(a, pltpu.HBM) for a in small),
        specs=[HBM] * 6,
        scratch=[pltpu.VMEM(a.shape, a.dtype) for a in small[:3]] + [pltpu.SemaphoreType.DMA((6,))],
    )
    keys, values = stay(cache_keys), stay(cache_values)
    tiles, keys, values = lax.optimization_barrier((exchange(tiles, CHIPS), keys, values))
    came = swap(tiles)
    bias, tables, turned_values = call(
        ready_body,
        "ready",
        (
            shape((512 + ROWS, 128), F32),
            shape((2, ROWS, 128), F32),
            shape((KVH, HD, 512), BF16),
        ),
        positions,
        span_segments,
        cache_segments,
        values,
    )
    message = shape((16, 40, 128), BF16)
    parts, q = call(
        first_body,
        "first",
        (message, shape((H * ROWS, HD), BF16)),
        tiles,
        came,
        tables,
        keys,
        turned_values,
        bias,
    )
    other = swap(parts)
    parts = call(
        second_body, "second", message, q, keys, turned_values, bias, tiles, came, tables
    )
    parts = call(couple_body, "couple", message, parts, other)
    parts = exchange(parts, PLANE)
    parts = call(merge_body, "merge", shape((8, 40, 128), BF16), parts)
    parts = exchange(parts, ("z",))
    tile = call(finish_body, "finish", shape((32, 128), BF16), parts)
    whole = call(pair_body, "pair", shape((16, 64, 128), BF16), tile, swap(tile))
    whole = exchange(whole, PLANE)
    return call(place_body, "place", shape((ROWS, H * HD), BF16), whole)


def solution(mesh):
    split = Mesh(mesh.devices.reshape(4, 8, 4, 2), ALL)
    return jax.shard_map(
        per_device,
        mesh=split,
        in_specs=(
            P(None, ALL),
            P(None, ALL),
            P(None, ALL),
            P(),
            P(),
            P(ALL, None),
            P(ALL, None),
            P(ALL),
        ),
        out_specs=P(),
        check_vma=False,
    )
```

```python
import functools

import jax
import jax.numpy as jnp
from jax import lax
from jax.experimental import pallas as pl
from jax.experimental.pallas import tpu as pltpu
from jax.sharding import Mesh
from jax.sharding import PartitionSpec as P

H = 64
KVH = 8
HD = 128
ROWS = 16
ALL = ("y", "z", "x", "c")
CHIPS = ("y", "z", "x")
PLANE = ("y", "x")
LOG2E = 1.4426950408889634
NONE = -1e30
HIDDEN = -2e30
F32 = jnp.float32
BF16 = jnp.bfloat16
VMEM = pl.BlockSpec(memory_space=pltpu.VMEM)
NT = (((1,), (1,)), ((), ()))

HBM = pl.BlockSpec(memory_space=pltpu.HBM)


def call(body, name, out_shape, *args, specs=None, scratch=(), limit=8 << 20, out_specs=None):
    return pl.pallas_call(
        body,
        name=name,
        out_shape=out_shape,
        in_specs=specs or [VMEM] * len(args),
        out_specs=out_specs or jax.tree.map(lambda _: VMEM, out_shape),
        scratch_shapes=scratch,
        compiler_params=pltpu.CompilerParams(vmem_limit_bytes=limit),
    )(*args)


def lanes(shape):
    return lax.broadcasted_iota(jnp.int32, shape, len(shape) - 1)


def move(value, by):
    by %= value.shape[-1]
    return pltpu.roll(value, by, value.ndim - 1) if by else value


def exchange(tiles, axes):
    return lax.all_to_all(tiles, axes, 0, 0, tiled=True)


def swap(value):
    return lax.ppermute(value, "c", ((0, 1), (1, 0)))


def rows_of(shape):
    return lax.broadcasted_iota(jnp.int32, shape, 0)


TN = (((0,), (0,)), ((), ()))
NN = (((1,), (0,)), ((), ()))


def dot(a, b, dims):
    return lax.dot_general(a, b, dims, preferred_element_type=F32)


def where_one(hit):
    return jnp.where(hit, 1.0, 0.0).astype(BF16)


def pack_body(*refs):
    out_ref, q_ref, k_ref, v_ref, sems = refs[6], *refs[10:]
    copies = [
        pltpu.make_async_copy(source, target, sems.at[n])
        for n, (source, target) in enumerate(zip(refs[:6], (q_ref, k_ref, v_ref, *refs[7:10])))
    ]
    for copy in copies:
        copy.start()
    for copy in copies:
        copy.wait()
    turn = (lax.axis_index("x") % 2) * 64

    def spread(count, at):
        return where_one(lanes((count, 128)) == rows_of((count, 128)) + (at + turn) % 128)

    tile = jnp.zeros((8, 128), F32)
    for late in range(2):
        part = dot(q_ref[...], spread(32, late * 32), NN)
        for ref, at in ((k_ref, 64), (v_ref, 96)):
            part = part + dot(ref[...], spread(4, at + late * 16), TN)
        tile = tile + part[late * 8 : (late + 1) * 8]
    tile = tile.astype(BF16)
    for d in range(out_ref.shape[0]):
        out_ref[d] = tile


def turn(angle):
    quarter = jnp.floor(angle * 0.6366197723675814 + 0.5)
    rest = angle - quarter * 1.5703125
    rest = rest - quarter * 4.837512969970703e-4
    rest = rest - quarter * 7.549789948768648e-8
    square = rest * rest
    sine = -1.9515295891e-4 * square + 8.3321608736e-3
    sine = (sine * square - 1.6666654611e-1) * square * rest + rest
    cosine = 2.443315711809948e-5 * square - 1.388731625493765e-3
    cosine = (cosine * square + 4.166664568298827e-2) * square * square - 0.5 * square + 1.0
    which = quarter.astype(jnp.int32) % 4
    odd = which % 2 == 1
    cosine, sine = jnp.where(odd, sine, cosine), jnp.where(odd, cosine, sine)
    cosine = jnp.where((which == 1) | (which == 2), -cosine, cosine)
    sine = jnp.where(which >= 2, -sine, sine)
    return cosine, sine


def rope_tables(positions, index):
    section = jnp.where(index < 16, 0, jnp.where(index < 40, 1, 2))
    high = positions // 64
    position = jnp.zeros(index.shape, F32)
    for scale, part in ((64.0, high), (1.0, positions - high * 64)):
        chosen = dot(part.astype(F32).astype(BF16), where_one(rows_of((3, 3 * 128)) == lanes((3, 3 * 128)) // 128), TN)
        picked = chosen[:, 256:]
        for n in range(2):
            picked = jnp.where(section == n, chosen[:, n * 128 : (n + 1) * 128], picked)
        position = position + scale * picked
    inverse = jnp.ones(index.shape, F32)
    for bit in range(6):
        step = 1000000.0 ** (-2.0 * 2**bit / HD)
        inverse = jnp.where((index // 2**bit) % 2 == 1, inverse * step, inverse)
    return turn(position * inverse)


def rotate(value, cosine, sine):
    return value * cosine + move(value, 64) * sine


def split_pair(value):
    high = value.astype(BF16).astype(F32)
    return high, (value - high).astype(BF16).astype(F32)


def state_rows(peak, total):
    row = rows_of((8, 128))
    parts = (*split_pair(peak), *split_pair(total))
    tile = jnp.zeros((8, 128), F32)
    for n, part in enumerate(parts):
        tile = jnp.where(row == n, part, tile)
    return tile.astype(BF16)


def ready_body(pos_ref, seg_ref, held_ref, k_hbm, v_hbm, bias_ref, table_ref, k_ref, vt_ref, v_ref, sems):
    copies = [
        pltpu.make_async_copy(source, target, sems.at[n])
        for n, (source, target) in enumerate(((v_hbm, v_ref), (k_hbm, k_ref)))
    ]
    for copy in copies:
        copy.start()
    lane = lanes((ROWS, 128))
    cosine, sine = rope_tables(pos_ref[...], lane % 64)
    table_ref[0] = cosine
    table_ref[1] = jnp.where(lane < 64, -sine, sine)
    pick = where_one(rows_of((ROWS, 128)) == lane % ROWS)
    kinds = where_one(rows_of((8, ROWS)) == seg_ref[...])
    wanted = dot(kinds, pick, NN).astype(BF16)
    for part in range(4):
        have = where_one(rows_of((8, 128)) == held_ref[part : part + 1, :])
        bias_ref[part * 128 : (part + 1) * 128, :] = (dot(have, wanted, TN) - 1.0) * -HIDDEN
    seen = dot(kinds, wanted, TN) * jnp.where(rows_of((ROWS, 128)) <= lane % ROWS, 1.0, 0.0)
    bias_ref[512:, :] = (seen - 1.0) * -HIDDEN
    copies[0].wait()
    for g in range(KVH):
        vt_ref[g] = v_ref[:, g * HD : (g + 1) * HD].T
    copies[1].wait()


def placing(core):
    row, lane = rows_of((128, 256)), lanes((128, 256))
    at = (row // 64) * 64 + core * 32 + row % 32 + ((row // 32) % 2) * 128
    return where_one(lane == at)


def join(own_ref, came_ref, table_ref, q_ref):
    c = lax.axis_index("c")
    near = lanes((1, 8, 128)) < 64

    def halves(ref):
        tiles = ref[...].astype(F32).reshape(64, 2, 8, 128)
        return jnp.where(near, tiles[:, 0], tiles[:, 1]).reshape(512, 128).astype(BF16)

    whole = dot(halves(own_ref), placing(c), NN) + dot(halves(came_ref), placing(1 - c), NN)
    for late in range(2):
        part = whole[:, late * 128 : (late + 1) * 128]
        at = slice(late * 8, (late + 1) * 8)
        cosine, sine = table_ref[0, at, :], table_ref[1, at, :]
        turned = move(part, 64).reshape(64, 8, 128)
        part = (part.reshape(64, 8, 128) * cosine[None] + turned * sine[None]).astype(BF16)
        for n in range(64):
            z, p = (n // 2) % 8, n % 2
            head = (n // 16) * 16 + z * 2 + p
            q_ref[head * 16 + late * 8 : head * 16 + late * 8 + 8, :] = part[n]


FACTOR = LOG2E / HD**0.5


def softened(scores):
    peak = jnp.maximum(jnp.max(scores, axis=0, keepdims=True), NONE)
    high, low = split_pair(peak)
    peak = high + low
    weights = jnp.exp2(scores - peak)
    return weights.astype(BF16), peak, jnp.sum(weights, axis=0, keepdims=True)


def heads_at(base, i):
    return pl.ds(pl.multiple_of((base + i) * 128, 128), 128)


def attend(base, q_ref, k_ref, vt_ref, bias_ref, out_ref):
    for pair in ((0, 1), (2, 3)):
        scores = [
            dot(k_ref[:, heads_at(base, i)], q_ref[heads_at(base, i), :], NT) * FACTOR
            + bias_ref[0:512, :]
            for i in pair
        ]
        parts = [softened(s) for s in scores]
        outs = [dot(vt_ref[base + i], w[0], NN) for i, w in zip(pair, parts)]
        for i, out, (_, peak, total) in zip(pair, outs, parts):
            emit(out_ref, i * 4, out.astype(BF16), state_rows(peak, total))


def emit(out_ref, first, out, state):
    for n in range(4):
        out_ref[first + n, 0:32, :] = out[n * 32 : (n + 1) * 32]
        out_ref[first + n, 32:40, :] = state


def first_body(own_ref, came_ref, table_ref, k_ref, vt_ref, bias_ref, out_ref, q_ref):
    join(own_ref, came_ref, table_ref, q_ref)
    attend((1 - lax.axis_index("c")) * 4, q_ref, k_ref, vt_ref, bias_ref, out_ref)


def second_body(q_ref, k_ref, vt_ref, bias_ref, in_ref, came_ref, table_ref, out_ref):
    c, y = lax.axis_index("c"), lax.axis_index("y")
    attend(c * 4, q_ref, k_ref, vt_ref, bias_ref, out_ref)

    @pl.when((lax.axis_index("z") == 0) & (lax.axis_index("x") == 0))
    def _():
        lane = lanes((8, 128))
        g = c * 4 + y
        start = (g // 2) * 32 + (g % 2) * 16
        found = []
        for kind in range(2):
            parts = []
            for late in range(2):
                value = jnp.zeros((8, 128), F32)
                for n in range(16):
                    own, came = in_ref[start + n].astype(F32), came_ref[start + n].astype(F32)
                    pair = (jnp.where(c == 0, own, came), jnp.where(c == 0, came, own))
                    for core in range(2):
                        at = n * 8 + core * 4
                        held = (1 - n % 2) * 64 + kind * 32 + late * 16
                        value = jnp.where(
                            (lane >= at) & (lane < at + 4), move(pair[core], at - held), value
                        )
                parts.append(value)
            if kind == 0:
                parts = [
                    rotate(v, table_ref[0, n * 8 : n * 8 + 8, :], table_ref[1, n * 8 : n * 8 + 8, :])
                    for n, v in enumerate(parts)
                ]
            found.append(jnp.concatenate(parts, axis=0).astype(BF16))
        scores = dot(found[0], q_ref[heads_at(c * 4, y), :], NT) * FACTOR + bias_ref[512:, :]
        weights, peak, total = softened(scores)
        own = dot(found[1], weights, TN)
        for n in range(4):
            tile = out_ref.at[y * 4 + n]
            out, peaks, totals = merge(
                [tile[0:32, :].astype(F32), own[n * 32 : (n + 1) * 32]],
                *zip(state_of(tile), (peak, total)),
            )
            tile[0:32, :] = out.astype(BF16)
            tile[32:40, :] = state_rows(peaks, totals)


def state_of(ref):
    state = ref[32:40, :].astype(F32)
    return state[0:1] + state[1:2], state[2:3] + state[3:4]


def merge(outs, peaks, totals):
    peak = functools.reduce(jnp.maximum, peaks)
    factors = [jnp.exp2(p - peak) for p in peaks]
    out = sum(o * f for o, f in zip(outs, factors))
    return out, peak, sum(t * f for t, f in zip(totals, factors))


def merged(refs):
    outs = [ref[0:32, :].astype(F32) for ref in refs]
    return merge(outs, *zip(*map(state_of, refs)))


def tiles_of(ref):
    return [ref.at[n] for n in range(ref.shape[0])]


def couple_body(own_ref, came_ref, out_ref):
    for n in range(16):
        out, peak, total = merged([own_ref.at[n], came_ref.at[n]])
        out_ref[n, 0:32, :] = out.astype(BF16)
        out_ref[n, 32:40, :] = state_rows(peak, total)


def merge_body(in_ref, out_ref):
    out, peak, total = merged(tiles_of(in_ref))
    out, state = out.astype(BF16), state_rows(peak, total)
    for d in range(out_ref.shape[0]):
        out_ref[d, 0:32, :] = out
        out_ref[d, 32:40, :] = state


def finish_body(in_ref, out_ref):
    out, _, total = merged(tiles_of(in_ref))
    out_ref[...] = (out / total).astype(BF16)


def pair_body(own_ref, came_ref, out_ref):
    first = lax.axis_index("c") == 0
    own, came = own_ref[...].astype(F32), came_ref[...].astype(F32)
    tiles = (jnp.where(first, own, came).astype(BF16), jnp.where(first, came, own).astype(BF16))
    for d in range(out_ref.shape[0]):
        for n, tile in enumerate(tiles):
            out_ref[d, n * 32 : (n + 1) * 32, :] = tile


def place_body(in_ref, out_hbm, out_ref, sems):
    copies = []
    eye = where_one(rows_of((128, 128)) == lanes((128, 128)))
    for g in range(KVH):
        half, y = divmod(g, 4)
        block = in_ref[y * 4 : (y + 1) * 4, half * 32 : (half + 1) * 32, :].reshape(128, 128)
        block = dot(eye, block, NT).astype(BF16)
        for i in range(8):
            at = (g * 8 + i) * HD
            out_ref[:, at : at + HD] = block[i * ROWS : (i + 1) * ROWS]
        if g % 2:
            part = slice((g - 1) * 8 * HD, (g + 1) * 8 * HD)
            copies.append(
                pltpu.make_async_copy(out_ref.at[:, part], out_hbm.at[:, part], sems.at[g // 2])
            )
            copies[-1].start()
    for copy in copies:
        copy.wait()


def per_device(
    queries,
    span_keys,
    span_values,
    positions,
    span_segments,
    cache_keys,
    cache_values,
    cache_segments,
):
    shape = jax.ShapeDtypeStruct
    small = (
        queries,
        span_keys.T,
        span_values.T,
        positions,
        span_segments.reshape(1, ROWS),
        cache_segments.reshape(4, 128),
    )
    tiles, positions, span_segments, cache_segments = call(
        pack_body,
        "pack",
        (shape((128, 8, 128), BF16), *(shape(a.shape, a.dtype) for a in small[3:])),
        *(pltpu.with_memory_space_constraint(a, pltpu.HBM) for a in small),
        specs=[HBM] * 6,
        scratch=[pltpu.VMEM(a.shape, a.dtype) for a in small[:3]] + [pltpu.SemaphoreType.DMA((6,))],
    )
    tiles = exchange(tiles, CHIPS)
    came = swap(tiles)
    bias, tables, keys, turned_values = call(
        ready_body,
        "ready",
        (
            shape((512 + ROWS, 128), F32),
            shape((2, ROWS, 128), F32),
            shape((512, KVH * HD), BF16),
            shape((KVH, HD, 512), BF16),
        ),
        positions,
        span_segments,
        cache_segments,
        *(pltpu.with_memory_space_constraint(a, pltpu.HBM) for a in (cache_keys, cache_values)),
        specs=[VMEM] * 3 + [HBM] * 2,
        scratch=[pltpu.VMEM((512, KVH * HD), BF16), pltpu.SemaphoreType.DMA((2,))],
    )
    message = shape((16, 40, 128), BF16)
    parts, q = call(
        first_body,
        "first",
        (message, shape((H * ROWS, HD), BF16)),
        tiles,
        came,
        tables,
        keys,
        turned_values,
        bias,
    )
    other = swap(parts)
    parts = call(
        second_body, "second", message, q, keys, turned_values, bias, tiles, came, tables
    )
    parts = call(couple_body, "couple", message, parts, other)
    parts = exchange(parts, PLANE)
    parts = call(merge_body, "merge", shape((8, 40, 128), BF16), parts)
    parts = exchange(parts, ("z",))
    tile = call(finish_body, "finish", shape((32, 128), BF16), parts)
    whole = call(pair_body, "pair", shape((16, 64, 128), BF16), tile, swap(tile))
    whole = exchange(whole, PLANE)
    return call(
        place_body,
        "place",
        shape((ROWS, H * HD), BF16),
        whole,
        scratch=[pltpu.VMEM((ROWS, H * HD), BF16), pltpu.SemaphoreType.DMA((4,))],
        out_specs=HBM,
    )


def solution(mesh):
    split = Mesh(mesh.devices.reshape(4, 8, 4, 2), ALL)
    return jax.shard_map(
        per_device,
        mesh=split,
        in_specs=(
            P(None, ALL),
            P(None, ALL),
            P(None, ALL),
            P(),
            P(),
            P(ALL, None),
            P(ALL, None),
            P(ALL),
        ),
        out_specs=P(),
        check_vma=False,
    )
```

```python
import functools

import jax
import jax.numpy as jnp
from jax import lax
from jax.experimental import pallas as pl
from jax.experimental.pallas import tpu as pltpu
from jax.sharding import Mesh
from jax.sharding import PartitionSpec as P

H = 64
KVH = 8
HD = 128
ROWS = 16
ALL = ("y", "z", "x", "c")
CHIPS = ("y", "z", "x")
PLANE = ("y", "x")
LOG2E = 1.4426950408889634
NONE = -1e30
HIDDEN = -2e30
F32 = jnp.float32
BF16 = jnp.bfloat16
VMEM = pl.BlockSpec(memory_space=pltpu.VMEM)
NT = (((1,), (1,)), ((), ()))

HBM = pl.BlockSpec(memory_space=pltpu.HBM)


def call(body, name, out_shape, *args, specs=None, scratch=(), limit=8 << 20, out_specs=None):
    return pl.pallas_call(
        body,
        name=name,
        out_shape=out_shape,
        in_specs=specs or [VMEM] * len(args),
        out_specs=out_specs or jax.tree.map(lambda _: VMEM, out_shape),
        scratch_shapes=scratch,
        compiler_params=pltpu.CompilerParams(vmem_limit_bytes=limit),
    )(*args)


def lanes(shape):
    return lax.broadcasted_iota(jnp.int32, shape, len(shape) - 1)


def move(value, by):
    by %= value.shape[-1]
    return pltpu.roll(value, by, value.ndim - 1) if by else value


def exchange(tiles, axes):
    return lax.all_to_all(tiles, axes, 0, 0, tiled=True)


def swap(value):
    return lax.ppermute(value, "c", ((0, 1), (1, 0)))


def rows_of(shape):
    return lax.broadcasted_iota(jnp.int32, shape, 0)


TN = (((0,), (0,)), ((), ()))
NN = (((1,), (0,)), ((), ()))


def dot(a, b, dims):
    return lax.dot_general(a, b, dims, preferred_element_type=F32)


def where_one(hit):
    return jnp.where(hit, 1.0, 0.0).astype(BF16)


def pack_body(*refs):
    out_ref, q_ref, k_ref, v_ref, sems = refs[6], *refs[10:]
    copies = [
        pltpu.make_async_copy(source, target, sems.at[n])
        for n, (source, target) in enumerate(zip(refs[:6], (q_ref, k_ref, v_ref, *refs[7:10])))
    ]
    for copy in copies:
        copy.start()
    for copy in copies:
        copy.wait()
    turn = (lax.axis_index("x") % 2) * 64

    def spread(count, at):
        return where_one(lanes((count, 128)) == rows_of((count, 128)) + (at + turn) % 128)

    tile = jnp.zeros((8, 128), F32)
    for late in range(2):
        part = dot(q_ref[...], spread(32, late * 32), NN)
        for ref, at in ((k_ref, 64), (v_ref, 96)):
            part = part + dot(ref[...], spread(4, at + late * 16), TN)
        tile = tile + part[late * 8 : (late + 1) * 8]
    tile = tile.astype(BF16)
    for d in range(out_ref.shape[0]):
        out_ref[d] = tile


def turn(angle):
    quarter = jnp.floor(angle * 0.6366197723675814 + 0.5)
    rest = angle - quarter * 1.5703125
    rest = rest - quarter * 4.837512969970703e-4
    rest = rest - quarter * 7.549789948768648e-8
    square = rest * rest
    sine = -1.9515295891e-4 * square + 8.3321608736e-3
    sine = (sine * square - 1.6666654611e-1) * square * rest + rest
    cosine = 2.443315711809948e-5 * square - 1.388731625493765e-3
    cosine = (cosine * square + 4.166664568298827e-2) * square * square - 0.5 * square + 1.0
    which = quarter.astype(jnp.int32) % 4
    odd = which % 2 == 1
    cosine, sine = jnp.where(odd, sine, cosine), jnp.where(odd, cosine, sine)
    cosine = jnp.where((which == 1) | (which == 2), -cosine, cosine)
    sine = jnp.where(which >= 2, -sine, sine)
    return cosine, sine


def rope_tables(positions, index):
    section = jnp.where(index < 16, 0, jnp.where(index < 40, 1, 2))
    high = positions // 64
    position = jnp.zeros(index.shape, F32)
    for scale, part in ((64.0, high), (1.0, positions - high * 64)):
        chosen = dot(part.astype(F32).astype(BF16), where_one(rows_of((3, 3 * 128)) == lanes((3, 3 * 128)) // 128), TN)
        picked = chosen[:, 256:]
        for n in range(2):
            picked = jnp.where(section == n, chosen[:, n * 128 : (n + 1) * 128], picked)
        position = position + scale * picked
    inverse = jnp.ones(index.shape, F32)
    for bit in range(6):
        step = 1000000.0 ** (-2.0 * 2**bit / HD)
        inverse = jnp.where((index // 2**bit) % 2 == 1, inverse * step, inverse)
    return turn(position * inverse)


def rotate(value, cosine, sine):
    return value * cosine + move(value, 64) * sine


def split_pair(value):
    high = value.astype(BF16).astype(F32)
    return high, (value - high).astype(BF16).astype(F32)


def state_rows(peak, total):
    row = rows_of((8, 128))
    parts = (*split_pair(peak), *split_pair(total))
    tile = jnp.zeros((8, 128), F32)
    for n, part in enumerate(parts):
        tile = jnp.where(row == n, part, tile)
    return tile.astype(BF16)


def ready_body(pos_ref, seg_ref, held_ref, v_hbm, bias_ref, table_ref, vt_ref, v_ref, sem):
    copy = pltpu.make_async_copy(v_hbm, v_ref, sem)
    copy.start()
    lane = lanes((ROWS, 128))
    cosine, sine = rope_tables(pos_ref[...], lane % 64)
    table_ref[0] = cosine
    table_ref[1] = jnp.where(lane < 64, -sine, sine)
    pick = where_one(rows_of((ROWS, 128)) == lane % ROWS)
    kinds = where_one(rows_of((8, ROWS)) == seg_ref[...])
    wanted = dot(kinds, pick, NN).astype(BF16)
    for part in range(4):
        have = where_one(rows_of((8, 128)) == held_ref[part : part + 1, :])
        bias_ref[part * 128 : (part + 1) * 128, :] = (dot(have, wanted, TN) - 1.0) * -HIDDEN
    seen = dot(kinds, wanted, TN) * jnp.where(rows_of((ROWS, 128)) <= lane % ROWS, 1.0, 0.0)
    bias_ref[512:, :] = (seen - 1.0) * -HIDDEN
    copy.wait()
    for g in range(KVH):
        vt_ref[g] = v_ref[:, g * HD : (g + 1) * HD].T


def placing(core):
    row, lane = rows_of((128, 256)), lanes((128, 256))
    at = (row // 64) * 64 + core * 32 + row % 32 + ((row // 32) % 2) * 128
    return where_one(lane == at)


def join(own_ref, came_ref, table_ref, q_ref):
    c = lax.axis_index("c")
    near = lanes((1, 8, 128)) < 64

    def halves(ref):
        tiles = ref[...].astype(F32).reshape(64, 2, 8, 128)
        return jnp.where(near, tiles[:, 0], tiles[:, 1]).reshape(512, 128).astype(BF16)

    whole = dot(halves(own_ref), placing(c), NN) + dot(halves(came_ref), placing(1 - c), NN)
    for late in range(2):
        part = whole[:, late * 128 : (late + 1) * 128]
        at = slice(late * 8, (late + 1) * 8)
        cosine, sine = table_ref[0, at, :], table_ref[1, at, :]
        turned = move(part, 64).reshape(64, 8, 128)
        part = (part.reshape(64, 8, 128) * cosine[None] + turned * sine[None]).astype(BF16)
        for n in range(64):
            z, p = (n // 2) % 8, n % 2
            head = (n // 16) * 16 + z * 2 + p
            q_ref[head * 16 + late * 8 : head * 16 + late * 8 + 8, :] = part[n]


FACTOR = LOG2E / HD**0.5


def softened(scores):
    peak = jnp.maximum(jnp.max(scores, axis=0, keepdims=True), NONE)
    high, low = split_pair(peak)
    peak = high + low
    weights = jnp.exp2(scores - peak)
    return weights.astype(BF16), peak, jnp.sum(weights, axis=0, keepdims=True)


def heads_at(base, i):
    return pl.ds(pl.multiple_of((base + i) * 128, 128), 128)


def attend(base, q_ref, k_ref, vt_ref, bias_ref, out_ref):
    scores = [
        dot(k_ref[:, heads_at(base, i)], q_ref[heads_at(base, i), :], NT) * FACTOR
        + bias_ref[0:512, :]
        for i in range(4)
    ]
    parts = [softened(s) for s in scores]
    outs = [dot(vt_ref[base + i], parts[i][0], NN) for i in range(4)]
    for i, (_, peak, total) in enumerate(parts):
        emit(out_ref, i * 4, outs[i].astype(BF16), state_rows(peak, total))


def emit(out_ref, first, out, state):
    for n in range(4):
        out_ref[first + n, 0:32, :] = out[n * 32 : (n + 1) * 32]
        out_ref[first + n, 32:40, :] = state


def first_body(own_ref, came_ref, table_ref, k_ref, vt_ref, bias_ref, out_ref, q_ref):
    join(own_ref, came_ref, table_ref, q_ref)
    attend((1 - lax.axis_index("c")) * 4, q_ref, k_ref, vt_ref, bias_ref, out_ref)


def second_body(q_ref, k_ref, vt_ref, bias_ref, in_ref, came_ref, table_ref, out_ref):
    c, y = lax.axis_index("c"), lax.axis_index("y")
    attend(c * 4, q_ref, k_ref, vt_ref, bias_ref, out_ref)

    @pl.when((lax.axis_index("z") == 0) & (lax.axis_index("x") == 0))
    def _():
        lane = lanes((8, 128))
        g = c * 4 + y
        start = (g // 2) * 32 + (g % 2) * 16
        found = []
        for kind in range(2):
            parts = []
            for late in range(2):
                value = jnp.zeros((8, 128), F32)
                for n in range(16):
                    own, came = in_ref[start + n].astype(F32), came_ref[start + n].astype(F32)
                    pair = (jnp.where(c == 0, own, came), jnp.where(c == 0, came, own))
                    for core in range(2):
                        at = n * 8 + core * 4
                        held = (1 - n % 2) * 64 + kind * 32 + late * 16
                        value = jnp.where(
                            (lane >= at) & (lane < at + 4), move(pair[core], at - held), value
                        )
                parts.append(value)
            if kind == 0:
                parts = [
                    rotate(v, table_ref[0, n * 8 : n * 8 + 8, :], table_ref[1, n * 8 : n * 8 + 8, :])
                    for n, v in enumerate(parts)
                ]
            found.append(jnp.concatenate(parts, axis=0).astype(BF16))
        scores = dot(found[0], q_ref[heads_at(c * 4, y), :], NT) * FACTOR + bias_ref[512:, :]
        weights, peak, total = softened(scores)
        own = dot(found[1], weights, TN)
        for n in range(4):
            tile = out_ref.at[y * 4 + n]
            out, peaks, totals = merge(
                [tile[0:32, :].astype(F32), own[n * 32 : (n + 1) * 32]],
                *zip(state_of(tile), (peak, total)),
            )
            tile[0:32, :] = out.astype(BF16)
            tile[32:40, :] = state_rows(peaks, totals)


def state_of(ref):
    state = ref[32:40, :].astype(F32)
    return state[0:1] + state[1:2], state[2:3] + state[3:4]


def merge(outs, peaks, totals):
    peak = functools.reduce(jnp.maximum, peaks)
    factors = [jnp.exp2(p - peak) for p in peaks]
    out = sum(o * f for o, f in zip(outs, factors))
    return out, peak, sum(t * f for t, f in zip(totals, factors))


def merged(refs):
    outs = [ref[0:32, :].astype(F32) for ref in refs]
    return merge(outs, *zip(*map(state_of, refs)))


def tiles_of(ref):
    return [ref.at[n] for n in range(ref.shape[0])]


def couple_body(own_ref, came_ref, out_ref):
    for n in range(16):
        out, peak, total = merged([own_ref.at[n], came_ref.at[n]])
        out_ref[n, 0:32, :] = out.astype(BF16)
        out_ref[n, 32:40, :] = state_rows(peak, total)


def merge_body(in_ref, out_ref):
    out, peak, total = merged(tiles_of(in_ref))
    out, state = out.astype(BF16), state_rows(peak, total)
    for d in range(out_ref.shape[0]):
        out_ref[d, 0:32, :] = out
        out_ref[d, 32:40, :] = state


def finish_body(in_ref, out_ref):
    out, _, total = merged(tiles_of(in_ref))
    out_ref[...] = (out / total).astype(BF16)


def pair_body(own_ref, came_ref, out_ref):
    first = lax.axis_index("c") == 0
    own, came = own_ref[...].astype(F32), came_ref[...].astype(F32)
    tiles = (jnp.where(first, own, came).astype(BF16), jnp.where(first, came, own).astype(BF16))
    for d in range(out_ref.shape[0]):
        for n, tile in enumerate(tiles):
            out_ref[d, n * 32 : (n + 1) * 32, :] = tile


def place_body(in_ref, out_hbm, out_ref, sems):
    copies = []
    eye = where_one(rows_of((128, 128)) == lanes((128, 128)))
    for g in range(KVH):
        half, y = divmod(g, 4)
        block = in_ref[y * 4 : (y + 1) * 4, half * 32 : (half + 1) * 32, :].reshape(128, 128)
        block = dot(eye, block, NT).astype(BF16)
        for i in range(8):
            at = (g * 8 + i) * HD
            out_ref[:, at : at + HD] = block[i * ROWS : (i + 1) * ROWS]
        if g % 2:
            part = slice((g - 1) * 8 * HD, (g + 1) * 8 * HD)
            copies.append(
                pltpu.make_async_copy(out_ref.at[:, part], out_hbm.at[:, part], sems.at[g // 2])
            )
            copies[-1].start()
    for copy in copies:
        copy.wait()


def per_device(
    queries,
    span_keys,
    span_values,
    positions,
    span_segments,
    cache_keys,
    cache_values,
    cache_segments,
):
    shape = jax.ShapeDtypeStruct
    small = (
        queries,
        span_keys.T,
        span_values.T,
        positions,
        span_segments.reshape(1, ROWS),
        cache_segments.reshape(4, 128),
    )
    tiles, positions, span_segments, cache_segments = call(
        pack_body,
        "pack",
        (shape((128, 8, 128), BF16), *(shape(a.shape, a.dtype) for a in small[3:])),
        *(pltpu.with_memory_space_constraint(a, pltpu.HBM) for a in small),
        specs=[HBM] * 6,
        scratch=[pltpu.VMEM(a.shape, a.dtype) for a in small[:3]] + [pltpu.SemaphoreType.DMA((6,))],
    )
    tiles = exchange(tiles, CHIPS)
    came = swap(tiles)
    bias, tables, turned_values = call(
        ready_body,
        "ready",
        (
            shape((512 + ROWS, 128), F32),
            shape((2, ROWS, 128), F32),
            shape((KVH, HD, 512), BF16),
        ),
        positions,
        span_segments,
        cache_segments,
        pltpu.with_memory_space_constraint(cache_values, pltpu.HBM),
        specs=[VMEM] * 3 + [HBM],
        scratch=[pltpu.VMEM((512, KVH * HD), BF16), pltpu.SemaphoreType.DMA],
    )
    message = shape((16, 40, 128), BF16)
    parts, q = call(
        first_body,
        "first",
        (message, shape((H * ROWS, HD), BF16)),
        tiles,
        came,
        tables,
        cache_keys,
        turned_values,
        bias,
    )
    other = swap(parts)
    parts = call(
        second_body, "second", message, q, cache_keys, turned_values, bias, tiles, came, tables
    )
    parts = call(couple_body, "couple", message, parts, other)
    parts = exchange(parts, PLANE)
    parts = call(merge_body, "merge", shape((8, 40, 128), BF16), parts)
    parts = exchange(parts, ("z",))
    tile = call(finish_body, "finish", shape((32, 128), BF16), parts)
    whole = call(pair_body, "pair", shape((16, 64, 128), BF16), tile, swap(tile))
    whole = exchange(whole, PLANE)
    return call(
        place_body,
        "place",
        shape((ROWS, H * HD), BF16),
        whole,
        scratch=[pltpu.VMEM((ROWS, H * HD), BF16), pltpu.SemaphoreType.DMA((4,))],
        out_specs=HBM,
    )


def solution(mesh):
    split = Mesh(mesh.devices.reshape(4, 8, 4, 2), ALL)
    return jax.shard_map(
        per_device,
        mesh=split,
        in_specs=(
            P(None, ALL),
            P(None, ALL),
            P(None, ALL),
            P(),
            P(),
            P(ALL, None),
            P(ALL, None),
            P(ALL),
        ),
        out_specs=P(),
        check_vma=False,
    )
```

```python
import functools

import jax
import jax.numpy as jnp
from jax import lax
from jax.experimental import pallas as pl
from jax.experimental.pallas import tpu as pltpu
from jax.sharding import Mesh
from jax.sharding import PartitionSpec as P

H = 64
KVH = 8
HD = 128
ROWS = 16
ALL = ("y", "z", "x", "c")
CHIPS = ("y", "z", "x")
PLANE = ("y", "x")
LOG2E = 1.4426950408889634
NONE = -1e30
HIDDEN = -2e30
F32 = jnp.float32
BF16 = jnp.bfloat16
VMEM = pl.BlockSpec(memory_space=pltpu.VMEM)
NT = (((1,), (1,)), ((), ()))

HBM = pl.BlockSpec(memory_space=pltpu.HBM)


def call(body, name, out_shape, *args, specs=None, scratch=(), limit=8 << 20, out_specs=None):
    return pl.pallas_call(
        body,
        name=name,
        out_shape=out_shape,
        in_specs=specs or [VMEM] * len(args),
        out_specs=out_specs or jax.tree.map(lambda _: VMEM, out_shape),
        scratch_shapes=scratch,
        compiler_params=pltpu.CompilerParams(vmem_limit_bytes=limit),
    )(*args)


def lanes(shape):
    return lax.broadcasted_iota(jnp.int32, shape, len(shape) - 1)


def move(value, by):
    by %= value.shape[-1]
    return pltpu.roll(value, by, value.ndim - 1) if by else value


def exchange(tiles, axes):
    return lax.all_to_all(tiles, axes, 0, 0, tiled=True)


def swap(value):
    return lax.ppermute(value, "c", ((0, 1), (1, 0)))


def rows_of(shape):
    return lax.broadcasted_iota(jnp.int32, shape, 0)


TN = (((0,), (0,)), ((), ()))
NN = (((1,), (0,)), ((), ()))


def dot(a, b, dims):
    return lax.dot_general(a, b, dims, preferred_element_type=F32)


def where_one(hit):
    return jnp.where(hit, 1.0, 0.0).astype(BF16)


def pack_body(*refs):
    out_ref, q_ref, k_ref, v_ref, sems = refs[6], *refs[10:]
    copies = [
        pltpu.make_async_copy(source, target, sems.at[n])
        for n, (source, target) in enumerate(zip(refs[:6], (q_ref, k_ref, v_ref, *refs[7:10])))
    ]
    for copy in copies:
        copy.start()
    for copy in copies:
        copy.wait()
    q = dot(q_ref[...], where_one(lanes((32, 128)) % 32 == rows_of((32, 128))), NN)
    q = jnp.where(lanes((ROWS, 128)) // 32 == rows_of((ROWS, 128)) // 4, q, 0.0).astype(BF16)
    token = lanes((ROWS, 128)) // 4 - rows_of((ROWS, 128))
    kv = dot(k_ref[...], where_one(token == 0), NN) + dot(v_ref[...], where_one(token == 16), NN)
    kv = jnp.where(lanes((4, 128)) % 4 == rows_of((4, 128)), kv, 0.0).astype(BF16)
    tiles = dot(where_one(rows_of((48, ROWS)) % 6 == lanes((48, ROWS)) % 4), q, NN)
    tiles = tiles + dot(where_one(rows_of((48, 4)) % 6 == 4), kv, NN)
    tiles = tiles.astype(BF16)
    for n in range(out_ref.shape[0] // 48):
        out_ref[n * 48 : (n + 1) * 48, :] = tiles


def turn(angle):
    quarter = jnp.floor(angle * 0.6366197723675814 + 0.5)
    rest = angle - quarter * 1.5703125
    rest = rest - quarter * 4.837512969970703e-4
    rest = rest - quarter * 7.549789948768648e-8
    square = rest * rest
    sine = -1.9515295891e-4 * square + 8.3321608736e-3
    sine = (sine * square - 1.6666654611e-1) * square * rest + rest
    cosine = 2.443315711809948e-5 * square - 1.388731625493765e-3
    cosine = (cosine * square + 4.166664568298827e-2) * square * square - 0.5 * square + 1.0
    which = quarter.astype(jnp.int32) % 4
    odd = which % 2 == 1
    cosine, sine = jnp.where(odd, sine, cosine), jnp.where(odd, cosine, sine)
    cosine = jnp.where((which == 1) | (which == 2), -cosine, cosine)
    sine = jnp.where(which >= 2, -sine, sine)
    return cosine, sine


def rope_tables(positions, index):
    section = jnp.where(index < 16, 0, jnp.where(index < 40, 1, 2))
    high = positions // 64
    position = jnp.zeros(index.shape, F32)
    for scale, part in ((64.0, high), (1.0, positions - high * 64)):
        chosen = dot(part.astype(F32).astype(BF16), where_one(rows_of((3, 3 * 128)) == lanes((3, 3 * 128)) // 128), TN)
        picked = chosen[:, 256:]
        for n in range(2):
            picked = jnp.where(section == n, chosen[:, n * 128 : (n + 1) * 128], picked)
        position = position + scale * picked
    inverse = jnp.ones(index.shape, F32)
    for bit in range(6):
        step = 1000000.0 ** (-2.0 * 2**bit / HD)
        inverse = jnp.where((index // 2**bit) % 2 == 1, inverse * step, inverse)
    return turn(position * inverse)


def rotate(value, cosine, sine):
    return value * cosine + move(value, 64) * sine


def split_pair(value):
    high = value.astype(BF16).astype(F32)
    return high, (value - high).astype(BF16).astype(F32)


def state_rows(peak, total):
    row = rows_of((8, 128))
    parts = (*split_pair(peak), *split_pair(total))
    tile = jnp.zeros((8, 128), F32)
    for n, part in enumerate(parts):
        tile = jnp.where(row == n, part, tile)
    return tile.astype(BF16)


def ready_body(pos_ref, seg_ref, held_ref, v_hbm, bias_ref, table_ref, vt_ref, v_ref, sem):
    copy = pltpu.make_async_copy(v_hbm, v_ref, sem)
    copy.start()
    lane = lanes((ROWS, 128))
    cosine, sine = rope_tables(pos_ref[...], lane % 64)
    table_ref[0] = cosine
    table_ref[1] = jnp.where(lane < 64, -sine, sine)
    pick = where_one(rows_of((ROWS, 128)) == lane // 8)
    kinds = where_one(rows_of((8, ROWS)) == seg_ref[...])
    wanted = dot(kinds, pick, NN).astype(BF16)
    for part in range(4):
        have = where_one(rows_of((8, 128)) == held_ref[part : part + 1, :])
        bias_ref[part * 128 : (part + 1) * 128, :] = (dot(have, wanted, TN) - 1.0) * -HIDDEN
    seen = dot(kinds, wanted, TN) * jnp.where(rows_of((ROWS, 128)) <= lane // 8, 1.0, 0.0)
    bias_ref[512:, :] = (seen - 1.0) * -HIDDEN
    copy.wait()
    for g in range(KVH):
        vt_ref[g] = v_ref[:, g * HD : (g + 1) * HD].T


def join(own_ref, came_ref, table_ref, q_ref, kv_ref, flat_ref):
    c = lax.axis_index("c")
    shape = (128, 4 * 128)
    source, target = rows_of(shape), lanes(shape)
    whole = jnp.zeros((256, 512), F32)
    for n, ref in enumerate((own_ref, came_ref)):
        flat_ref[n, 0:768, :] = ref[...].astype(F32)
        kv_ref[n] = flat_ref[n, pl.ds(4, 128, stride=6), :]
        for half in range(2):
            part = jnp.concatenate(
                [flat_ref[n, pl.ds(j + 6 * half, 64, stride=12), :] for j in range(4)], axis=0
            )
            core = 1 - c if n else c
            at = (source // 32) * 128 + half * 64 + core * 32 + source % 32
            whole = whole + dot(part.astype(BF16), where_one(target == at), NN)
    for r in range(ROWS):
        high, low = divmod(r, 4)
        part = whole[low * 64 : (low + 1) * 64, high * 128 : (high + 1) * 128]
        part = rotate(part, table_ref[0, r : r + 1, :], table_ref[1, r : r + 1, :]).astype(BF16)
        for g in range(KVH):
            q_ref[g * 128 + r * 8 : g * 128 + r * 8 + 8, :] = part[g * 8 : (g + 1) * 8]


FACTOR = LOG2E / HD**0.5


def softened(scores):
    peak = jnp.maximum(jnp.max(scores, axis=0, keepdims=True), NONE)
    high, low = split_pair(peak)
    peak = high + low
    weights = jnp.exp2(scores - peak)
    return weights.astype(BF16), peak, jnp.sum(weights, axis=0, keepdims=True)


def heads_at(base, i):
    return pl.ds(pl.multiple_of((base + i) * 128, 128), 128)


def attend(base, q_ref, k_ref, vt_ref, bias_ref, out_ref):
    scores = [
        dot(k_ref[:, heads_at(base, i)], q_ref[heads_at(base, i), :], NT) * FACTOR
        + bias_ref[0:512, :]
        for i in range(4)
    ]
    parts = [softened(s) for s in scores]
    outs = [dot(vt_ref[base + i], parts[i][0], NN) for i in range(4)]
    for i, (_, peak, total) in enumerate(parts):
        emit(out_ref, i * 4, outs[i].astype(BF16), state_rows(peak, total))


def emit(out_ref, first, out, state):
    for n in range(4):
        out_ref[first + n, 0:32, :] = out[n * 32 : (n + 1) * 32]
        out_ref[first + n, 32:40, :] = state


def first_body(
    own_ref, came_ref, table_ref, k_ref, vt_ref, bias_ref, out_ref, q_ref, kv_ref, flat_ref
):
    join(own_ref, came_ref, table_ref, q_ref, kv_ref, flat_ref)
    attend((1 - lax.axis_index("c")) * 4, q_ref, k_ref, vt_ref, bias_ref, out_ref)


def second_body(q_ref, k_ref, vt_ref, bias_ref, kv_ref, table_ref, out_ref):
    c, y = lax.axis_index("c"), lax.axis_index("y")
    attend(c * 4, q_ref, k_ref, vt_ref, bias_ref, out_ref)

    @pl.when((lax.axis_index("z") == 0) & (lax.axis_index("x") == 0))
    def _():
        g = c * 4 + y
        chips = pl.ds(pl.multiple_of(g * 16, 16), 16)
        own, came = kv_ref[0, chips, :], kv_ref[1, chips, :]
        held = [jnp.where(c == core, own, came).astype(BF16) for core in range(2)]
        row, lane = rows_of((64, 128)), lanes((64, 128))
        found = []
        for kind in range(2):
            pick = where_one(lane == kind * 64 + (row % 16) * 4 + row // 16)
            value = jnp.zeros((ROWS, 128), F32)
            for core in range(2):
                columns = dot(pick, held[core], NT).astype(BF16)
                for i in range(4):
                    at = rows_of((ROWS, 128)) * 8 + core * 4 + i
                    value = value + dot(
                        columns[i * 16 : (i + 1) * 16], where_one(lanes((ROWS, 128)) == at), NN
                    )
            if kind == 0:
                value = rotate(value, table_ref[0], table_ref[1])
            found.append(value.astype(BF16))
        scores = dot(found[0], q_ref[heads_at(c * 4, y), :], NT) * FACTOR + bias_ref[512:, :]
        weights, peak, total = softened(scores)
        own = dot(found[1], weights, TN)
        for n in range(4):
            tile = out_ref.at[y * 4 + n]
            out, peaks, totals = merge(
                [tile[0:32, :].astype(F32), own[n * 32 : (n + 1) * 32]],
                *zip(state_of(tile), (peak, total)),
            )
            tile[0:32, :] = out.astype(BF16)
            tile[32:40, :] = state_rows(peaks, totals)


def state_of(ref):
    state = ref[32:40, :].astype(F32)
    return state[0:1] + state[1:2], state[2:3] + state[3:4]


def merge(outs, peaks, totals):
    peak = functools.reduce(jnp.maximum, peaks)
    factors = [jnp.exp2(p - peak) for p in peaks]
    out = sum(o * f for o, f in zip(outs, factors))
    return out, peak, sum(t * f for t, f in zip(totals, factors))


def merged(refs):
    outs = [ref[0:32, :].astype(F32) for ref in refs]
    return merge(outs, *zip(*map(state_of, refs)))


def tiles_of(ref):
    return [ref.at[n] for n in range(ref.shape[0])]


def couple_body(own_ref, came_ref, out_ref):
    for n in range(16):
        out, peak, total = merged([own_ref.at[n], came_ref.at[n]])
        out_ref[n, 0:32, :] = out.astype(BF16)
        out_ref[n, 32:40, :] = state_rows(peak, total)


def merge_body(in_ref, out_ref):
    out, peak, total = merged(tiles_of(in_ref))
    out, state = out.astype(BF16), state_rows(peak, total)
    for d in range(out_ref.shape[0]):
        out_ref[d, 0:32, :] = out
        out_ref[d, 32:40, :] = state


def finish_body(in_ref, out_ref):
    out, _, total = merged(tiles_of(in_ref))
    out_ref[...] = (out / total).astype(BF16)


def pair_body(own_ref, came_ref, out_ref):
    first = lax.axis_index("c") == 0
    own, came = own_ref[...].astype(F32), came_ref[...].astype(F32)
    tiles = (jnp.where(first, own, came).astype(BF16), jnp.where(first, came, own).astype(BF16))
    for d in range(out_ref.shape[0]):
        for n, tile in enumerate(tiles):
            out_ref[d, n * 32 : (n + 1) * 32, :] = tile


def place_body(in_ref, out_hbm, out_ref, sems):
    copies = []
    row = rows_of((128, 128))
    eye = where_one((row % 16) * 8 + row // 16 == lanes((128, 128)))
    for g in range(KVH):
        half, y = divmod(g, 4)
        block = in_ref[y * 4 : (y + 1) * 4, half * 32 : (half + 1) * 32, :].reshape(128, 128)
        block = dot(eye, block, NT).astype(BF16)
        for i in range(8):
            at = (g * 8 + i) * HD
            out_ref[:, at : at + HD] = block[i * ROWS : (i + 1) * ROWS]
        if g % 2:
            part = slice((g - 1) * 8 * HD, (g + 1) * 8 * HD)
            copies.append(
                pltpu.make_async_copy(out_ref.at[:, part], out_hbm.at[:, part], sems.at[g // 2])
            )
            copies[-1].start()
    for copy in copies:
        copy.wait()


def per_device(
    queries,
    span_keys,
    span_values,
    positions,
    span_segments,
    cache_keys,
    cache_values,
    cache_segments,
):
    shape = jax.ShapeDtypeStruct
    small = (
        queries,
        span_keys.T,
        span_values.T,
        positions,
        span_segments.reshape(1, ROWS),
        cache_segments.reshape(4, 128),
    )
    tiles, positions, span_segments, cache_segments = call(
        pack_body,
        "pack",
        (shape((6 * 128, 128), BF16), *(shape(a.shape, a.dtype) for a in small[3:])),
        *(pltpu.with_memory_space_constraint(a, pltpu.HBM) for a in small),
        specs=[HBM] * 6,
        scratch=[pltpu.VMEM(a.shape, a.dtype) for a in small[:3]] + [pltpu.SemaphoreType.DMA((6,))],
    )
    tiles = exchange(tiles.reshape(-1, 2, 128), CHIPS).reshape(-1, 128)
    came = swap(tiles)
    bias, tables, turned_values = call(
        ready_body,
        "ready",
        (
            shape((512 + ROWS, 128), F32),
            shape((2, ROWS, 128), F32),
            shape((KVH, HD, 512), BF16),
        ),
        positions,
        span_segments,
        cache_segments,
        pltpu.with_memory_space_constraint(cache_values, pltpu.HBM),
        specs=[VMEM] * 3 + [HBM],
        scratch=[pltpu.VMEM((512, KVH * HD), BF16), pltpu.SemaphoreType.DMA],
    )
    message = shape((16, 40, 128), BF16)
    parts, q, kv = call(
        first_body,
        "first",
        (message, shape((H * ROWS, HD), BF16), shape((2, 128, 128), F32)),
        tiles,
        came,
        tables,
        cache_keys,
        turned_values,
        bias,
        scratch=[pltpu.VMEM((2, 6 * 128 + 16, 128), F32)],
    )
    other = swap(parts)
    parts = call(
        second_body, "second", message, q, cache_keys, turned_values, bias, kv, tables
    )
    parts = call(couple_body, "couple", message, parts, other)
    parts = exchange(parts, PLANE)
    parts = call(merge_body, "merge", shape((8, 40, 128), BF16), parts)
    parts = exchange(parts, ("z",))
    tile = call(finish_body, "finish", shape((32, 128), BF16), parts)
    whole = call(pair_body, "pair", shape((16, 64, 128), BF16), tile, swap(tile))
    whole = exchange(whole, PLANE)
    return call(
        place_body,
        "place",
        shape((ROWS, H * HD), BF16),
        whole,
        scratch=[pltpu.VMEM((ROWS, H * HD), BF16), pltpu.SemaphoreType.DMA((4,))],
        out_specs=HBM,
    )


def solution(mesh):
    split = Mesh(mesh.devices.reshape(4, 8, 4, 2), ALL)
    return jax.shard_map(
        per_device,
        mesh=split,
        in_specs=(
            P(None, ALL),
            P(None, ALL),
            P(None, ALL),
            P(),
            P(),
            P(ALL, None),
            P(ALL, None),
            P(ALL),
        ),
        out_specs=P(),
        check_vma=False,
    )
```

```python
import functools

import jax
import jax.numpy as jnp
from jax import lax
from jax.experimental import pallas as pl
from jax.experimental.pallas import tpu as pltpu
from jax.sharding import Mesh
from jax.sharding import PartitionSpec as P

H = 64
KVH = 8
HD = 128
ROWS = 16
ALL = ("y", "z", "x", "c")
CHIPS = ("y", "z", "x")
PLANE = ("y", "x")
NEAR = ("y", "x", "c")
LOG2E = 1.4426950408889634
NONE = -1e30
HIDDEN = -2e30
F32 = jnp.float32
BF16 = jnp.bfloat16
VMEM = pl.BlockSpec(memory_space=pltpu.VMEM)
NT = (((1,), (1,)), ((), ()))

HBM = pl.BlockSpec(memory_space=pltpu.HBM)


def call(body, name, out_shape, *args, specs=None, scratch=(), limit=8 << 20, out_specs=None):
    return pl.pallas_call(
        body,
        name=name,
        out_shape=out_shape,
        in_specs=specs or [VMEM] * len(args),
        out_specs=out_specs or jax.tree.map(lambda _: VMEM, out_shape),
        scratch_shapes=scratch,
        compiler_params=pltpu.CompilerParams(vmem_limit_bytes=limit),
    )(*args)


def lanes(shape):
    return lax.broadcasted_iota(jnp.int32, shape, len(shape) - 1)


def move(value, by):
    by %= value.shape[-1]
    return pltpu.roll(value, by, value.ndim - 1) if by else value


def exchange(tiles, axes):
    return lax.all_to_all(tiles, axes, 0, 0, tiled=True)


def swap(value):
    return lax.ppermute(value, "c", ((0, 1), (1, 0)))


def rows_of(shape):
    return lax.broadcasted_iota(jnp.int32, shape, 0)


TN = (((0,), (0,)), ((), ()))
NN = (((1,), (0,)), ((), ()))


def dot(a, b, dims):
    return lax.dot_general(a, b, dims, preferred_element_type=F32)


def where_one(hit):
    return jnp.where(hit, 1.0, 0.0).astype(BF16)


def pack_body(*refs):
    out_ref, q_ref, k_ref, v_ref, sems = refs[6], *refs[10:]
    copies = [
        pltpu.make_async_copy(source, target, sems.at[n])
        for n, (source, target) in enumerate(zip(refs[:6], (q_ref, k_ref, v_ref, *refs[7:10])))
    ]
    for copy in copies:
        copy.start()
    for copy in copies:
        copy.wait()
    q = dot(q_ref[...], where_one(lanes((32, 128)) % 32 == rows_of((32, 128))), NN)
    q = jnp.where(lanes((ROWS, 128)) // 32 == rows_of((ROWS, 128)) // 4, q, 0.0).astype(BF16)
    token = lanes((ROWS, 128)) // 4 - rows_of((ROWS, 128))
    kv = dot(k_ref[...], where_one(token == 0), NN) + dot(v_ref[...], where_one(token == 16), NN)
    kv = jnp.where(lanes((4, 128)) % 4 == rows_of((4, 128)), kv, 0.0).astype(BF16)
    tiles = dot(where_one(rows_of((48, ROWS)) % 6 == lanes((48, ROWS)) % 4), q, NN)
    tiles = tiles + dot(where_one(rows_of((48, 4)) % 6 == 4), kv, NN)
    tiles = tiles.astype(BF16)
    for n in range(out_ref.shape[0] // 48):
        out_ref[n * 48 : (n + 1) * 48, :] = tiles


def turn(angle):
    quarter = jnp.floor(angle * 0.6366197723675814 + 0.5)
    rest = angle - quarter * 1.5703125
    rest = rest - quarter * 4.837512969970703e-4
    rest = rest - quarter * 7.549789948768648e-8
    square = rest * rest
    sine = -1.9515295891e-4 * square + 8.3321608736e-3
    sine = (sine * square - 1.6666654611e-1) * square * rest + rest
    cosine = 2.443315711809948e-5 * square - 1.388731625493765e-3
    cosine = (cosine * square + 4.166664568298827e-2) * square * square - 0.5 * square + 1.0
    which = quarter.astype(jnp.int32) % 4
    odd = which % 2 == 1
    cosine, sine = jnp.where(odd, sine, cosine), jnp.where(odd, cosine, sine)
    cosine = jnp.where((which == 1) | (which == 2), -cosine, cosine)
    sine = jnp.where(which >= 2, -sine, sine)
    return cosine, sine


def rope_tables(positions, index):
    section = jnp.where(index < 16, 0, jnp.where(index < 40, 1, 2))
    high = positions // 64
    position = jnp.zeros(index.shape, F32)
    for scale, part in ((64.0, high), (1.0, positions - high * 64)):
        chosen = dot(part.astype(F32).astype(BF16), where_one(rows_of((3, 3 * 128)) == lanes((3, 3 * 128)) // 128), TN)
        picked = chosen[:, 256:]
        for n in range(2):
            picked = jnp.where(section == n, chosen[:, n * 128 : (n + 1) * 128], picked)
        position = position + scale * picked
    inverse = jnp.ones(index.shape, F32)
    for bit in range(6):
        step = 1000000.0 ** (-2.0 * 2**bit / HD)
        inverse = jnp.where((index // 2**bit) % 2 == 1, inverse * step, inverse)
    return turn(position * inverse)


def rotate(value, cosine, sine):
    return value * cosine + move(value, 64) * sine


def split_pair(value):
    high = value.astype(BF16).astype(F32)
    return high, (value - high).astype(BF16).astype(F32)


def state_rows(peak, total):
    row = rows_of((8, 128))
    parts = (*split_pair(peak), *split_pair(total))
    tile = jnp.zeros((8, 128), F32)
    for n, part in enumerate(parts):
        tile = jnp.where(row == n, part, tile)
    return tile.astype(BF16)


def ready_body(pos_ref, seg_ref, held_ref, v_hbm, bias_ref, table_ref, vt_ref, v_ref, sem):
    copy = pltpu.make_async_copy(v_hbm, v_ref, sem)
    copy.start()
    lane = lanes((ROWS, 128))
    cosine, sine = rope_tables(pos_ref[...], lane % 64)
    table_ref[0] = cosine
    table_ref[1] = jnp.where(lane < 64, -sine, sine)
    pick = where_one(rows_of((ROWS, 128)) == lane // 8)
    kinds = where_one(rows_of((8, ROWS)) == seg_ref[...])
    wanted = dot(kinds, pick, NN).astype(BF16)
    for part in range(4):
        have = where_one(rows_of((8, 128)) == held_ref[part : part + 1, :])
        bias_ref[part * 128 : (part + 1) * 128, :] = (dot(have, wanted, TN) - 1.0) * -HIDDEN
    seen = dot(kinds, wanted, TN) * jnp.where(rows_of((ROWS, 128)) <= lane // 8, 1.0, 0.0)
    bias_ref[512:, :] = (seen - 1.0) * -HIDDEN
    copy.wait()
    for g in range(KVH):
        vt_ref[g] = v_ref[:, g * HD : (g + 1) * HD].T


def join(own_ref, came_ref, table_ref, q_ref, kv_ref, flat_ref):
    c = lax.axis_index("c")
    shape = (128, 4 * 128)
    source, target = rows_of(shape), lanes(shape)
    whole = jnp.zeros((256, 512), F32)
    for n, ref in enumerate((own_ref, came_ref)):
        flat_ref[n, 0:768, :] = ref[...].astype(F32)
        kv_ref[n] = flat_ref[n, pl.ds(4, 128, stride=6), :]
        for half in range(2):
            part = jnp.concatenate(
                [flat_ref[n, pl.ds(j + 6 * half, 64, stride=12), :] for j in range(4)], axis=0
            )
            core = 1 - c if n else c
            at = (source // 32) * 128 + half * 64 + core * 32 + source % 32
            whole = whole + dot(part.astype(BF16), where_one(target == at), NN)
    for r in range(ROWS):
        high, low = divmod(r, 4)
        part = whole[low * 64 : (low + 1) * 64, high * 128 : (high + 1) * 128]
        part = rotate(part, table_ref[0, r : r + 1, :], table_ref[1, r : r + 1, :]).astype(BF16)
        for g in range(KVH):
            q_ref[g * 128 + r * 8 : g * 128 + r * 8 + 8, :] = part[g * 8 : (g + 1) * 8]


FACTOR = LOG2E / HD**0.5


def softened(scores):
    peak = jnp.maximum(jnp.max(scores, axis=0, keepdims=True), NONE)
    high, low = split_pair(peak)
    peak = high + low
    weights = jnp.exp2(scores - peak)
    return weights.astype(BF16), peak, jnp.sum(weights, axis=0, keepdims=True)


def heads_at(base, i):
    return pl.ds(pl.multiple_of((base + i) * 128, 128), 128)


def attend(base, q_ref, k_ref, vt_ref, bias_ref, out_ref):
    scores = [
        dot(k_ref[:, heads_at(base, i)], q_ref[heads_at(base, i), :], NT) * FACTOR
        + bias_ref[0:512, :]
        for i in range(4)
    ]
    parts = [softened(s) for s in scores]
    outs = [dot(vt_ref[base + i], parts[i][0], NN) for i in range(4)]
    for i, (_, peak, total) in enumerate(parts):
        emit(out_ref, i * 4, outs[i].astype(BF16), state_rows(peak, total))


def emit(out_ref, first, out, state):
    for n in range(4):
        out_ref[first + n, 0:32, :] = out[n * 32 : (n + 1) * 32]
        out_ref[first + n, 32:40, :] = state


def first_body(
    own_ref, came_ref, table_ref, k_ref, vt_ref, bias_ref, out_ref, q_ref, kv_ref, flat_ref
):
    join(own_ref, came_ref, table_ref, q_ref, kv_ref, flat_ref)
    attend((1 - lax.axis_index("c")) * 4, q_ref, k_ref, vt_ref, bias_ref, out_ref)


def second_body(q_ref, k_ref, vt_ref, bias_ref, kv_ref, table_ref, out_ref):
    c, y = lax.axis_index("c"), lax.axis_index("y")
    attend(c * 4, q_ref, k_ref, vt_ref, bias_ref, out_ref)

    @pl.when((lax.axis_index("z") == 0) & (lax.axis_index("x") == 0))
    def _():
        g = c * 4 + y
        chips = pl.ds(pl.multiple_of(g * 16, 16), 16)
        own, came = kv_ref[0, chips, :], kv_ref[1, chips, :]
        held = [jnp.where(c == core, own, came).astype(BF16) for core in range(2)]
        row, lane = rows_of((64, 128)), lanes((64, 128))
        found = []
        for kind in range(2):
            pick = where_one(lane == kind * 64 + (row % 16) * 4 + row // 16)
            value = jnp.zeros((ROWS, 128), F32)
            for core in range(2):
                columns = dot(pick, held[core], NT).astype(BF16)
                for i in range(4):
                    at = rows_of((ROWS, 128)) * 8 + core * 4 + i
                    value = value + dot(
                        columns[i * 16 : (i + 1) * 16], where_one(lanes((ROWS, 128)) == at), NN
                    )
            if kind == 0:
                value = rotate(value, table_ref[0], table_ref[1])
            found.append(value.astype(BF16))
        scores = dot(found[0], q_ref[heads_at(c * 4, y), :], NT) * FACTOR + bias_ref[512:, :]
        weights, peak, total = softened(scores)
        own = dot(found[1], weights, TN)
        for n in range(4):
            tile = out_ref.at[y * 4 + n]
            out, peaks, totals = merge(
                [tile[0:32, :].astype(F32), own[n * 32 : (n + 1) * 32]],
                *zip(state_of(tile), (peak, total)),
            )
            tile[0:32, :] = out.astype(BF16)
            tile[32:40, :] = state_rows(peaks, totals)


def state_of(ref):
    state = ref[32:40, :].astype(F32)
    return state[0:1] + state[1:2], state[2:3] + state[3:4]


def merge(outs, peaks, totals):
    peak = functools.reduce(jnp.maximum, peaks)
    factors = [jnp.exp2(p - peak) for p in peaks]
    out = sum(o * f for o, f in zip(outs, factors))
    return out, peak, sum(t * f for t, f in zip(totals, factors))


def merged(refs):
    outs = [ref[0:32, :].astype(F32) for ref in refs]
    return merge(outs, *zip(*map(state_of, refs)))


def tiles_of(ref):
    return [ref.at[n] for n in range(ref.shape[0])]


def couple_body(own_ref, came_ref, out_ref):
    for n in range(16):
        out, peak, total = merged([own_ref.at[n], came_ref.at[n]])
        out_ref[n, 0:32, :] = out.astype(BF16)
        out_ref[n, 32:40, :] = state_rows(peak, total)


def merge_body(in_ref, out_ref):
    out, peak, total = merged(tiles_of(in_ref))
    out, state = out.astype(BF16), state_rows(peak, total)
    for d in range(out_ref.shape[0]):
        out_ref[d, 0:32, :] = out
        out_ref[d, 32:40, :] = state


def finish_body(in_ref, out_ref):
    out, _, total = merged(tiles_of(in_ref))
    out = (out / total).astype(BF16)
    for d in range(out_ref.shape[0]):
        out_ref[d] = out


def place_body(in_ref, out_hbm, out_ref, sems):
    copies = []
    row = rows_of((128, 128))
    eye = where_one((row % 16) * 8 + row // 16 == lanes((128, 128)))
    for g in range(KVH):
        half, y = divmod(g, 4)
        block = jnp.concatenate([in_ref[(y * 4 + n) * 2 + half] for n in range(4)], axis=0)
        block = dot(eye, block, NT).astype(BF16)
        for i in range(8):
            at = (g * 8 + i) * HD
            out_ref[:, at : at + HD] = block[i * ROWS : (i + 1) * ROWS]
        if g % 2:
            part = slice((g - 1) * 8 * HD, (g + 1) * 8 * HD)
            copies.append(
                pltpu.make_async_copy(out_ref.at[:, part], out_hbm.at[:, part], sems.at[g // 2])
            )
            copies[-1].start()
    for copy in copies:
        copy.wait()


def per_device(
    queries,
    span_keys,
    span_values,
    positions,
    span_segments,
    cache_keys,
    cache_values,
    cache_segments,
):
    shape = jax.ShapeDtypeStruct
    small = (
        queries,
        span_keys.T,
        span_values.T,
        positions,
        span_segments.reshape(1, ROWS),
        cache_segments.reshape(4, 128),
    )
    tiles, positions, span_segments, cache_segments = call(
        pack_body,
        "pack",
        (shape((6 * 128, 128), BF16), *(shape(a.shape, a.dtype) for a in small[3:])),
        *(pltpu.with_memory_space_constraint(a, pltpu.HBM) for a in small),
        specs=[HBM] * 6,
        scratch=[pltpu.VMEM(a.shape, a.dtype) for a in small[:3]] + [pltpu.SemaphoreType.DMA((6,))],
    )
    tiles = exchange(tiles.reshape(-1, 2, 128), CHIPS).reshape(-1, 128)
    came = swap(tiles)
    bias, tables, turned_values = call(
        ready_body,
        "ready",
        (
            shape((512 + ROWS, 128), F32),
            shape((2, ROWS, 128), F32),
            shape((KVH, HD, 512), BF16),
        ),
        positions,
        span_segments,
        cache_segments,
        pltpu.with_memory_space_constraint(cache_values, pltpu.HBM),
        specs=[VMEM] * 3 + [HBM],
        scratch=[pltpu.VMEM((512, KVH * HD), BF16), pltpu.SemaphoreType.DMA],
    )
    message = shape((16, 40, 128), BF16)
    parts, q, kv = call(
        first_body,
        "first",
        (message, shape((H * ROWS, HD), BF16), shape((2, 128, 128), F32)),
        tiles,
        came,
        tables,
        cache_keys,
        turned_values,
        bias,
        scratch=[pltpu.VMEM((2, 6 * 128 + 16, 128), F32)],
    )
    other = swap(parts)
    parts = call(
        second_body, "second", message, q, cache_keys, turned_values, bias, kv, tables
    )
    parts = call(couple_body, "couple", message, parts, other)
    parts = exchange(parts, PLANE)
    parts = call(merge_body, "merge", shape((8, 40, 128), BF16), parts)
    parts = exchange(parts, ("z",))
    whole = call(finish_body, "finish", shape((32, 32, 128), BF16), parts)
    whole = exchange(whole, NEAR)
    return call(
        place_body,
        "place",
        shape((ROWS, H * HD), BF16),
        whole,
        scratch=[pltpu.VMEM((ROWS, H * HD), BF16), pltpu.SemaphoreType.DMA((4,))],
        out_specs=HBM,
    )


def solution(mesh):
    split = Mesh(mesh.devices.reshape(4, 8, 4, 2), ALL)
    return jax.shard_map(
        per_device,
        mesh=split,
        in_specs=(
            P(None, ALL),
            P(None, ALL),
            P(None, ALL),
            P(),
            P(),
            P(ALL, None),
            P(ALL, None),
            P(ALL),
        ),
        out_specs=P(),
        check_vma=False,
    )
```

```python
import functools

import jax
import jax.numpy as jnp
from jax import lax
from jax.experimental import pallas as pl
from jax.experimental.pallas import tpu as pltpu
from jax.sharding import Mesh
from jax.sharding import PartitionSpec as P

H = 64
KVH = 8
HD = 128
ROWS = 16
ALL = ("y", "z", "x", "c")
CHIPS = ("y", "z", "x")
PLANE = ("y", "x")
LOG2E = 1.4426950408889634
NONE = -1e30
HIDDEN = -2e30
F32 = jnp.float32
BF16 = jnp.bfloat16
VMEM = pl.BlockSpec(memory_space=pltpu.VMEM)
NT = (((1,), (1,)), ((), ()))

HBM = pl.BlockSpec(memory_space=pltpu.HBM)


def call(body, name, out_shape, *args, specs=None, scratch=(), limit=8 << 20, out_specs=None):
    return pl.pallas_call(
        body,
        name=name,
        out_shape=out_shape,
        in_specs=specs or [VMEM] * len(args),
        out_specs=out_specs or jax.tree.map(lambda _: VMEM, out_shape),
        scratch_shapes=scratch,
        compiler_params=pltpu.CompilerParams(vmem_limit_bytes=limit),
    )(*args)


def lanes(shape):
    return lax.broadcasted_iota(jnp.int32, shape, len(shape) - 1)


def move(value, by):
    by %= value.shape[-1]
    return pltpu.roll(value, by, value.ndim - 1) if by else value


def exchange(tiles, axes):
    return lax.all_to_all(tiles, axes, 0, 0, tiled=True)


def swap(value):
    return lax.ppermute(value, "c", ((0, 1), (1, 0)))


def rows_of(shape):
    return lax.broadcasted_iota(jnp.int32, shape, 0)


TN = (((0,), (0,)), ((), ()))
NN = (((1,), (0,)), ((), ()))


def dot(a, b, dims):
    return lax.dot_general(a, b, dims, preferred_element_type=F32)


def where_one(hit):
    return jnp.where(hit, 1.0, 0.0).astype(BF16)


def pack_body(*refs):
    out_ref, q_ref, k_ref, v_ref, sems = refs[6], *refs[10:]
    copies = [
        pltpu.make_async_copy(source, target, sems.at[n])
        for n, (source, target) in enumerate(zip(refs[:6], (q_ref, k_ref, v_ref, *refs[7:10])))
    ]
    for copy in copies:
        copy.start()
    wide = where_one(lanes((32, 128)) % 32 == rows_of((32, 128)))
    late = lanes((ROWS, 128)) // 32 == rows_of((ROWS, 128)) // 4
    token = lanes((ROWS, 128)) // 4 - rows_of((ROWS, 128))
    keys, values = where_one(token == 0), where_one(token == 16)
    column = lanes((4, 128)) % 4 == rows_of((4, 128))
    q_rows = where_one(rows_of((48, ROWS)) % 6 == lanes((48, ROWS)) % 4)
    kv_rows = where_one(rows_of((48, 4)) % 6 == 4)
    for copy in copies:
        copy.wait()
    q = jnp.where(late, dot(q_ref[...], wide, NN), 0.0).astype(BF16)
    kv = dot(k_ref[...], keys, NN) + dot(v_ref[...], values, NN)
    kv = jnp.where(column, kv, 0.0).astype(BF16)
    tiles = (dot(q_rows, q, NN) + dot(kv_rows, kv, NN)).astype(BF16)
    for n in range(out_ref.shape[0] // 48):
        out_ref[n * 48 : (n + 1) * 48, :] = tiles


def turn(angle):
    quarter = jnp.floor(angle * 0.6366197723675814 + 0.5)
    rest = angle - quarter * 1.5703125
    rest = rest - quarter * 4.837512969970703e-4
    rest = rest - quarter * 7.549789948768648e-8
    square = rest * rest
    sine = -1.9515295891e-4 * square + 8.3321608736e-3
    sine = (sine * square - 1.6666654611e-1) * square * rest + rest
    cosine = 2.443315711809948e-5 * square - 1.388731625493765e-3
    cosine = (cosine * square + 4.166664568298827e-2) * square * square - 0.5 * square + 1.0
    which = quarter.astype(jnp.int32) % 4
    odd = which % 2 == 1
    cosine, sine = jnp.where(odd, sine, cosine), jnp.where(odd, cosine, sine)
    cosine = jnp.where((which == 1) | (which == 2), -cosine, cosine)
    sine = jnp.where(which >= 2, -sine, sine)
    return cosine, sine


def rope_tables(positions, index):
    section = jnp.where(index < 16, 0, jnp.where(index < 40, 1, 2))
    high = positions // 64
    position = jnp.zeros(index.shape, F32)
    for scale, part in ((64.0, high), (1.0, positions - high * 64)):
        chosen = dot(part.astype(F32).astype(BF16), where_one(rows_of((3, 3 * 128)) == lanes((3, 3 * 128)) // 128), TN)
        picked = chosen[:, 256:]
        for n in range(2):
            picked = jnp.where(section == n, chosen[:, n * 128 : (n + 1) * 128], picked)
        position = position + scale * picked
    inverse = jnp.ones(index.shape, F32)
    for bit in range(6):
        step = 1000000.0 ** (-2.0 * 2**bit / HD)
        inverse = jnp.where((index // 2**bit) % 2 == 1, inverse * step, inverse)
    return turn(position * inverse)


def rotate(value, cosine, sine):
    return value * cosine + move(value, 64) * sine


def split_pair(value):
    high = value.astype(BF16).astype(F32)
    return high, (value - high).astype(BF16).astype(F32)


def state_rows(peak, total):
    row = rows_of((8, 128))
    parts = (*split_pair(peak), *split_pair(total))
    tile = jnp.zeros((8, 128), F32)
    for n, part in enumerate(parts):
        tile = jnp.where(row == n, part, tile)
    return tile.astype(BF16)


def ready_body(pos_ref, seg_ref, held_ref, v_hbm, bias_ref, table_ref, vt_ref, v_ref, sem):
    copy = pltpu.make_async_copy(v_hbm, v_ref, sem)
    copy.start()
    lane = lanes((ROWS, 128))
    cosine, sine = rope_tables(pos_ref[...], lane % 64)
    table_ref[0] = cosine
    table_ref[1] = jnp.where(lane < 64, -sine, sine)
    pick = where_one(rows_of((ROWS, 128)) == lane // 8)
    kinds = where_one(rows_of((8, ROWS)) == seg_ref[...])
    wanted = dot(kinds, pick, NN).astype(BF16)
    for part in range(4):
        have = where_one(rows_of((8, 128)) == held_ref[part : part + 1, :])
        bias_ref[part * 128 : (part + 1) * 128, :] = (dot(have, wanted, TN) - 1.0) * -HIDDEN
    seen = dot(kinds, wanted, TN) * jnp.where(rows_of((ROWS, 128)) <= lane // 8, 1.0, 0.0)
    bias_ref[512:, :] = (seen - 1.0) * -HIDDEN
    copy.wait()
    for g in range(KVH):
        vt_ref[g] = v_ref[:, g * HD : (g + 1) * HD].T


def join(base, own_ref, came_ref, table_ref, q_ref, flat_ref):
    c = lax.axis_index("c")
    shape = (128, 4 * 128)
    source, target = rows_of(shape), lanes(shape)
    rows = pl.ds(pl.multiple_of(base * 96, 384), 384)
    whole = jnp.zeros((128, 512), F32)
    for n, ref in enumerate((own_ref, came_ref)):
        flat_ref[n, 0:384, :] = ref[rows, :].astype(F32)
        for half in range(2):
            part = jnp.concatenate(
                [flat_ref[n, pl.ds(j + 6 * half, 32, stride=12), :] for j in range(4)], axis=0
            )
            core = 1 - c if n else c
            at = (source // 32) * 128 + half * 64 + core * 32 + source % 32
            whole = whole + dot(part.astype(BF16), where_one(target == at), NN)
    for r in range(ROWS):
        high, low = divmod(r, 4)
        part = whole[low * 32 : (low + 1) * 32, high * 128 : (high + 1) * 128]
        part = rotate(part, table_ref[0, r : r + 1, :], table_ref[1, r : r + 1, :]).astype(BF16)
        for i in range(4):
            q_ref[i * 128 + r * 8 : i * 128 + r * 8 + 8, :] = part[i * 8 : (i + 1) * 8]


FACTOR = LOG2E / HD**0.5


def softened(scores):
    peak = jnp.maximum(jnp.max(scores, axis=0, keepdims=True), NONE)
    high, low = split_pair(peak)
    peak = high + low
    weights = jnp.exp2(scores - peak)
    return weights.astype(BF16), peak, jnp.sum(weights, axis=0, keepdims=True)


def heads_at(base, i):
    return pl.ds(pl.multiple_of((base + i) * 128, 128), 128)


def attend(base, q_ref, k_ref, vt_ref, bias_ref, out_ref):
    scores = [
        dot(k_ref[:, heads_at(base, i)], q_ref[i * 128 : (i + 1) * 128, :], NT) * FACTOR
        + bias_ref[0:512, :]
        for i in range(4)
    ]
    parts = [softened(s) for s in scores]
    outs = [dot(vt_ref[base + i], parts[i][0], NN) for i in range(4)]
    for i, (_, peak, total) in enumerate(parts):
        emit(out_ref, i * 4, outs[i].astype(BF16), state_rows(peak, total))


def emit(out_ref, first, out, state):
    for n in range(4):
        out_ref[first + n, 0:32, :] = out[n * 32 : (n + 1) * 32]
        out_ref[first + n, 32:40, :] = state


def first_body(
    own_ref, came_ref, table_ref, k_ref, vt_ref, bias_ref, out_ref, q_ref, flat_ref
):
    base = (1 - lax.axis_index("c")) * 4
    join(base, own_ref, came_ref, table_ref, q_ref, flat_ref)
    attend(base, q_ref, k_ref, vt_ref, bias_ref, out_ref)


def second_body(
    own_ref, came_ref, table_ref, k_ref, vt_ref, bias_ref, out_ref, q_ref, flat_ref
):
    c, y = lax.axis_index("c"), lax.axis_index("y")
    join(c * 4, own_ref, came_ref, table_ref, q_ref, flat_ref)
    attend(c * 4, q_ref, k_ref, vt_ref, bias_ref, out_ref)

    @pl.when((lax.axis_index("z") == 0) & (lax.axis_index("x") == 0))
    def _():
        chips = rows_of((16, 6 * 16)) * 6 + 4 == lanes((16, 6 * 16))
        rows = pl.ds(pl.multiple_of((c * 4 + y) * 96, 96), 96)
        own, came = [dot(where_one(chips), ref[rows, :], NN) for ref in (own_ref, came_ref)]
        held = [jnp.where(c == core, own, came).astype(BF16) for core in range(2)]
        row, lane = rows_of((64, 128)), lanes((64, 128))
        found = []
        for kind in range(2):
            pick = where_one(lane == kind * 64 + (row % 16) * 4 + row // 16)
            value = jnp.zeros((ROWS, 128), F32)
            for core in range(2):
                columns = dot(pick, held[core], NT).astype(BF16)
                for i in range(4):
                    at = rows_of((ROWS, 128)) * 8 + core * 4 + i
                    value = value + dot(
                        columns[i * 16 : (i + 1) * 16], where_one(lanes((ROWS, 128)) == at), NN
                    )
            if kind == 0:
                value = rotate(value, table_ref[0], table_ref[1])
            found.append(value.astype(BF16))
        scores = dot(found[0], q_ref[heads_at(0, y), :], NT) * FACTOR + bias_ref[512:, :]
        weights, peak, total = softened(scores)
        own = dot(found[1], weights, TN)
        for n in range(4):
            tile = out_ref.at[y * 4 + n]
            out, peaks, totals = merge(
                [tile[0:32, :].astype(F32), own[n * 32 : (n + 1) * 32]],
                *zip(state_of(tile), (peak, total)),
            )
            tile[0:32, :] = out.astype(BF16)
            tile[32:40, :] = state_rows(peaks, totals)


def state_of(ref):
    state = ref[32:40, :].astype(F32)
    return state[0:1] + state[1:2], state[2:3] + state[3:4]


def merge(outs, peaks, totals):
    peak = functools.reduce(jnp.maximum, peaks)
    factors = [jnp.exp2(p - peak) for p in peaks]
    out = sum(o * f for o, f in zip(outs, factors))
    return out, peak, sum(t * f for t, f in zip(totals, factors))


def merged(refs):
    outs = [ref[0:32, :].astype(F32) for ref in refs]
    return merge(outs, *zip(*map(state_of, refs)))


def tiles_of(ref):
    return [ref.at[n] for n in range(ref.shape[0])]


def couple_body(own_ref, came_ref, out_ref):
    for n in range(16):
        out, peak, total = merged([own_ref.at[n], came_ref.at[n]])
        out_ref[n, 0:32, :] = out.astype(BF16)
        out_ref[n, 32:40, :] = state_rows(peak, total)


def merge_body(in_ref, out_ref):
    out, peak, total = merged(tiles_of(in_ref))
    out, state = out.astype(BF16), state_rows(peak, total)
    for d in range(out_ref.shape[0]):
        out_ref[d, 0:32, :] = out
        out_ref[d, 32:40, :] = state


def finish_body(in_ref, out_ref):
    out, _, total = merged(tiles_of(in_ref))
    out = (out / total).astype(BF16)
    for d in range(out_ref.shape[0]):
        out_ref[d] = out


def upright(in_ref, g):
    row = rows_of((128, 128))
    order = where_one((row % 16) * 8 + row // 16 == lanes((128, 128)))
    block = in_ref[g * 4 : (g + 1) * 4].reshape(128, 128)
    return dot(order, block, NT).astype(BF16)


def half_body(in_ref, out_ref):
    for g in range(4):
        block = upright(in_ref, g)
        for i in range(8):
            at = (g * 8 + i) * HD
            out_ref[:, at : at + HD] = block[i * ROWS : (i + 1) * ROWS]


def place_body(in_ref, own_ref, out_hbm, out_ref, sems):
    half = H * HD // 2
    c = lax.axis_index("c")
    mine = pl.ds(pl.multiple_of(c * half, half), half)
    copies = [pltpu.make_async_copy(own_ref, out_hbm.at[:, mine], sems.at[0])]
    copies[0].start()
    half_body(in_ref, out_ref)
    rest = pl.ds(pl.multiple_of((1 - c) * half, half), half)
    copies.append(pltpu.make_async_copy(out_ref, out_hbm.at[:, rest], sems.at[1]))
    copies[1].start()
    for copy in copies:
        copy.wait()


def per_device(
    queries,
    span_keys,
    span_values,
    positions,
    span_segments,
    cache_keys,
    cache_values,
    cache_segments,
):
    shape = jax.ShapeDtypeStruct
    small = (
        queries,
        span_keys.T,
        span_values.T,
        positions,
        span_segments.reshape(1, ROWS),
        cache_segments.reshape(4, 128),
    )
    tiles, positions, span_segments, cache_segments = call(
        pack_body,
        "pack",
        (shape((6 * 128, 128), BF16), *(shape(a.shape, a.dtype) for a in small[3:])),
        *(pltpu.with_memory_space_constraint(a, pltpu.HBM) for a in small),
        specs=[HBM] * 6,
        scratch=[pltpu.VMEM(a.shape, a.dtype) for a in small[:3]] + [pltpu.SemaphoreType.DMA((6,))],
    )
    tiles = exchange(tiles.reshape(-1, 2, 128), CHIPS).reshape(-1, 128)
    came = swap(tiles)
    bias, tables, turned_values = call(
        ready_body,
        "ready",
        (
            shape((512 + ROWS, 128), F32),
            shape((2, ROWS, 128), F32),
            shape((KVH, HD, 512), BF16),
        ),
        positions,
        span_segments,
        cache_segments,
        pltpu.with_memory_space_constraint(cache_values, pltpu.HBM),
        specs=[VMEM] * 3 + [HBM],
        scratch=[pltpu.VMEM((512, KVH * HD), BF16), pltpu.SemaphoreType.DMA],
    )
    message = shape((16, 40, 128), BF16)
    operands = (tiles, came, tables, cache_keys, turned_values, bias)
    scratch = [pltpu.VMEM((4 * 128, HD), BF16), pltpu.VMEM((2, 400, 128), F32)]
    parts = call(first_body, "first", message, *operands, scratch=scratch)
    other = swap(parts)
    parts = call(second_body, "second", message, *operands, scratch=scratch)
    parts = call(couple_body, "couple", message, parts, other)
    parts = exchange(parts, PLANE)
    parts = call(merge_body, "merge", shape((8, 40, 128), BF16), parts)
    parts = exchange(parts, ("z",))
    whole = call(finish_body, "finish", shape((16, 32, 128), BF16), parts)
    whole = exchange(whole, PLANE)
    own = call(half_body, "half", shape((ROWS, H * HD // 2), BF16), whole)
    return call(
        place_body,
        "place",
        shape((ROWS, H * HD), BF16),
        swap(whole),
        own,
        scratch=[pltpu.VMEM((ROWS, H * HD // 2), BF16), pltpu.SemaphoreType.DMA((2,))],
        out_specs=HBM,
    )


def solution(mesh):
    split = Mesh(mesh.devices.reshape(4, 8, 4, 2), ALL)
    return jax.shard_map(
        per_device,
        mesh=split,
        in_specs=(
            P(None, ALL),
            P(None, ALL),
            P(None, ALL),
            P(),
            P(),
            P(ALL, None),
            P(ALL, None),
            P(ALL),
        ),
        out_specs=P(),
        check_vma=False,
    )
```

```python
import functools

import jax
import jax.numpy as jnp
from jax import lax
from jax.experimental import pallas as pl
from jax.experimental.pallas import tpu as pltpu
from jax.sharding import Mesh
from jax.sharding import PartitionSpec as P

H = 64
KVH = 8
HD = 128
ROWS = 16
ALL = ("y", "z", "x", "c")
CHIPS = ("y", "z", "x")
PLANE = ("y", "x")
LOG2E = 1.4426950408889634
NONE = -1e30
HIDDEN = -2e30
F32 = jnp.float32
BF16 = jnp.bfloat16
VMEM = pl.BlockSpec(memory_space=pltpu.VMEM)
NT = (((1,), (1,)), ((), ()))

HBM = pl.BlockSpec(memory_space=pltpu.HBM)


def call(body, name, out_shape, *args, specs=None, scratch=(), limit=8 << 20, out_specs=None):
    return pl.pallas_call(
        body,
        name=name,
        out_shape=out_shape,
        in_specs=specs or [VMEM] * len(args),
        out_specs=out_specs or jax.tree.map(lambda _: VMEM, out_shape),
        scratch_shapes=scratch,
        compiler_params=pltpu.CompilerParams(vmem_limit_bytes=limit),
    )(*args)


def lanes(shape):
    return lax.broadcasted_iota(jnp.int32, shape, len(shape) - 1)


def move(value, by):
    by %= value.shape[-1]
    return pltpu.roll(value, by, value.ndim - 1) if by else value


def exchange(tiles, axes):
    return lax.all_to_all(tiles, axes, 0, 0, tiled=True)


def swap(value):
    return lax.ppermute(value, "c", ((0, 1), (1, 0)))


def rows_of(shape):
    return lax.broadcasted_iota(jnp.int32, shape, 0)


TN = (((0,), (0,)), ((), ()))
NN = (((1,), (0,)), ((), ()))


def dot(a, b, dims):
    return lax.dot_general(a, b, dims, preferred_element_type=F32)


def where_one(hit):
    return jnp.where(hit, 1.0, 0.0).astype(BF16)


def pack_body(*refs):
    out_ref, q_ref, k_ref, v_ref, sems = refs[6], *refs[10:]
    copies = [
        pltpu.make_async_copy(source, target, sems.at[n])
        for n, (source, target) in enumerate(zip(refs[:6], (q_ref, k_ref, v_ref, *refs[7:10])))
    ]
    for copy in copies:
        copy.start()
    wide = where_one(lanes((32, 128)) % 32 == rows_of((32, 128)))
    late = lanes((ROWS, 128)) // 32 == rows_of((ROWS, 128)) // 4
    token = lanes((ROWS, 128)) // 4 - rows_of((ROWS, 128))
    keys, values = where_one(token == 0), where_one(token == 16)
    column = lanes((4, 128)) % 4 == rows_of((4, 128))
    q_rows = where_one(rows_of((48, ROWS)) % 6 == lanes((48, ROWS)) % 4)
    kv_rows = where_one(rows_of((48, 4)) % 6 == 4)
    for copy in copies:
        copy.wait()
    q = jnp.where(late, dot(q_ref[...], wide, NN), 0.0).astype(BF16)
    kv = dot(k_ref[...], keys, NN) + dot(v_ref[...], values, NN)
    kv = jnp.where(column, kv, 0.0).astype(BF16)
    tiles = (dot(q_rows, q, NN) + dot(kv_rows, kv, NN)).astype(BF16)
    for n in range(out_ref.shape[0] // 48):
        out_ref[n * 48 : (n + 1) * 48, :] = tiles


def turn(angle):
    quarter = jnp.floor(angle * 0.6366197723675814 + 0.5)
    rest = angle - quarter * 1.5703125
    rest = rest - quarter * 4.837512969970703e-4
    rest = rest - quarter * 7.549789948768648e-8
    square = rest * rest
    sine = -1.9515295891e-4 * square + 8.3321608736e-3
    sine = (sine * square - 1.6666654611e-1) * square * rest + rest
    cosine = 2.443315711809948e-5 * square - 1.388731625493765e-3
    cosine = (cosine * square + 4.166664568298827e-2) * square * square - 0.5 * square + 1.0
    which = quarter.astype(jnp.int32) % 4
    odd = which % 2 == 1
    cosine, sine = jnp.where(odd, sine, cosine), jnp.where(odd, cosine, sine)
    cosine = jnp.where((which == 1) | (which == 2), -cosine, cosine)
    sine = jnp.where(which >= 2, -sine, sine)
    return cosine, sine


def rope_tables(positions, index):
    section = jnp.where(index < 16, 0, jnp.where(index < 40, 1, 2))
    high = positions // 64
    position = jnp.zeros(index.shape, F32)
    for scale, part in ((64.0, high), (1.0, positions - high * 64)):
        chosen = dot(part.astype(F32).astype(BF16), where_one(rows_of((3, 3 * 128)) == lanes((3, 3 * 128)) // 128), TN)
        picked = chosen[:, 256:]
        for n in range(2):
            picked = jnp.where(section == n, chosen[:, n * 128 : (n + 1) * 128], picked)
        position = position + scale * picked
    inverse = jnp.ones(index.shape, F32)
    for bit in range(6):
        step = 1000000.0 ** (-2.0 * 2**bit / HD)
        inverse = jnp.where((index // 2**bit) % 2 == 1, inverse * step, inverse)
    return turn(position * inverse)


def rotate(value, cosine, sine):
    return value * cosine + move(value, 64) * sine


def split_pair(value):
    high = value.astype(BF16).astype(F32)
    return high, (value - high).astype(BF16).astype(F32)


def state_rows(peak, total):
    row = rows_of((8, 128))
    parts = (*split_pair(peak), *split_pair(total))
    tile = jnp.zeros((8, 128), F32)
    for n, part in enumerate(parts):
        tile = jnp.where(row == n, part, tile)
    return tile.astype(BF16)


def half_of(ref, core):
    half = KVH * HD // 2
    return ref.at[:, pl.ds(pl.multiple_of(core * half, half), half)]


def turn_half(v_ref, vt_ref):
    for i in range(4):
        vt_ref[i] = v_ref[:, i * HD : (i + 1) * HD].T


def ready_body(pos_ref, seg_ref, held_ref, v_hbm, bias_ref, table_ref, vt_ref, v_ref, sem):
    copy = pltpu.make_async_copy(half_of(v_hbm, 1 - lax.axis_index("c")), v_ref, sem)
    copy.start()
    lane = lanes((ROWS, 128))
    cosine, sine = rope_tables(pos_ref[...], lane % 64)
    table_ref[0] = cosine
    table_ref[1] = jnp.where(lane < 64, -sine, sine)
    pick = where_one(rows_of((ROWS, 128)) == lane // 8)
    kinds = where_one(rows_of((8, ROWS)) == seg_ref[...])
    wanted = dot(kinds, pick, NN).astype(BF16)
    for part in range(4):
        have = where_one(rows_of((8, 128)) == held_ref[part : part + 1, :])
        bias_ref[part * 128 : (part + 1) * 128, :] = (dot(have, wanted, TN) - 1.0) * -HIDDEN
    seen = dot(kinds, wanted, TN) * jnp.where(rows_of((ROWS, 128)) <= lane // 8, 1.0, 0.0)
    bias_ref[512:, :] = (seen - 1.0) * -HIDDEN
    copy.wait()
    turn_half(v_ref, vt_ref)


def join(base, own_ref, came_ref, table_ref, q_ref, flat_ref):
    c = lax.axis_index("c")
    shape = (128, 4 * 128)
    source, target = rows_of(shape), lanes(shape)
    rows = pl.ds(pl.multiple_of(base * 96, 384), 384)
    whole = jnp.zeros((128, 512), F32)
    for n, ref in enumerate((own_ref, came_ref)):
        flat_ref[n, 0:384, :] = ref[rows, :].astype(F32)
        for half in range(2):
            part = jnp.concatenate(
                [flat_ref[n, pl.ds(j + 6 * half, 32, stride=12), :] for j in range(4)], axis=0
            )
            core = 1 - c if n else c
            at = (source // 32) * 128 + half * 64 + core * 32 + source % 32
            whole = whole + dot(part.astype(BF16), where_one(target == at), NN)
    for r in range(ROWS):
        high, low = divmod(r, 4)
        part = whole[low * 32 : (low + 1) * 32, high * 128 : (high + 1) * 128]
        part = rotate(part, table_ref[0, r : r + 1, :], table_ref[1, r : r + 1, :]).astype(BF16)
        for i in range(4):
            q_ref[i * 128 + r * 8 : i * 128 + r * 8 + 8, :] = part[i * 8 : (i + 1) * 8]


FACTOR = LOG2E / HD**0.5


def softened(scores):
    peak = jnp.maximum(jnp.max(scores, axis=0, keepdims=True), NONE)
    high, low = split_pair(peak)
    peak = high + low
    weights = jnp.exp2(scores - peak)
    return weights.astype(BF16), peak, jnp.sum(weights, axis=0, keepdims=True)


def heads_at(base, i):
    return pl.ds(pl.multiple_of((base + i) * 128, 128), 128)


def attend(base, q_ref, k_ref, vt_ref, bias_ref, out_ref):
    scores = [
        dot(k_ref[:, heads_at(base, i)], q_ref[i * 128 : (i + 1) * 128, :], NT) * FACTOR
        + bias_ref[0:512, :]
        for i in range(4)
    ]
    parts = [softened(s) for s in scores]
    outs = [dot(vt_ref[i], parts[i][0], NN) for i in range(4)]
    for i, (_, peak, total) in enumerate(parts):
        emit(out_ref, i * 4, outs[i].astype(BF16), state_rows(peak, total))


def emit(out_ref, first, out, state):
    for n in range(4):
        out_ref[first + n, 0:32, :] = out[n * 32 : (n + 1) * 32]
        out_ref[first + n, 32:40, :] = state


def first_body(
    own_ref, came_ref, table_ref, k_ref, vt_ref, bias_ref, v_hbm,
    out_ref, turned_ref, q_ref, flat_ref, v_ref, sem,
):
    copy = pltpu.make_async_copy(half_of(v_hbm, lax.axis_index("c")), v_ref, sem)
    copy.start()
    base = (1 - lax.axis_index("c")) * 4
    join(base, own_ref, came_ref, table_ref, q_ref, flat_ref)
    attend(base, q_ref, k_ref, vt_ref, bias_ref, out_ref)
    copy.wait()
    turn_half(v_ref, turned_ref)


def second_body(
    own_ref, came_ref, table_ref, k_ref, vt_ref, bias_ref, out_ref, q_ref, flat_ref
):
    c, y = lax.axis_index("c"), lax.axis_index("y")
    join(c * 4, own_ref, came_ref, table_ref, q_ref, flat_ref)
    attend(c * 4, q_ref, k_ref, vt_ref, bias_ref, out_ref)

    @pl.when((lax.axis_index("z") == 0) & (lax.axis_index("x") == 0))
    def _():
        chips = rows_of((16, 6 * 16)) * 6 + 4 == lanes((16, 6 * 16))
        rows = pl.ds(pl.multiple_of((c * 4 + y) * 96, 96), 96)
        own, came = [dot(where_one(chips), ref[rows, :], NN) for ref in (own_ref, came_ref)]
        held = [jnp.where(c == core, own, came).astype(BF16) for core in range(2)]
        row, lane = rows_of((64, 128)), lanes((64, 128))
        found = []
        for kind in range(2):
            pick = where_one(lane == kind * 64 + (row % 16) * 4 + row // 16)
            value = jnp.zeros((ROWS, 128), F32)
            for core in range(2):
                columns = dot(pick, held[core], NT).astype(BF16)
                for i in range(4):
                    at = rows_of((ROWS, 128)) * 8 + core * 4 + i
                    value = value + dot(
                        columns[i * 16 : (i + 1) * 16], where_one(lanes((ROWS, 128)) == at), NN
                    )
            if kind == 0:
                value = rotate(value, table_ref[0], table_ref[1])
            found.append(value.astype(BF16))
        scores = dot(found[0], q_ref[heads_at(0, y), :], NT) * FACTOR + bias_ref[512:, :]
        weights, peak, total = softened(scores)
        own = dot(found[1], weights, TN)
        for n in range(4):
            tile = out_ref.at[y * 4 + n]
            out, peaks, totals = merge(
                [tile[0:32, :].astype(F32), own[n * 32 : (n + 1) * 32]],
                *zip(state_of(tile), (peak, total)),
            )
            tile[0:32, :] = out.astype(BF16)
            tile[32:40, :] = state_rows(peaks, totals)


def state_of(ref):
    state = ref[32:40, :].astype(F32)
    return state[0:1] + state[1:2], state[2:3] + state[3:4]


def merge(outs, peaks, totals):
    peak = functools.reduce(jnp.maximum, peaks)
    factors = [jnp.exp2(p - peak) for p in peaks]
    out = sum(o * f for o, f in zip(outs, factors))
    return out, peak, sum(t * f for t, f in zip(totals, factors))


def merged(refs):
    outs = [ref[0:32, :].astype(F32) for ref in refs]
    return merge(outs, *zip(*map(state_of, refs)))


def tiles_of(ref):
    return [ref.at[n] for n in range(ref.shape[0])]


def couple_body(own_ref, came_ref, out_ref):
    for n in range(16):
        out, peak, total = merged([own_ref.at[n], came_ref.at[n]])
        out_ref[n, 0:32, :] = out.astype(BF16)
        out_ref[n, 32:40, :] = state_rows(peak, total)


def merge_body(in_ref, out_ref):
    out, peak, total = merged(tiles_of(in_ref))
    out, state = out.astype(BF16), state_rows(peak, total)
    for d in range(out_ref.shape[0]):
        out_ref[d, 0:32, :] = out
        out_ref[d, 32:40, :] = state


def finish_body(in_ref, out_ref):
    out, _, total = merged(tiles_of(in_ref))
    out_ref[...] = (out / total).astype(BF16)


def pair_body(own_ref, came_ref, out_ref):
    first = lax.axis_index("c") == 0
    own, came = own_ref[...].astype(F32), came_ref[...].astype(F32)
    tiles = (jnp.where(first, own, came).astype(BF16), jnp.where(first, came, own).astype(BF16))
    for d in range(out_ref.shape[0]):
        for n, tile in enumerate(tiles):
            out_ref[d, n * 32 : (n + 1) * 32, :] = tile


def place_body(in_ref, out_hbm, out_ref, sems):
    copies = []
    row = rows_of((128, 128))
    eye = where_one((row % 16) * 8 + row // 16 == lanes((128, 128)))
    for g in range(KVH):
        half, y = divmod(g, 4)
        block = in_ref[y * 4 : (y + 1) * 4, half * 32 : (half + 1) * 32, :].reshape(128, 128)
        block = dot(eye, block, NT).astype(BF16)
        for i in range(8):
            at = (g * 8 + i) * HD
            out_ref[:, at : at + HD] = block[i * ROWS : (i + 1) * ROWS]
        if g % 2:
            part = slice((g - 1) * 8 * HD, (g + 1) * 8 * HD)
            copies.append(
                pltpu.make_async_copy(out_ref.at[:, part], out_hbm.at[:, part], sems.at[g // 2])
            )
            copies[-1].start()
    for copy in copies:
        copy.wait()


def per_device(
    queries,
    span_keys,
    span_values,
    positions,
    span_segments,
    cache_keys,
    cache_values,
    cache_segments,
):
    shape = jax.ShapeDtypeStruct
    small = (
        queries,
        span_keys.T,
        span_values.T,
        positions,
        span_segments.reshape(1, ROWS),
        cache_segments.reshape(4, 128),
    )
    tiles, positions, span_segments, cache_segments = call(
        pack_body,
        "pack",
        (shape((6 * 128, 128), BF16), *(shape(a.shape, a.dtype) for a in small[3:])),
        *(pltpu.with_memory_space_constraint(a, pltpu.HBM) for a in small),
        specs=[HBM] * 6,
        scratch=[pltpu.VMEM(a.shape, a.dtype) for a in small[:3]] + [pltpu.SemaphoreType.DMA((6,))],
    )
    tiles = exchange(tiles.reshape(-1, 2, 128), CHIPS).reshape(-1, 128)
    came = swap(tiles)
    values = pltpu.with_memory_space_constraint(cache_values, pltpu.HBM)
    turned = shape((4, HD, 512), BF16)
    fetched = [pltpu.VMEM((512, 4 * HD), BF16), pltpu.SemaphoreType.DMA]
    bias, tables, other_values = call(
        ready_body,
        "ready",
        (shape((512 + ROWS, 128), F32), shape((2, ROWS, 128), F32), turned),
        positions,
        span_segments,
        cache_segments,
        values,
        specs=[VMEM] * 3 + [HBM],
        scratch=fetched,
    )
    message = shape((16, 40, 128), BF16)
    scratch = [pltpu.VMEM((4 * 128, HD), BF16), pltpu.VMEM((2, 400, 128), F32)]
    parts, own_values = call(
        first_body,
        "first",
        (message, turned),
        *(tiles, came, tables, cache_keys, other_values, bias, values),
        specs=[VMEM] * 6 + [HBM],
        scratch=scratch + fetched,
    )
    other = swap(parts)
    operands = (tiles, came, tables, cache_keys, own_values, bias)
    parts = call(second_body, "second", message, *operands, scratch=scratch)
    parts = call(couple_body, "couple", message, parts, other)
    parts = exchange(parts, PLANE)
    parts = call(merge_body, "merge", shape((8, 40, 128), BF16), parts)
    parts = exchange(parts, ("z",))
    tile = call(finish_body, "finish", shape((32, 128), BF16), parts)
    whole = call(pair_body, "pair", shape((16, 64, 128), BF16), tile, swap(tile))
    whole = exchange(whole, PLANE)
    return call(
        place_body,
        "place",
        shape((ROWS, H * HD), BF16),
        whole,
        scratch=[pltpu.VMEM((ROWS, H * HD), BF16), pltpu.SemaphoreType.DMA((4,))],
        out_specs=HBM,
    )


def solution(mesh):
    split = Mesh(mesh.devices.reshape(4, 8, 4, 2), ALL)
    return jax.shard_map(
        per_device,
        mesh=split,
        in_specs=(
            P(None, ALL),
            P(None, ALL),
            P(None, ALL),
            P(),
            P(),
            P(ALL, None),
            P(ALL, None),
            P(ALL),
        ),
        out_specs=P(),
        check_vma=False,
    )
```

```python
import functools

import jax
import jax.numpy as jnp
from jax import lax
from jax.experimental import pallas as pl
from jax.experimental.pallas import tpu as pltpu
from jax.sharding import Mesh
from jax.sharding import PartitionSpec as P

H = 64
KVH = 8
HD = 128
ROWS = 16
ALL = ("y", "z", "x", "c")
CHIPS = ("y", "z", "x")
PLANE = ("y", "x")
LOG2E = 1.4426950408889634
NONE = -1e30
HIDDEN = -2e30
F32 = jnp.float32
BF16 = jnp.bfloat16
VMEM = pl.BlockSpec(memory_space=pltpu.VMEM)
NT = (((1,), (1,)), ((), ()))

HBM = pl.BlockSpec(memory_space=pltpu.HBM)


def call(body, name, out_shape, *args, specs=None, scratch=(), limit=8 << 20, out_specs=None):
    return pl.pallas_call(
        body,
        name=name,
        out_shape=out_shape,
        in_specs=specs or [VMEM] * len(args),
        out_specs=out_specs or jax.tree.map(lambda _: VMEM, out_shape),
        scratch_shapes=scratch,
        compiler_params=pltpu.CompilerParams(vmem_limit_bytes=limit),
    )(*args)


def lanes(shape):
    return lax.broadcasted_iota(jnp.int32, shape, len(shape) - 1)


def move(value, by):
    by %= value.shape[-1]
    return pltpu.roll(value, by, value.ndim - 1) if by else value


def exchange(tiles, axes):
    return lax.all_to_all(tiles, axes, 0, 0, tiled=True)


def swap(value):
    return lax.ppermute(value, "c", ((0, 1), (1, 0)))


def rows_of(shape):
    return lax.broadcasted_iota(jnp.int32, shape, 0)


TN = (((0,), (0,)), ((), ()))
NN = (((1,), (0,)), ((), ()))


def dot(a, b, dims):
    return lax.dot_general(a, b, dims, preferred_element_type=F32)


def where_one(hit):
    return jnp.where(hit, 1.0, 0.0).astype(BF16)


def pack_body(*refs):
    out_ref, q_ref, k_ref, v_ref, sems = refs[6], *refs[10:]
    copies = [
        pltpu.make_async_copy(source, target, sems.at[n])
        for n, (source, target) in enumerate(zip(refs[:6], (q_ref, k_ref, v_ref, *refs[7:10])))
    ]
    for copy in copies:
        copy.start()
    for copy in copies:
        copy.wait()
    q = dot(q_ref[...], where_one(lanes((32, 128)) % 32 == rows_of((32, 128))), NN)
    q = jnp.where(lanes((ROWS, 128)) // 32 == rows_of((ROWS, 128)) // 4, q, 0.0).astype(BF16)
    token = lanes((ROWS, 128)) // 4 - rows_of((ROWS, 128))
    kv = dot(k_ref[...], where_one(token == 0), NN) + dot(v_ref[...], where_one(token == 16), NN)
    kv = jnp.where(lanes((4, 128)) % 4 == rows_of((4, 128)), kv, 0.0).astype(BF16)
    tiles = dot(where_one(rows_of((48, ROWS)) % 6 == lanes((48, ROWS)) % 4), q, NN)
    tiles = tiles + dot(where_one(rows_of((48, 4)) % 6 == 4), kv, NN)
    tiles = tiles.astype(BF16)
    for n in range(out_ref.shape[0] // 48):
        out_ref[n * 48 : (n + 1) * 48, :] = tiles


def turn(angle):
    quarter = jnp.floor(angle * 0.6366197723675814 + 0.5)
    rest = angle - quarter * 1.5703125
    rest = rest - quarter * 4.837512969970703e-4
    rest = rest - quarter * 7.549789948768648e-8
    square = rest * rest
    sine = -1.9515295891e-4 * square + 8.3321608736e-3
    sine = (sine * square - 1.6666654611e-1) * square * rest + rest
    cosine = 2.443315711809948e-5 * square - 1.388731625493765e-3
    cosine = (cosine * square + 4.166664568298827e-2) * square * square - 0.5 * square + 1.0
    which = quarter.astype(jnp.int32) % 4
    odd = which % 2 == 1
    cosine, sine = jnp.where(odd, sine, cosine), jnp.where(odd, cosine, sine)
    cosine = jnp.where((which == 1) | (which == 2), -cosine, cosine)
    sine = jnp.where(which >= 2, -sine, sine)
    return cosine, sine


def rope_tables(positions, index):
    section = jnp.where(index < 16, 0, jnp.where(index < 40, 1, 2))
    high = positions // 64
    position = jnp.zeros(index.shape, F32)
    for scale, part in ((64.0, high), (1.0, positions - high * 64)):
        chosen = dot(part.astype(F32).astype(BF16), where_one(rows_of((3, 3 * 128)) == lanes((3, 3 * 128)) // 128), TN)
        picked = chosen[:, 256:]
        for n in range(2):
            picked = jnp.where(section == n, chosen[:, n * 128 : (n + 1) * 128], picked)
        position = position + scale * picked
    inverse = jnp.ones(index.shape, F32)
    for bit in range(6):
        step = 1000000.0 ** (-2.0 * 2**bit / HD)
        inverse = jnp.where((index // 2**bit) % 2 == 1, inverse * step, inverse)
    return turn(position * inverse)


def rotate(value, cosine, sine):
    return value * cosine + move(value, 64) * sine


def split_pair(value):
    high = value.astype(BF16).astype(F32)
    return high, (value - high).astype(BF16).astype(F32)


def state_rows(peak, total):
    row = rows_of((8, 128))
    parts = (*split_pair(peak), *split_pair(total))
    tile = jnp.zeros((8, 128), F32)
    for n, part in enumerate(parts):
        tile = jnp.where(row == n, part, tile)
    return tile.astype(BF16)


def ready_body(pos_ref, seg_ref, held_ref, v_hbm, bias_ref, table_ref, vt_ref, v_ref, sem):
    copy = pltpu.make_async_copy(v_hbm, v_ref, sem)
    copy.start()
    lane = lanes((ROWS, 128))
    cosine, sine = rope_tables(pos_ref[...], lane % 64)
    table_ref[0] = cosine
    table_ref[1] = jnp.where(lane < 64, -sine, sine)
    pick = where_one(rows_of((ROWS, 128)) == lane // 8)
    kinds = where_one(rows_of((8, ROWS)) == seg_ref[...])
    wanted = dot(kinds, pick, NN).astype(BF16)
    for part in range(4):
        have = where_one(rows_of((8, 128)) == held_ref[part : part + 1, :])
        bias_ref[part * 128 : (part + 1) * 128, :] = (dot(have, wanted, TN) - 1.0) * -HIDDEN
    seen = dot(kinds, wanted, TN) * jnp.where(rows_of((ROWS, 128)) <= lane // 8, 1.0, 0.0)
    bias_ref[512:, :] = (seen - 1.0) * -HIDDEN
    copy.wait()
    for g in range(KVH):
        vt_ref[g] = v_ref[:, g * HD : (g + 1) * HD].T


def join(own_ref, came_ref, table_ref, q_ref, kv_ref, flat_ref):
    c = lax.axis_index("c")
    shape = (128, 4 * 128)
    source, target = rows_of(shape), lanes(shape)
    whole = jnp.zeros((256, 512), F32)
    for n, ref in enumerate((own_ref, came_ref)):
        flat_ref[n, 0:768, :] = ref[...].astype(F32)
        kv_ref[n] = flat_ref[n, pl.ds(4, 128, stride=6), :]
        for half in range(2):
            part = jnp.concatenate(
                [flat_ref[n, pl.ds(j + 6 * half, 64, stride=12), :] for j in range(4)], axis=0
            )
            core = 1 - c if n else c
            at = (source // 32) * 128 + half * 64 + core * 32 + source % 32
            whole = whole + dot(part.astype(BF16), where_one(target == at), NN)
    for r in range(ROWS):
        high, low = divmod(r, 4)
        part = whole[low * 64 : (low + 1) * 64, high * 128 : (high + 1) * 128]
        part = rotate(part, table_ref[0, r : r + 1, :], table_ref[1, r : r + 1, :]).astype(BF16)
        for g in range(KVH):
            q_ref[g * 128 + r * 8 : g * 128 + r * 8 + 8, :] = part[g * 8 : (g + 1) * 8]


FACTOR = LOG2E / HD**0.5


def softened(scores):
    peak = jnp.maximum(jnp.max(scores, axis=0, keepdims=True), NONE)
    high, low = split_pair(peak)
    peak = high + low
    weights = jnp.exp2(scores - peak)
    return weights.astype(BF16), peak, jnp.sum(weights, axis=0, keepdims=True)


def heads_at(base, i):
    return pl.ds(pl.multiple_of((base + i) * 128, 128), 128)


def attend(base, q_ref, k_ref, vt_ref, bias_ref, out_ref):
    scores = [
        dot(k_ref[:, heads_at(base, i)], q_ref[heads_at(base, i), :], NT) * FACTOR
        + bias_ref[0:512, :]
        for i in range(4)
    ]
    parts = [softened(s) for s in scores]
    outs = [dot(vt_ref[base + i], parts[i][0], NN) for i in range(4)]
    for i, (_, peak, total) in enumerate(parts):
        emit(out_ref, i * 4, outs[i].astype(BF16), state_rows(peak, total))


def emit(out_ref, first, out, state):
    for n in range(4):
        out_ref[first + n, 0:32, :] = out[n * 32 : (n + 1) * 32]
        out_ref[first + n, 32:40, :] = state


def first_body(
    own_ref, came_ref, table_ref, k_ref, vt_ref, bias_ref, out_ref, q_ref, kv_ref, flat_ref
):
    join(own_ref, came_ref, table_ref, q_ref, kv_ref, flat_ref)
    attend((1 - lax.axis_index("c")) * 4, q_ref, k_ref, vt_ref, bias_ref, out_ref)


def second_body(q_ref, k_ref, vt_ref, bias_ref, kv_ref, table_ref, out_ref):
    c, y = lax.axis_index("c"), lax.axis_index("y")
    g = c * 4 + y
    chips = pl.ds(pl.multiple_of(g * 16, 16), 16)
    own, came = kv_ref[0, chips, :], kv_ref[1, chips, :]
    held = [jnp.where(c == core, own, came).astype(BF16) for core in range(2)]
    row, lane = rows_of((64, 128)), lanes((64, 128))
    found = []
    for kind in range(2):
        pick = where_one(lane == kind * 64 + (row % 16) * 4 + row // 16)
        value = jnp.zeros((ROWS, 128), F32)
        for core in range(2):
            columns = dot(pick, held[core], NT).astype(BF16)
            for i in range(4):
                at = rows_of((ROWS, 128)) * 8 + core * 4 + i
                value = value + dot(
                    columns[i * 16 : (i + 1) * 16], where_one(lanes((ROWS, 128)) == at), NN
                )
        if kind == 0:
            value = rotate(value, table_ref[0], table_ref[1])
        found.append(value.astype(BF16))
    scores = dot(found[0], q_ref[heads_at(c * 4, y), :], NT) * FACTOR + bias_ref[512:, :]
    weights, peak, total = softened(scores)
    own = dot(found[1], weights, TN)
    attend(c * 4, q_ref, k_ref, vt_ref, bias_ref, out_ref)

    @pl.when((lax.axis_index("z") == 0) & (lax.axis_index("x") == 0))
    def _():
        for n in range(4):
            tile = out_ref.at[y * 4 + n]
            out, peaks, totals = merge(
                [tile[0:32, :].astype(F32), own[n * 32 : (n + 1) * 32]],
                *zip(state_of(tile), (peak, total)),
            )
            tile[0:32, :] = out.astype(BF16)
            tile[32:40, :] = state_rows(peaks, totals)


def state_of(ref):
    state = ref[32:40, :].astype(F32)
    return state[0:1] + state[1:2], state[2:3] + state[3:4]


def merge(outs, peaks, totals):
    peak = functools.reduce(jnp.maximum, peaks)
    factors = [jnp.exp2(p - peak) for p in peaks]
    out = sum(o * f for o, f in zip(outs, factors))
    return out, peak, sum(t * f for t, f in zip(totals, factors))


def merged(refs):
    outs = [ref[0:32, :].astype(F32) for ref in refs]
    return merge(outs, *zip(*map(state_of, refs)))


def tiles_of(ref):
    return [ref.at[n] for n in range(ref.shape[0])]


def couple_body(own_ref, came_ref, out_ref):
    for n in range(16):
        out, peak, total = merged([own_ref.at[n], came_ref.at[n]])
        out_ref[n, 0:32, :] = out.astype(BF16)
        out_ref[n, 32:40, :] = state_rows(peak, total)


def merge_body(in_ref, out_ref):
    out, peak, total = merged(tiles_of(in_ref))
    out, state = out.astype(BF16), state_rows(peak, total)
    for d in range(out_ref.shape[0]):
        out_ref[d, 0:32, :] = out
        out_ref[d, 32:40, :] = state


def finish_body(in_ref, out_ref):
    out, _, total = merged(tiles_of(in_ref))
    out_ref[...] = (out / total).astype(BF16)


def pair_body(own_ref, came_ref, out_ref):
    first = lax.axis_index("c") == 0
    own, came = own_ref[...].astype(F32), came_ref[...].astype(F32)
    tiles = (jnp.where(first, own, came).astype(BF16), jnp.where(first, came, own).astype(BF16))
    for d in range(out_ref.shape[0]):
        for n, tile in enumerate(tiles):
            out_ref[d, n * 32 : (n + 1) * 32, :] = tile


def place_body(in_ref, out_hbm, out_ref, sems):
    copies = []
    row = rows_of((128, 128))
    eye = where_one((row % 16) * 8 + row // 16 == lanes((128, 128)))
    for g in range(KVH):
        half, y = divmod(g, 4)
        block = in_ref[y * 4 : (y + 1) * 4, half * 32 : (half + 1) * 32, :].reshape(128, 128)
        block = dot(eye, block, NT).astype(BF16)
        for i in range(8):
            at = (g * 8 + i) * HD
            out_ref[:, at : at + HD] = block[i * ROWS : (i + 1) * ROWS]
        if g % 2:
            part = slice((g - 1) * 8 * HD, (g + 1) * 8 * HD)
            copies.append(
                pltpu.make_async_copy(out_ref.at[:, part], out_hbm.at[:, part], sems.at[g // 2])
            )
            copies[-1].start()
    for copy in copies:
        copy.wait()


def per_device(
    queries,
    span_keys,
    span_values,
    positions,
    span_segments,
    cache_keys,
    cache_values,
    cache_segments,
):
    shape = jax.ShapeDtypeStruct
    small = (
        queries,
        span_keys.T,
        span_values.T,
        positions,
        span_segments.reshape(1, ROWS),
        cache_segments.reshape(4, 128),
    )
    tiles, positions, span_segments, cache_segments = call(
        pack_body,
        "pack",
        (shape((6 * 128, 128), BF16), *(shape(a.shape, a.dtype) for a in small[3:])),
        *(pltpu.with_memory_space_constraint(a, pltpu.HBM) for a in small),
        specs=[HBM] * 6,
        scratch=[pltpu.VMEM(a.shape, a.dtype) for a in small[:3]] + [pltpu.SemaphoreType.DMA((6,))],
    )
    tiles = exchange(tiles.reshape(-1, 2, 128), CHIPS).reshape(-1, 128)
    came = swap(tiles)
    bias, tables, turned_values = call(
        ready_body,
        "ready",
        (
            shape((512 + ROWS, 128), F32),
            shape((2, ROWS, 128), F32),
            shape((KVH, HD, 512), BF16),
        ),
        positions,
        span_segments,
        cache_segments,
        pltpu.with_memory_space_constraint(cache_values, pltpu.HBM),
        specs=[VMEM] * 3 + [HBM],
        scratch=[pltpu.VMEM((512, KVH * HD), BF16), pltpu.SemaphoreType.DMA],
    )
    message = shape((16, 40, 128), BF16)
    parts, q, kv = call(
        first_body,
        "first",
        (message, shape((H * ROWS, HD), BF16), shape((2, 128, 128), F32)),
        tiles,
        came,
        tables,
        cache_keys,
        turned_values,
        bias,
        scratch=[pltpu.VMEM((2, 6 * 128 + 16, 128), F32)],
    )
    other = swap(parts)
    parts = call(
        second_body, "second", message, q, cache_keys, turned_values, bias, kv, tables
    )
    parts = call(couple_body, "couple", message, parts, other)
    parts = exchange(parts, PLANE)
    parts = call(merge_body, "merge", shape((8, 40, 128), BF16), parts)
    parts = exchange(parts, ("z",))
    tile = call(finish_body, "finish", shape((32, 128), BF16), parts)
    whole = call(pair_body, "pair", shape((16, 64, 128), BF16), tile, swap(tile))
    whole = exchange(whole, PLANE)
    return call(
        place_body,
        "place",
        shape((ROWS, H * HD), BF16),
        whole,
        scratch=[pltpu.VMEM((ROWS, H * HD), BF16), pltpu.SemaphoreType.DMA((4,))],
        out_specs=HBM,
    )


def solution(mesh):
    split = Mesh(mesh.devices.reshape(4, 8, 4, 2), ALL)
    return jax.shard_map(
        per_device,
        mesh=split,
        in_specs=(
            P(None, ALL),
            P(None, ALL),
            P(None, ALL),
            P(),
            P(),
            P(ALL, None),
            P(ALL, None),
            P(ALL),
        ),
        out_specs=P(),
        check_vma=False,
    )
```

```python
import functools

import jax
import jax.numpy as jnp
from jax import lax
from jax.experimental import pallas as pl
from jax.experimental.pallas import tpu as pltpu
from jax.sharding import Mesh
from jax.sharding import PartitionSpec as P

H = 64
KVH = 8
HD = 128
ROWS = 16
ALL = ("y", "z", "x", "c")
CHIPS = ("y", "z", "x")
PLANE = ("y", "x")
LOG2E = 1.4426950408889634
NONE = -1e30
HIDDEN = -2e30
F32 = jnp.float32
BF16 = jnp.bfloat16
VMEM = pl.BlockSpec(memory_space=pltpu.VMEM)
NT = (((1,), (1,)), ((), ()))

HBM = pl.BlockSpec(memory_space=pltpu.HBM)


def call(body, name, out_shape, *args, specs=None, scratch=(), limit=8 << 20, out_specs=None):
    return pl.pallas_call(
        body,
        name=name,
        out_shape=out_shape,
        in_specs=specs or [VMEM] * len(args),
        out_specs=out_specs or jax.tree.map(lambda _: VMEM, out_shape),
        scratch_shapes=scratch,
        compiler_params=pltpu.CompilerParams(vmem_limit_bytes=limit),
    )(*args)


def lanes(shape):
    return lax.broadcasted_iota(jnp.int32, shape, len(shape) - 1)


def move(value, by):
    by %= value.shape[-1]
    return pltpu.roll(value, by, value.ndim - 1) if by else value


def exchange(tiles, axes):
    return lax.all_to_all(tiles, axes, 0, 0, tiled=True)


def swap(value):
    return lax.ppermute(value, "c", ((0, 1), (1, 0)))


def rows_of(shape):
    return lax.broadcasted_iota(jnp.int32, shape, 0)


TN = (((0,), (0,)), ((), ()))
NN = (((1,), (0,)), ((), ()))


def dot(a, b, dims):
    return lax.dot_general(a, b, dims, preferred_element_type=F32)


def where_one(hit):
    return jnp.where(hit, 1.0, 0.0).astype(BF16)


def pack_body(*refs):
    out_ref, q_ref, k_ref, v_ref, sems = refs[6], *refs[10:]
    copies = [
        pltpu.make_async_copy(source, target, sems.at[n])
        for n, (source, target) in enumerate(zip(refs[:6], (q_ref, k_ref, v_ref, *refs[7:10])))
    ]
    for copy in copies:
        copy.start()
    for copy in copies:
        copy.wait()
    q = dot(q_ref[...], where_one(lanes((32, 128)) % 32 == rows_of((32, 128))), NN)
    q = jnp.where(lanes((ROWS, 128)) // 32 == rows_of((ROWS, 128)) // 4, q, 0.0).astype(BF16)
    token = lanes((ROWS, 128)) // 4 - rows_of((ROWS, 128))
    kv = dot(k_ref[...], where_one(token == 0), NN) + dot(v_ref[...], where_one(token == 16), NN)
    kv = jnp.where(lanes((4, 128)) % 4 == rows_of((4, 128)), kv, 0.0).astype(BF16)
    tiles = dot(where_one(rows_of((48, ROWS)) % 6 == lanes((48, ROWS)) % 4), q, NN)
    tiles = tiles + dot(where_one(rows_of((48, 4)) % 6 == 4), kv, NN)
    tiles = tiles.astype(BF16)
    for n in range(out_ref.shape[0] // 48):
        out_ref[n * 48 : (n + 1) * 48, :] = tiles


def turn(angle):
    quarter = jnp.floor(angle * 0.6366197723675814 + 0.5)
    rest = angle - quarter * 1.5703125
    rest = rest - quarter * 4.837512969970703e-4
    rest = rest - quarter * 7.549789948768648e-8
    square = rest * rest
    sine = -1.9515295891e-4 * square + 8.3321608736e-3
    sine = (sine * square - 1.6666654611e-1) * square * rest + rest
    cosine = 2.443315711809948e-5 * square - 1.388731625493765e-3
    cosine = (cosine * square + 4.166664568298827e-2) * square * square - 0.5 * square + 1.0
    which = quarter.astype(jnp.int32) % 4
    odd = which % 2 == 1
    cosine, sine = jnp.where(odd, sine, cosine), jnp.where(odd, cosine, sine)
    cosine = jnp.where((which == 1) | (which == 2), -cosine, cosine)
    sine = jnp.where(which >= 2, -sine, sine)
    return cosine, sine


def rope_tables(positions, index):
    section = jnp.where(index < 16, 0, jnp.where(index < 40, 1, 2))
    high = positions // 64
    position = jnp.zeros(index.shape, F32)
    for scale, part in ((64.0, high), (1.0, positions - high * 64)):
        chosen = dot(part.astype(F32).astype(BF16), where_one(rows_of((3, 3 * 128)) == lanes((3, 3 * 128)) // 128), TN)
        picked = chosen[:, 256:]
        for n in range(2):
            picked = jnp.where(section == n, chosen[:, n * 128 : (n + 1) * 128], picked)
        position = position + scale * picked
    inverse = jnp.ones(index.shape, F32)
    for bit in range(6):
        step = 1000000.0 ** (-2.0 * 2**bit / HD)
        inverse = jnp.where((index // 2**bit) % 2 == 1, inverse * step, inverse)
    return turn(position * inverse)


def rotate(value, cosine, sine):
    return value * cosine + move(value, 64) * sine


def split_pair(value):
    high = value.astype(BF16).astype(F32)
    return high, (value - high).astype(BF16).astype(F32)


def state_rows(peak, total):
    row = rows_of((8, 128))
    parts = (*split_pair(peak), *split_pair(total))
    tile = jnp.zeros((8, 128), F32)
    for n, part in enumerate(parts):
        tile = jnp.where(row == n, part, tile)
    return tile.astype(BF16)


def span_columns(ref, core, cosine, sine):
    g = lax.axis_index("c") * 4 + lax.axis_index("y")
    chips = where_one(rows_of((16, 96)) * 6 + 4 == lanes((16, 96)))
    held = dot(chips, ref[pl.ds(pl.multiple_of(g * 96, 96), 96), :], NN).astype(BF16)
    row, lane = rows_of((64, 128)), lanes((64, 128))
    found = []
    for kind in range(2):
        pick = where_one(lane == kind * 64 + (row % 16) * 4 + row // 16)
        columns = dot(pick, held, NT).astype(BF16)
        value = jnp.zeros((ROWS, 128), F32)
        for i in range(4):
            at = rows_of((ROWS, 128)) * 8 + core * 4 + i
            value = value + dot(
                columns[i * 16 : (i + 1) * 16], where_one(lanes((ROWS, 128)) == at), NN
            )
        found.append(value if kind else rotate(value, cosine, sine))
    return found


def ready_body(
    pos_ref, seg_ref, held_ref, own_ref, v_hbm, bias_ref, table_ref, span_ref, vt_ref, v_ref, sem
):
    copy = pltpu.make_async_copy(v_hbm, v_ref, sem)
    copy.start()
    lane = lanes((ROWS, 128))
    cosine, sine = rope_tables(pos_ref[...], lane % 64)
    table_ref[0] = cosine
    table_ref[1] = jnp.where(lane < 64, -sine, sine)
    pick = where_one(rows_of((ROWS, 128)) == lane // 8)
    kinds = where_one(rows_of((8, ROWS)) == seg_ref[...])
    wanted = dot(kinds, pick, NN).astype(BF16)
    for part in range(4):
        have = where_one(rows_of((8, 128)) == held_ref[part : part + 1, :])
        bias_ref[part * 128 : (part + 1) * 128, :] = (dot(have, wanted, TN) - 1.0) * -HIDDEN
    seen = dot(kinds, wanted, TN) * jnp.where(rows_of((ROWS, 128)) <= lane // 8, 1.0, 0.0)
    bias_ref[512:, :] = (seen - 1.0) * -HIDDEN
    for n, part in enumerate(
        span_columns(own_ref, lax.axis_index("c"), cosine, jnp.where(lane < 64, -sine, sine))
    ):
        span_ref[n] = part
    copy.wait()
    for g in range(KVH):
        vt_ref[g] = v_ref[:, g * HD : (g + 1) * HD].T


def join(own_ref, came_ref, table_ref, q_ref, flat_ref):
    c = lax.axis_index("c")
    shape = (128, 4 * 128)
    source, target = rows_of(shape), lanes(shape)
    whole = jnp.zeros((256, 512), F32)
    for n, ref in enumerate((own_ref, came_ref)):
        flat_ref[n, 0:768, :] = ref[...].astype(F32)
        for half in range(2):
            part = jnp.concatenate(
                [flat_ref[n, pl.ds(j + 6 * half, 64, stride=12), :] for j in range(4)], axis=0
            )
            core = 1 - c if n else c
            at = (source // 32) * 128 + half * 64 + core * 32 + source % 32
            whole = whole + dot(part.astype(BF16), where_one(target == at), NN)
    for r in range(ROWS):
        high, low = divmod(r, 4)
        part = whole[low * 64 : (low + 1) * 64, high * 128 : (high + 1) * 128]
        part = rotate(part, table_ref[0, r : r + 1, :], table_ref[1, r : r + 1, :]).astype(BF16)
        for g in range(KVH):
            q_ref[g * 128 + r * 8 : g * 128 + r * 8 + 8, :] = part[g * 8 : (g + 1) * 8]


FACTOR = LOG2E / HD**0.5


def softened(scores):
    peak = jnp.maximum(jnp.max(scores, axis=0, keepdims=True), NONE)
    high, low = split_pair(peak)
    peak = high + low
    weights = jnp.exp2(scores - peak)
    return weights.astype(BF16), peak, jnp.sum(weights, axis=0, keepdims=True)


def heads_at(base, i):
    return pl.ds(pl.multiple_of((base + i) * 128, 128), 128)


def attend(base, q_ref, k_ref, vt_ref, bias_ref, out_ref):
    scores = [
        dot(k_ref[:, heads_at(base, i)], q_ref[heads_at(base, i), :], NT) * FACTOR
        + bias_ref[0:512, :]
        for i in range(4)
    ]
    parts = [softened(s) for s in scores]
    outs = [dot(vt_ref[base + i], parts[i][0], NN) for i in range(4)]
    for i, (_, peak, total) in enumerate(parts):
        emit(out_ref, i * 4, outs[i].astype(BF16), state_rows(peak, total))


def emit(out_ref, first, out, state):
    for n in range(4):
        out_ref[first + n, 0:32, :] = out[n * 32 : (n + 1) * 32]
        out_ref[first + n, 32:40, :] = state


def first_body(
    own_ref, came_ref, table_ref, k_ref, vt_ref, bias_ref, out_ref, q_ref, flat_ref
):
    join(own_ref, came_ref, table_ref, q_ref, flat_ref)
    attend((1 - lax.axis_index("c")) * 4, q_ref, k_ref, vt_ref, bias_ref, out_ref)


def second_body(q_ref, k_ref, vt_ref, bias_ref, came_ref, span_ref, table_ref, out_ref):
    c, y = lax.axis_index("c"), lax.axis_index("y")
    attend(c * 4, q_ref, k_ref, vt_ref, bias_ref, out_ref)

    @pl.when((lax.axis_index("z") == 0) & (lax.axis_index("x") == 0))
    def _():
        found = [
            (span_ref[n] + part).astype(BF16)
            for n, part in enumerate(span_columns(came_ref, 1 - c, table_ref[0], table_ref[1]))
        ]
        scores = dot(found[0], q_ref[heads_at(c * 4, y), :], NT) * FACTOR + bias_ref[512:, :]
        weights, peak, total = softened(scores)
        own = dot(found[1], weights, TN)
        for n in range(4):
            tile = out_ref.at[y * 4 + n]
            out, peaks, totals = merge(
                [tile[0:32, :].astype(F32), own[n * 32 : (n + 1) * 32]],
                *zip(state_of(tile), (peak, total)),
            )
            tile[0:32, :] = out.astype(BF16)
            tile[32:40, :] = state_rows(peaks, totals)


def state_of(ref):
    state = ref[32:40, :].astype(F32)
    return state[0:1] + state[1:2], state[2:3] + state[3:4]


def merge(outs, peaks, totals):
    peak = functools.reduce(jnp.maximum, peaks)
    factors = [jnp.exp2(p - peak) for p in peaks]
    out = sum(o * f for o, f in zip(outs, factors))
    return out, peak, sum(t * f for t, f in zip(totals, factors))


def merged(refs):
    outs = [ref[0:32, :].astype(F32) for ref in refs]
    return merge(outs, *zip(*map(state_of, refs)))


def tiles_of(ref):
    return [ref.at[n] for n in range(ref.shape[0])]


def couple_body(own_ref, came_ref, out_ref):
    for n in range(16):
        out, peak, total = merged([own_ref.at[n], came_ref.at[n]])
        out_ref[n, 0:32, :] = out.astype(BF16)
        out_ref[n, 32:40, :] = state_rows(peak, total)


def merge_body(in_ref, out_ref):
    out, peak, total = merged(tiles_of(in_ref))
    out, state = out.astype(BF16), state_rows(peak, total)
    for d in range(out_ref.shape[0]):
        out_ref[d, 0:32, :] = out
        out_ref[d, 32:40, :] = state


def finish_body(in_ref, out_ref):
    out, _, total = merged(tiles_of(in_ref))
    out_ref[...] = (out / total).astype(BF16)


def pair_body(own_ref, came_ref, out_ref):
    first = lax.axis_index("c") == 0
    own, came = own_ref[...].astype(F32), came_ref[...].astype(F32)
    tiles = (jnp.where(first, own, came).astype(BF16), jnp.where(first, came, own).astype(BF16))
    for d in range(out_ref.shape[0]):
        for n, tile in enumerate(tiles):
            out_ref[d, n * 32 : (n + 1) * 32, :] = tile


def place_body(in_ref, out_hbm, out_ref, sems):
    copies = []
    row = rows_of((128, 128))
    eye = where_one((row % 16) * 8 + row // 16 == lanes((128, 128)))
    for g in range(KVH):
        half, y = divmod(g, 4)
        block = in_ref[y * 4 : (y + 1) * 4, half * 32 : (half + 1) * 32, :].reshape(128, 128)
        block = dot(eye, block, NT).astype(BF16)
        for i in range(8):
            at = (g * 8 + i) * HD
            out_ref[:, at : at + HD] = block[i * ROWS : (i + 1) * ROWS]
        if g % 2:
            part = slice((g - 1) * 8 * HD, (g + 1) * 8 * HD)
            copies.append(
                pltpu.make_async_copy(out_ref.at[:, part], out_hbm.at[:, part], sems.at[g // 2])
            )
            copies[-1].start()
    for copy in copies:
        copy.wait()


def per_device(
    queries,
    span_keys,
    span_values,
    positions,
    span_segments,
    cache_keys,
    cache_values,
    cache_segments,
):
    shape = jax.ShapeDtypeStruct
    small = (
        queries,
        span_keys.T,
        span_values.T,
        positions,
        span_segments.reshape(1, ROWS),
        cache_segments.reshape(4, 128),
    )
    tiles, positions, span_segments, cache_segments = call(
        pack_body,
        "pack",
        (shape((6 * 128, 128), BF16), *(shape(a.shape, a.dtype) for a in small[3:])),
        *(pltpu.with_memory_space_constraint(a, pltpu.HBM) for a in small),
        specs=[HBM] * 6,
        scratch=[pltpu.VMEM(a.shape, a.dtype) for a in small[:3]] + [pltpu.SemaphoreType.DMA((6,))],
    )
    tiles = exchange(tiles.reshape(-1, 2, 128), CHIPS).reshape(-1, 128)
    came = swap(tiles)
    bias, tables, span, turned_values = call(
        ready_body,
        "ready",
        (
            shape((512 + ROWS, 128), F32),
            shape((2, ROWS, 128), F32),
            shape((2, ROWS, 128), F32),
            shape((KVH, HD, 512), BF16),
        ),
        positions,
        span_segments,
        cache_segments,
        tiles,
        pltpu.with_memory_space_constraint(cache_values, pltpu.HBM),
        specs=[VMEM] * 4 + [HBM],
        scratch=[pltpu.VMEM((512, KVH * HD), BF16), pltpu.SemaphoreType.DMA],
    )
    message = shape((16, 40, 128), BF16)
    parts, q = call(
        first_body,
        "first",
        (message, shape((H * ROWS, HD), BF16)),
        tiles,
        came,
        tables,
        cache_keys,
        turned_values,
        bias,
        scratch=[pltpu.VMEM((2, 6 * 128 + 16, 128), F32)],
    )
    other = swap(parts)
    parts = call(
        second_body, "second", message, q, cache_keys, turned_values, bias, came, span, tables
    )
    parts = call(couple_body, "couple", message, parts, other)
    parts = exchange(parts, PLANE)
    parts = call(merge_body, "merge", shape((8, 40, 128), BF16), parts)
    parts = exchange(parts, ("z",))
    tile = call(finish_body, "finish", shape((32, 128), BF16), parts)
    whole = call(pair_body, "pair", shape((16, 64, 128), BF16), tile, swap(tile))
    whole = exchange(whole, PLANE)
    return call(
        place_body,
        "place",
        shape((ROWS, H * HD), BF16),
        whole,
        scratch=[pltpu.VMEM((ROWS, H * HD), BF16), pltpu.SemaphoreType.DMA((4,))],
        out_specs=HBM,
    )


def solution(mesh):
    split = Mesh(mesh.devices.reshape(4, 8, 4, 2), ALL)
    return jax.shard_map(
        per_device,
        mesh=split,
        in_specs=(
            P(None, ALL),
            P(None, ALL),
            P(None, ALL),
            P(),
            P(),
            P(ALL, None),
            P(ALL, None),
            P(ALL),
        ),
        out_specs=P(),
        check_vma=False,
    )
```

```python
import functools

import jax
import jax.numpy as jnp
from jax import lax
from jax.experimental import pallas as pl
from jax.experimental.pallas import tpu as pltpu
from jax.sharding import Mesh
from jax.sharding import PartitionSpec as P

H = 64
KVH = 8
HD = 128
ROWS = 16
ALL = ("y", "z", "x", "c")
CHIPS = ("y", "z", "x")
PLANE = ("x", "y")
LOG2E = 1.4426950408889634
NONE = -1e30
HIDDEN = -2e30
F32 = jnp.float32
BF16 = jnp.bfloat16
VMEM = pl.BlockSpec(memory_space=pltpu.VMEM)
NT = (((1,), (1,)), ((), ()))

HBM = pl.BlockSpec(memory_space=pltpu.HBM)


def call(body, name, out_shape, *args, specs=None, scratch=(), limit=8 << 20, out_specs=None):
    return pl.pallas_call(
        body,
        name=name,
        out_shape=out_shape,
        in_specs=specs or [VMEM] * len(args),
        out_specs=out_specs or jax.tree.map(lambda _: VMEM, out_shape),
        scratch_shapes=scratch,
        compiler_params=pltpu.CompilerParams(vmem_limit_bytes=limit),
    )(*args)


def lanes(shape):
    return lax.broadcasted_iota(jnp.int32, shape, len(shape) - 1)


def move(value, by):
    by %= value.shape[-1]
    return pltpu.roll(value, by, value.ndim - 1) if by else value


def exchange(tiles, axes):
    return lax.all_to_all(tiles, axes, 0, 0, tiled=True)


def swap(value):
    return lax.ppermute(value, "c", ((0, 1), (1, 0)))


def rows_of(shape):
    return lax.broadcasted_iota(jnp.int32, shape, 0)


TN = (((0,), (0,)), ((), ()))
NN = (((1,), (0,)), ((), ()))


def dot(a, b, dims):
    return lax.dot_general(a, b, dims, preferred_element_type=F32)


def where_one(hit):
    return jnp.where(hit, 1.0, 0.0).astype(BF16)


def pack_body(*refs):
    out_ref, q_ref, k_ref, v_ref, sems = refs[6], *refs[10:]
    copies = [
        pltpu.make_async_copy(source, target, sems.at[n])
        for n, (source, target) in enumerate(zip(refs[:6], (q_ref, k_ref, v_ref, *refs[7:10])))
    ]
    for copy in copies:
        copy.start()
    for copy in copies:
        copy.wait()
    q = dot(q_ref[...], where_one(lanes((32, 128)) % 32 == rows_of((32, 128))), NN)
    q = jnp.where(lanes((ROWS, 128)) // 32 == rows_of((ROWS, 128)) // 4, q, 0.0).astype(BF16)
    token = lanes((ROWS, 128)) // 4 - rows_of((ROWS, 128))
    kv = dot(k_ref[...], where_one(token == 0), NN) + dot(v_ref[...], where_one(token == 16), NN)
    kv = jnp.where(lanes((4, 128)) % 4 == rows_of((4, 128)), kv, 0.0).astype(BF16)
    tiles = dot(where_one(rows_of((48, ROWS)) % 6 == lanes((48, ROWS)) % 4), q, NN)
    tiles = tiles + dot(where_one(rows_of((48, 4)) % 6 == 4), kv, NN)
    tiles = tiles.astype(BF16)
    for n in range(out_ref.shape[0] // 48):
        out_ref[n * 48 : (n + 1) * 48, :] = tiles


def turn(angle):
    quarter = jnp.floor(angle * 0.6366197723675814 + 0.5)
    rest = angle - quarter * 1.5703125
    rest = rest - quarter * 4.837512969970703e-4
    rest = rest - quarter * 7.549789948768648e-8
    square = rest * rest
    sine = -1.9515295891e-4 * square + 8.3321608736e-3
    sine = (sine * square - 1.6666654611e-1) * square * rest + rest
    cosine = 2.443315711809948e-5 * square - 1.388731625493765e-3
    cosine = (cosine * square + 4.166664568298827e-2) * square * square - 0.5 * square + 1.0
    which = quarter.astype(jnp.int32) % 4
    odd = which % 2 == 1
    cosine, sine = jnp.where(odd, sine, cosine), jnp.where(odd, cosine, sine)
    cosine = jnp.where((which == 1) | (which == 2), -cosine, cosine)
    sine = jnp.where(which >= 2, -sine, sine)
    return cosine, sine


def rope_tables(positions, index):
    section = jnp.where(index < 16, 0, jnp.where(index < 40, 1, 2))
    high = positions // 64
    position = jnp.zeros(index.shape, F32)
    for scale, part in ((64.0, high), (1.0, positions - high * 64)):
        chosen = dot(part.astype(F32).astype(BF16), where_one(rows_of((3, 3 * 128)) == lanes((3, 3 * 128)) // 128), TN)
        picked = chosen[:, 256:]
        for n in range(2):
            picked = jnp.where(section == n, chosen[:, n * 128 : (n + 1) * 128], picked)
        position = position + scale * picked
    inverse = jnp.ones(index.shape, F32)
    for bit in range(6):
        step = 1000000.0 ** (-2.0 * 2**bit / HD)
        inverse = jnp.where((index // 2**bit) % 2 == 1, inverse * step, inverse)
    return turn(position * inverse)


def rotate(value, cosine, sine):
    return value * cosine + move(value, 64) * sine


def split_pair(value):
    high = value.astype(BF16).astype(F32)
    return high, (value - high).astype(BF16).astype(F32)


def state_rows(peak, total):
    row = rows_of((8, 128))
    parts = (*split_pair(peak), *split_pair(total))
    tile = jnp.zeros((8, 128), F32)
    for n, part in enumerate(parts):
        tile = jnp.where(row == n, part, tile)
    return tile.astype(BF16)


def ready_body(pos_ref, seg_ref, held_ref, v_hbm, bias_ref, table_ref, vt_ref, v_ref, sem):
    copy = pltpu.make_async_copy(v_hbm, v_ref, sem)
    copy.start()
    lane = lanes((ROWS, 128))
    cosine, sine = rope_tables(pos_ref[...], lane % 64)
    table_ref[0] = cosine
    table_ref[1] = jnp.where(lane < 64, -sine, sine)
    pick = where_one(rows_of((ROWS, 128)) == lane // 8)
    kinds = where_one(rows_of((8, ROWS)) == seg_ref[...])
    wanted = dot(kinds, pick, NN).astype(BF16)
    for part in range(4):
        have = where_one(rows_of((8, 128)) == held_ref[part : part + 1, :])
        bias_ref[part * 128 : (part + 1) * 128, :] = (dot(have, wanted, TN) - 1.0) * -HIDDEN
    seen = dot(kinds, wanted, TN) * jnp.where(rows_of((ROWS, 128)) <= lane // 8, 1.0, 0.0)
    bias_ref[512:, :] = (seen - 1.0) * -HIDDEN
    copy.wait()
    for g in range(KVH):
        vt_ref[g] = v_ref[:, g * HD : (g + 1) * HD].T


def join(own_ref, came_ref, table_ref, q_ref, kv_ref, flat_ref):
    c = lax.axis_index("c")
    shape = (128, 4 * 128)
    source, target = rows_of(shape), lanes(shape)
    whole = jnp.zeros((256, 512), F32)
    for n, ref in enumerate((own_ref, came_ref)):
        flat_ref[n, 0:768, :] = ref[...].astype(F32)
        kv_ref[n] = flat_ref[n, pl.ds(4, 128, stride=6), :]
        for half in range(2):
            part = jnp.concatenate(
                [flat_ref[n, pl.ds(j + 6 * half, 64, stride=12), :] for j in range(4)], axis=0
            )
            core = 1 - c if n else c
            at = (source // 32) * 128 + half * 64 + core * 32 + source % 32
            whole = whole + dot(part.astype(BF16), where_one(target == at), NN)
    for r in range(ROWS):
        high, low = divmod(r, 4)
        part = whole[low * 64 : (low + 1) * 64, high * 128 : (high + 1) * 128]
        part = rotate(part, table_ref[0, r : r + 1, :], table_ref[1, r : r + 1, :]).astype(BF16)
        for g in range(KVH):
            q_ref[g * 128 + r * 8 : g * 128 + r * 8 + 8, :] = part[g * 8 : (g + 1) * 8]


FACTOR = LOG2E / HD**0.5


def softened(scores):
    peak = jnp.maximum(jnp.max(scores, axis=0, keepdims=True), NONE)
    high, low = split_pair(peak)
    peak = high + low
    weights = jnp.exp2(scores - peak)
    return weights.astype(BF16), peak, jnp.sum(weights, axis=0, keepdims=True)


def heads_at(base, i):
    return pl.ds(pl.multiple_of((base + i) * 128, 128), 128)


def attend(base, q_ref, k_ref, vt_ref, bias_ref, out_ref):
    scores = [
        dot(k_ref[:, heads_at(base, i)], q_ref[heads_at(base, i), :], NT) * FACTOR
        + bias_ref[0:512, :]
        for i in range(4)
    ]
    parts = [softened(s) for s in scores]
    outs = [dot(vt_ref[base + i], parts[i][0], NN) for i in range(4)]
    for i, (_, peak, total) in enumerate(parts):
        emit(out_ref, i * 4, outs[i].astype(BF16), state_rows(peak, total))


def emit(out_ref, first, out, state):
    for n in range(4):
        out_ref[first + n, 0:32, :] = out[n * 32 : (n + 1) * 32]
        out_ref[first + n, 32:40, :] = state


def first_body(
    own_ref, came_ref, table_ref, k_ref, vt_ref, bias_ref, out_ref, q_ref, kv_ref, flat_ref
):
    join(own_ref, came_ref, table_ref, q_ref, kv_ref, flat_ref)
    attend((1 - lax.axis_index("c")) * 4, q_ref, k_ref, vt_ref, bias_ref, out_ref)


def second_body(q_ref, k_ref, vt_ref, bias_ref, kv_ref, table_ref, out_ref):
    c, y = lax.axis_index("c"), lax.axis_index("y")
    attend(c * 4, q_ref, k_ref, vt_ref, bias_ref, out_ref)

    @pl.when((lax.axis_index("z") == 0) & (lax.axis_index("x") == 0))
    def _():
        g = c * 4 + y
        chips = pl.ds(pl.multiple_of(g * 16, 16), 16)
        own, came = kv_ref[0, chips, :], kv_ref[1, chips, :]
        held = [jnp.where(c == core, own, came).astype(BF16) for core in range(2)]
        row, lane = rows_of((64, 128)), lanes((64, 128))
        found = []
        for kind in range(2):
            pick = where_one(lane == kind * 64 + (row % 16) * 4 + row // 16)
            value = jnp.zeros((ROWS, 128), F32)
            for core in range(2):
                columns = dot(pick, held[core], NT).astype(BF16)
                for i in range(4):
                    at = rows_of((ROWS, 128)) * 8 + core * 4 + i
                    value = value + dot(
                        columns[i * 16 : (i + 1) * 16], where_one(lanes((ROWS, 128)) == at), NN
                    )
            if kind == 0:
                value = rotate(value, table_ref[0], table_ref[1])
            found.append(value.astype(BF16))
        scores = dot(found[0], q_ref[heads_at(c * 4, y), :], NT) * FACTOR + bias_ref[512:, :]
        weights, peak, total = softened(scores)
        own = dot(found[1], weights, TN)
        for n in range(4):
            tile = out_ref.at[y * 4 + n]
            out, peaks, totals = merge(
                [tile[0:32, :].astype(F32), own[n * 32 : (n + 1) * 32]],
                *zip(state_of(tile), (peak, total)),
            )
            tile[0:32, :] = out.astype(BF16)
            tile[32:40, :] = state_rows(peaks, totals)


def state_of(ref):
    state = ref[32:40, :].astype(F32)
    return state[0:1] + state[1:2], state[2:3] + state[3:4]


def merge(outs, peaks, totals):
    peak = functools.reduce(jnp.maximum, peaks)
    factors = [jnp.exp2(p - peak) for p in peaks]
    out = sum(o * f for o, f in zip(outs, factors))
    return out, peak, sum(t * f for t, f in zip(totals, factors))


def merged(refs):
    outs = [ref[0:32, :].astype(F32) for ref in refs]
    return merge(outs, *zip(*map(state_of, refs)))


def tiles_of(ref):
    return [ref.at[n] for n in range(ref.shape[0])]


def couple_body(own_ref, came_ref, out_ref):
    for n in range(16):
        out, peak, total = merged([own_ref.at[n], came_ref.at[n]])
        out_ref[n, 0:32, :] = out.astype(BF16)
        out_ref[n, 32:40, :] = state_rows(peak, total)


def merge_body(in_ref, out_ref):
    out, peak, total = merged(tiles_of(in_ref))
    out, state = out.astype(BF16), state_rows(peak, total)
    for d in range(out_ref.shape[0]):
        out_ref[d, 0:32, :] = out
        out_ref[d, 32:40, :] = state


def finish_body(in_ref, out_ref):
    out, _, total = merged(tiles_of(in_ref))
    out_ref[...] = (out / total).astype(BF16)


def pair_body(own_ref, came_ref, out_ref):
    first = lax.axis_index("c") == 0
    own, came = own_ref[...].astype(F32), came_ref[...].astype(F32)
    tiles = (jnp.where(first, own, came).astype(BF16), jnp.where(first, came, own).astype(BF16))
    for d in range(out_ref.shape[0]):
        for n, tile in enumerate(tiles):
            out_ref[d, n * 32 : (n + 1) * 32, :] = tile


def place_body(in_ref, out_hbm, out_ref, sems):
    copies = []
    row = rows_of((128, 128))
    eye = where_one((row % 16) * 8 + row // 16 == lanes((128, 128)))
    for g in range(KVH):
        half, y = divmod(g, 4)
        block = in_ref[y * 4 : (y + 1) * 4, half * 32 : (half + 1) * 32, :].reshape(128, 128)
        block = dot(eye, block, NT).astype(BF16)
        for i in range(8):
            at = (g * 8 + i) * HD
            out_ref[:, at : at + HD] = block[i * ROWS : (i + 1) * ROWS]
        if g % 2:
            part = slice((g - 1) * 8 * HD, (g + 1) * 8 * HD)
            copies.append(
                pltpu.make_async_copy(out_ref.at[:, part], out_hbm.at[:, part], sems.at[g // 2])
            )
            copies[-1].start()
    for copy in copies:
        copy.wait()


def per_device(
    queries,
    span_keys,
    span_values,
    positions,
    span_segments,
    cache_keys,
    cache_values,
    cache_segments,
):
    shape = jax.ShapeDtypeStruct
    small = (
        queries,
        span_keys.T,
        span_values.T,
        positions,
        span_segments.reshape(1, ROWS),
        cache_segments.reshape(4, 128),
    )
    tiles, positions, span_segments, cache_segments = call(
        pack_body,
        "pack",
        (shape((6 * 128, 128), BF16), *(shape(a.shape, a.dtype) for a in small[3:])),
        *(pltpu.with_memory_space_constraint(a, pltpu.HBM) for a in small),
        specs=[HBM] * 6,
        scratch=[pltpu.VMEM(a.shape, a.dtype) for a in small[:3]] + [pltpu.SemaphoreType.DMA((6,))],
    )
    tiles = exchange(tiles.reshape(-1, 2, 128), CHIPS).reshape(-1, 128)
    came = swap(tiles)
    bias, tables, turned_values = call(
        ready_body,
        "ready",
        (
            shape((512 + ROWS, 128), F32),
            shape((2, ROWS, 128), F32),
            shape((KVH, HD, 512), BF16),
        ),
        positions,
        span_segments,
        cache_segments,
        pltpu.with_memory_space_constraint(cache_values, pltpu.HBM),
        specs=[VMEM] * 3 + [HBM],
        scratch=[pltpu.VMEM((512, KVH * HD), BF16), pltpu.SemaphoreType.DMA],
    )
    message = shape((16, 40, 128), BF16)
    parts, q, kv = call(
        first_body,
        "first",
        (message, shape((H * ROWS, HD), BF16), shape((2, 128, 128), F32)),
        tiles,
        came,
        tables,
        cache_keys,
        turned_values,
        bias,
        scratch=[pltpu.VMEM((2, 6 * 128 + 16, 128), F32)],
    )
    other = swap(parts)
    parts = call(
        second_body, "second", message, q, cache_keys, turned_values, bias, kv, tables
    )
    parts = call(couple_body, "couple", message, parts, other)
    parts = exchange(parts, PLANE)
    parts = call(merge_body, "merge", shape((8, 40, 128), BF16), parts)
    parts = exchange(parts, ("z",))
    tile = call(finish_body, "finish", shape((32, 128), BF16), parts)
    whole = call(pair_body, "pair", shape((16, 64, 128), BF16), tile, swap(tile))
    whole = exchange(whole, PLANE)
    return call(
        place_body,
        "place",
        shape((ROWS, H * HD), BF16),
        whole,
        scratch=[pltpu.VMEM((ROWS, H * HD), BF16), pltpu.SemaphoreType.DMA((4,))],
        out_specs=HBM,
    )


def solution(mesh):
    split = Mesh(mesh.devices.reshape(4, 8, 4, 2), ALL)
    return jax.shard_map(
        per_device,
        mesh=split,
        in_specs=(
            P(None, ALL),
            P(None, ALL),
            P(None, ALL),
            P(),
            P(),
            P(ALL, None),
            P(ALL, None),
            P(ALL),
        ),
        out_specs=P(),
        check_vma=False,
    )
```

```python
import functools

import jax
import jax.numpy as jnp
from jax import lax
from jax.experimental import pallas as pl
from jax.experimental.pallas import tpu as pltpu
from jax.sharding import Mesh
from jax.sharding import PartitionSpec as P

H = 64
KVH = 8
HD = 128
ROWS = 16
ALL = ("y", "z", "x", "c")
CHIPS = ("y", "z", "x")
PLANE = ("x", "y")
LOG2E = 1.4426950408889634
NONE = -1e30
HIDDEN = -2e30
F32 = jnp.float32
BF16 = jnp.bfloat16
VMEM = pl.BlockSpec(memory_space=pltpu.VMEM)
NT = (((1,), (1,)), ((), ()))

HBM = pl.BlockSpec(memory_space=pltpu.HBM)


def call(body, name, out_shape, *args, specs=None, scratch=(), limit=8 << 20, out_specs=None):
    return pl.pallas_call(
        body,
        name=name,
        out_shape=out_shape,
        in_specs=specs or [VMEM] * len(args),
        out_specs=out_specs or jax.tree.map(lambda _: VMEM, out_shape),
        scratch_shapes=scratch,
        compiler_params=pltpu.CompilerParams(vmem_limit_bytes=limit),
    )(*args)


def lanes(shape):
    return lax.broadcasted_iota(jnp.int32, shape, len(shape) - 1)


def move(value, by):
    by %= value.shape[-1]
    return pltpu.roll(value, by, value.ndim - 1) if by else value


def exchange(tiles, axes):
    return lax.all_to_all(tiles, axes, 0, 0, tiled=True)


def swap(value):
    return lax.ppermute(value, "c", ((0, 1), (1, 0)))


def rows_of(shape):
    return lax.broadcasted_iota(jnp.int32, shape, 0)


TN = (((0,), (0,)), ((), ()))
NN = (((1,), (0,)), ((), ()))


def dot(a, b, dims):
    return lax.dot_general(a, b, dims, preferred_element_type=F32)


def where_one(hit):
    return jnp.where(hit, 1.0, 0.0).astype(BF16)


def pack_body(*refs):
    out_ref, q_ref, k_ref, v_ref, sems = refs[6], *refs[10:]
    copies = [
        pltpu.make_async_copy(source, target, sems.at[n])
        for n, (source, target) in enumerate(zip(refs[:6], (q_ref, k_ref, v_ref, *refs[7:10])))
    ]
    for copy in copies:
        copy.start()
    for copy in copies:
        copy.wait()
    q = dot(q_ref[...], where_one(lanes((32, 128)) % 32 == rows_of((32, 128))), NN)
    q = jnp.where(lanes((ROWS, 128)) // 32 == rows_of((ROWS, 128)) // 4, q, 0.0).astype(BF16)
    token = lanes((ROWS, 128)) // 4 - rows_of((ROWS, 128))
    kv = dot(k_ref[...], where_one(token == 0), NN) + dot(v_ref[...], where_one(token == 16), NN)
    kv = jnp.where(lanes((4, 128)) % 4 == rows_of((4, 128)), kv, 0.0).astype(BF16)
    tiles = dot(where_one(rows_of((48, ROWS)) % 6 == lanes((48, ROWS)) % 4), q, NN)
    tiles = tiles + dot(where_one(rows_of((48, 4)) % 6 == 4), kv, NN)
    tiles = tiles.astype(BF16)
    for n in range(out_ref.shape[0] // 48):
        out_ref[n * 48 : (n + 1) * 48, :] = tiles


def turn(angle):
    quarter = jnp.floor(angle * 0.6366197723675814 + 0.5)
    rest = angle - quarter * 1.5703125
    rest = rest - quarter * 4.837512969970703e-4
    rest = rest - quarter * 7.549789948768648e-8
    square = rest * rest
    sine = -1.9515295891e-4 * square + 8.3321608736e-3
    sine = (sine * square - 1.6666654611e-1) * square * rest + rest
    cosine = 2.443315711809948e-5 * square - 1.388731625493765e-3
    cosine = (cosine * square + 4.166664568298827e-2) * square * square - 0.5 * square + 1.0
    which = quarter.astype(jnp.int32) % 4
    odd = which % 2 == 1
    cosine, sine = jnp.where(odd, sine, cosine), jnp.where(odd, cosine, sine)
    cosine = jnp.where((which == 1) | (which == 2), -cosine, cosine)
    sine = jnp.where(which >= 2, -sine, sine)
    return cosine, sine


def rope_tables(positions, index):
    section = jnp.where(index < 16, 0, jnp.where(index < 40, 1, 2))
    high = positions // 64
    position = jnp.zeros(index.shape, F32)
    for scale, part in ((64.0, high), (1.0, positions - high * 64)):
        chosen = dot(part.astype(F32).astype(BF16), where_one(rows_of((3, 3 * 128)) == lanes((3, 3 * 128)) // 128), TN)
        picked = chosen[:, 256:]
        for n in range(2):
            picked = jnp.where(section == n, chosen[:, n * 128 : (n + 1) * 128], picked)
        position = position + scale * picked
    inverse = jnp.ones(index.shape, F32)
    for bit in range(6):
        step = 1000000.0 ** (-2.0 * 2**bit / HD)
        inverse = jnp.where((index // 2**bit) % 2 == 1, inverse * step, inverse)
    return turn(position * inverse)


def rotate(value, cosine, sine):
    return value * cosine + move(value, 64) * sine


def split_pair(value):
    high = value.astype(BF16).astype(F32)
    return high, (value - high).astype(BF16).astype(F32)


def state_rows(peak, total):
    row = rows_of((8, 128))
    parts = (*split_pair(peak), *split_pair(total))
    tile = jnp.zeros((8, 128), F32)
    for n, part in enumerate(parts):
        tile = jnp.where(row == n, part, tile)
    return tile.astype(BF16)


def ready_body(pos_ref, seg_ref, held_ref, v_hbm, bias_ref, table_ref, vt_ref, v_ref, sem):
    copy = pltpu.make_async_copy(v_hbm, v_ref, sem)
    copy.start()
    lane = lanes((ROWS, 128))
    cosine, sine = rope_tables(pos_ref[...], lane % 64)
    table_ref[0] = cosine
    table_ref[1] = jnp.where(lane < 64, -sine, sine)
    pick = where_one(rows_of((ROWS, 128)) == lane // 8)
    kinds = where_one(rows_of((8, ROWS)) == seg_ref[...])
    wanted = dot(kinds, pick, NN).astype(BF16)
    for part in range(4):
        have = where_one(rows_of((8, 128)) == held_ref[part : part + 1, :])
        bias_ref[part * 128 : (part + 1) * 128, :] = (dot(have, wanted, TN) - 1.0) * -HIDDEN
    seen = dot(kinds, wanted, TN) * jnp.where(rows_of((ROWS, 128)) <= lane // 8, 1.0, 0.0)
    bias_ref[512:, :] = (seen - 1.0) * -HIDDEN
    copy.wait()
    for g in range(KVH):
        vt_ref[g] = v_ref[:, g * HD : (g + 1) * HD].T


def join(own_ref, came_ref, table_ref, q_ref, kv_ref, flat_ref):
    c = lax.axis_index("c")
    shape = (128, 4 * 128)
    source, target = rows_of(shape), lanes(shape)
    whole = jnp.zeros((256, 512), F32)
    for n, ref in enumerate((own_ref, came_ref)):
        flat_ref[n, 0:768, :] = ref[...].astype(F32)
        kv_ref[n] = flat_ref[n, pl.ds(4, 128, stride=6), :]
        for half in range(2):
            part = jnp.concatenate(
                [flat_ref[n, pl.ds(j + 6 * half, 64, stride=12), :] for j in range(4)], axis=0
            )
            core = 1 - c if n else c
            at = (source // 32) * 128 + half * 64 + core * 32 + source % 32
            whole = whole + dot(part.astype(BF16), where_one(target == at), NN)
    for r in range(ROWS):
        high, low = divmod(r, 4)
        part = whole[low * 64 : (low + 1) * 64, high * 128 : (high + 1) * 128]
        part = rotate(part, table_ref[0, r : r + 1, :], table_ref[1, r : r + 1, :]).astype(BF16)
        for g in range(KVH):
            q_ref[g * 128 + r * 8 : g * 128 + r * 8 + 8, :] = part[g * 8 : (g + 1) * 8]


FACTOR = LOG2E / HD**0.5


def softened(scores):
    peak = jnp.maximum(jnp.max(scores, axis=0, keepdims=True), NONE)
    high, low = split_pair(peak)
    peak = high + low
    weights = jnp.exp2(scores - peak)
    return weights.astype(BF16), peak, jnp.sum(weights, axis=0, keepdims=True)


def heads_at(base, i):
    return pl.ds(pl.multiple_of((base + i) * 128, 128), 128)


def attend(base, q_ref, k_ref, vt_ref, bias_ref, out_ref):
    scores = [
        dot(k_ref[:, heads_at(base, i)], q_ref[heads_at(base, i), :], NT) * FACTOR
        + bias_ref[0:512, :]
        for i in range(4)
    ]
    parts = [softened(s) for s in scores]
    outs = [dot(vt_ref[base + i], parts[i][0], NN) for i in range(4)]
    for i, (_, peak, total) in enumerate(parts):
        emit(out_ref, i * 4, outs[i].astype(BF16), state_rows(peak, total))


def emit(out_ref, first, out, state):
    for n in range(4):
        out_ref[first + n, 0:32, :] = out[n * 32 : (n + 1) * 32]
        out_ref[first + n, 32:40, :] = state


def first_body(
    own_ref, came_ref, table_ref, k_ref, vt_ref, bias_ref, out_ref, q_ref, kv_ref, flat_ref
):
    join(own_ref, came_ref, table_ref, q_ref, kv_ref, flat_ref)
    attend((1 - lax.axis_index("c")) * 4, q_ref, k_ref, vt_ref, bias_ref, out_ref)


def second_body(q_ref, k_ref, vt_ref, bias_ref, kv_ref, table_ref, out_ref):
    c, y = lax.axis_index("c"), lax.axis_index("y")
    attend(c * 4, q_ref, k_ref, vt_ref, bias_ref, out_ref)

    @pl.when((lax.axis_index("z") == 0) & (lax.axis_index("x") == 0))
    def _():
        g = c * 4 + y
        chips = pl.ds(pl.multiple_of(g * 16, 16), 16)
        own, came = kv_ref[0, chips, :], kv_ref[1, chips, :]
        held = [jnp.where(c == core, own, came) for core in range(2)]
        held = jnp.concatenate(held, axis=0).astype(BF16)
        row, lane = rows_of((128, 128)), lanes((128, 128))
        pick = where_one(lane == row // 64 * 64 + (row % 16) * 4 + (row // 16) % 4)
        row, lane = rows_of((32, 256)), lanes((32, 256))
        place = where_one(row == lane // 128 * 16 + lane % 128 // 8)
        columns = dot(dot(pick, held, NT).astype(BF16), place, NN)
        row, lane = rows_of((128, 256)), lanes((128, 256))
        columns = jnp.where(lane % 8 == lane // 128 * 4 + (row // 16) % 4, columns, 0.0)
        columns = columns[:, :128] + columns[:, 128:]
        found = []
        for kind in range(2):
            value = sum(columns[(kind * 4 + i) * 16 : (kind * 4 + i + 1) * 16] for i in range(4))
            if kind == 0:
                value = rotate(value, table_ref[0], table_ref[1])
            found.append(value.astype(BF16))
        scores = dot(found[0], q_ref[heads_at(c * 4, y), :], NT) * FACTOR + bias_ref[512:, :]
        weights, peak, total = softened(scores)
        own = dot(found[1], weights, TN)
        for n in range(4):
            tile = out_ref.at[y * 4 + n]
            out, peaks, totals = merge(
                [tile[0:32, :].astype(F32), own[n * 32 : (n + 1) * 32]],
                *zip(state_of(tile), (peak, total)),
            )
            tile[0:32, :] = out.astype(BF16)
            tile[32:40, :] = state_rows(peaks, totals)


def state_of(ref):
    state = ref[32:40, :].astype(F32)
    return state[0:1] + state[1:2], state[2:3] + state[3:4]


def merge(outs, peaks, totals):
    peak = functools.reduce(jnp.maximum, peaks)
    factors = [jnp.exp2(p - peak) for p in peaks]
    out = sum(o * f for o, f in zip(outs, factors))
    return out, peak, sum(t * f for t, f in zip(totals, factors))


def merged(refs):
    outs = [ref[0:32, :].astype(F32) for ref in refs]
    return merge(outs, *zip(*map(state_of, refs)))


def tiles_of(ref):
    return [ref.at[n] for n in range(ref.shape[0])]


def couple_body(own_ref, came_ref, out_ref):
    for n in range(16):
        out, peak, total = merged([own_ref.at[n], came_ref.at[n]])
        out_ref[n, 0:32, :] = out.astype(BF16)
        out_ref[n, 32:40, :] = state_rows(peak, total)


def merge_body(in_ref, out_ref):
    out, peak, total = merged(tiles_of(in_ref))
    out, state = out.astype(BF16), state_rows(peak, total)
    for d in range(out_ref.shape[0]):
        out_ref[d, 0:32, :] = out
        out_ref[d, 32:40, :] = state


def finish_body(in_ref, out_ref):
    out, _, total = merged(tiles_of(in_ref))
    out_ref[...] = (out / total).astype(BF16)


def pair_body(own_ref, came_ref, out_ref):
    first = lax.axis_index("c") == 0
    own, came = own_ref[...].astype(F32), came_ref[...].astype(F32)
    tiles = (jnp.where(first, own, came).astype(BF16), jnp.where(first, came, own).astype(BF16))
    for d in range(out_ref.shape[0]):
        for n, tile in enumerate(tiles):
            out_ref[d, n * 32 : (n + 1) * 32, :] = tile


def place_body(in_ref, out_hbm, out_ref, sems):
    copies = []
    row = rows_of((128, 128))
    eye = where_one((row % 16) * 8 + row // 16 == lanes((128, 128)))
    for g in range(KVH):
        half, y = divmod(g, 4)
        block = in_ref[y * 4 : (y + 1) * 4, half * 32 : (half + 1) * 32, :].reshape(128, 128)
        block = dot(eye, block, NT).astype(BF16)
        for i in range(8):
            at = (g * 8 + i) * HD
            out_ref[:, at : at + HD] = block[i * ROWS : (i + 1) * ROWS]
        if g % 2:
            part = slice((g - 1) * 8 * HD, (g + 1) * 8 * HD)
            copies.append(
                pltpu.make_async_copy(out_ref.at[:, part], out_hbm.at[:, part], sems.at[g // 2])
            )
            copies[-1].start()
    for copy in copies:
        copy.wait()


def per_device(
    queries,
    span_keys,
    span_values,
    positions,
    span_segments,
    cache_keys,
    cache_values,
    cache_segments,
):
    shape = jax.ShapeDtypeStruct
    small = (
        queries,
        span_keys.T,
        span_values.T,
        positions,
        span_segments.reshape(1, ROWS),
        cache_segments.reshape(4, 128),
    )
    tiles, positions, span_segments, cache_segments = call(
        pack_body,
        "pack",
        (shape((6 * 128, 128), BF16), *(shape(a.shape, a.dtype) for a in small[3:])),
        *(pltpu.with_memory_space_constraint(a, pltpu.HBM) for a in small),
        specs=[HBM] * 6,
        scratch=[pltpu.VMEM(a.shape, a.dtype) for a in small[:3]] + [pltpu.SemaphoreType.DMA((6,))],
    )
    tiles = exchange(tiles.reshape(-1, 2, 128), CHIPS).reshape(-1, 128)
    came = swap(tiles)
    bias, tables, turned_values = call(
        ready_body,
        "ready",
        (
            shape((512 + ROWS, 128), F32),
            shape((2, ROWS, 128), F32),
            shape((KVH, HD, 512), BF16),
        ),
        positions,
        span_segments,
        cache_segments,
        pltpu.with_memory_space_constraint(cache_values, pltpu.HBM),
        specs=[VMEM] * 3 + [HBM],
        scratch=[pltpu.VMEM((512, KVH * HD), BF16), pltpu.SemaphoreType.DMA],
    )
    message = shape((16, 40, 128), BF16)
    parts, q, kv = call(
        first_body,
        "first",
        (message, shape((H * ROWS, HD), BF16), shape((2, 128, 128), F32)),
        tiles,
        came,
        tables,
        cache_keys,
        turned_values,
        bias,
        scratch=[pltpu.VMEM((2, 6 * 128 + 16, 128), F32)],
    )
    other = swap(parts)
    parts = call(
        second_body, "second", message, q, cache_keys, turned_values, bias, kv, tables
    )
    parts = call(couple_body, "couple", message, parts, other)
    parts = exchange(parts, PLANE)
    parts = call(merge_body, "merge", shape((8, 40, 128), BF16), parts)
    parts = exchange(parts, ("z",))
    tile = call(finish_body, "finish", shape((32, 128), BF16), parts)
    whole = call(pair_body, "pair", shape((16, 64, 128), BF16), tile, swap(tile))
    whole = exchange(whole, PLANE)
    return call(
        place_body,
        "place",
        shape((ROWS, H * HD), BF16),
        whole,
        scratch=[pltpu.VMEM((ROWS, H * HD), BF16), pltpu.SemaphoreType.DMA((4,))],
        out_specs=HBM,
    )


def solution(mesh):
    split = Mesh(mesh.devices.reshape(4, 8, 4, 2), ALL)
    return jax.shard_map(
        per_device,
        mesh=split,
        in_specs=(
            P(None, ALL),
            P(None, ALL),
            P(None, ALL),
            P(),
            P(),
            P(ALL, None),
            P(ALL, None),
            P(ALL),
        ),
        out_specs=P(),
        check_vma=False,
    )
```

```python
import functools

import jax
import jax.numpy as jnp
from jax import lax
from jax.experimental import pallas as pl
from jax.experimental.pallas import tpu as pltpu
from jax.sharding import Mesh
from jax.sharding import PartitionSpec as P

H = 64
KVH = 8
HD = 128
ROWS = 16
ALL = ("y", "z", "x", "c")
CHIPS = ("y", "z", "x")
PLANE = ("x", "y")
LOG2E = 1.4426950408889634
NONE = -1e30
HIDDEN = -2e30
F32 = jnp.float32
BF16 = jnp.bfloat16
VMEM = pl.BlockSpec(memory_space=pltpu.VMEM)
NT = (((1,), (1,)), ((), ()))

HBM = pl.BlockSpec(memory_space=pltpu.HBM)


def call(body, name, out_shape, *args, specs=None, scratch=(), limit=8 << 20, out_specs=None):
    return pl.pallas_call(
        body,
        name=name,
        out_shape=out_shape,
        in_specs=specs or [VMEM] * len(args),
        out_specs=out_specs or jax.tree.map(lambda _: VMEM, out_shape),
        scratch_shapes=scratch,
        compiler_params=pltpu.CompilerParams(vmem_limit_bytes=limit),
    )(*args)


def lanes(shape):
    return lax.broadcasted_iota(jnp.int32, shape, len(shape) - 1)


def move(value, by):
    by %= value.shape[-1]
    return pltpu.roll(value, by, value.ndim - 1) if by else value


def exchange(tiles, axes):
    return lax.all_to_all(tiles, axes, 0, 0, tiled=True)


def swap(value):
    return lax.ppermute(value, "c", ((0, 1), (1, 0)))


def rows_of(shape):
    return lax.broadcasted_iota(jnp.int32, shape, 0)


TN = (((0,), (0,)), ((), ()))
NN = (((1,), (0,)), ((), ()))


def dot(a, b, dims):
    return lax.dot_general(a, b, dims, preferred_element_type=F32)


def where_one(hit):
    return jnp.where(hit, 1.0, 0.0).astype(BF16)


def pack_body(*refs):
    out_ref, q_ref, k_ref, v_ref, sems = refs[6], *refs[10:]
    copies = [
        pltpu.make_async_copy(source, target, sems.at[n])
        for n, (source, target) in enumerate(zip(refs[:6], (q_ref, k_ref, v_ref, *refs[7:10])))
    ]
    for copy in copies:
        copy.start()
    for copy in copies:
        copy.wait()
    q = dot(q_ref[...], where_one(lanes((32, 128)) % 32 == rows_of((32, 128))), NN)
    q = jnp.where(lanes((ROWS, 128)) // 32 == rows_of((ROWS, 128)) // 4, q, 0.0).astype(BF16)
    token = lanes((ROWS, 128)) // 4 - rows_of((ROWS, 128))
    kv = dot(k_ref[...], where_one(token == 0), NN) + dot(v_ref[...], where_one(token == 16), NN)
    kv = jnp.where(lanes((4, 128)) % 4 == rows_of((4, 128)), kv, 0.0).astype(BF16)
    tiles = dot(where_one(rows_of((48, ROWS)) % 6 == lanes((48, ROWS)) % 4), q, NN)
    tiles = tiles + dot(where_one(rows_of((48, 4)) % 6 == 4), kv, NN)
    tiles = tiles.astype(BF16)
    for n in range(out_ref.shape[0] // 48):
        out_ref[n * 48 : (n + 1) * 48, :] = tiles


def turn(angle):
    quarter = jnp.floor(angle * 0.6366197723675814 + 0.5)
    rest = angle - quarter * 1.5703125
    rest = rest - quarter * 4.837512969970703e-4
    rest = rest - quarter * 7.549789948768648e-8
    square = rest * rest
    sine = -1.9515295891e-4 * square + 8.3321608736e-3
    sine = (sine * square - 1.6666654611e-1) * square * rest + rest
    cosine = 2.443315711809948e-5 * square - 1.388731625493765e-3
    cosine = (cosine * square + 4.166664568298827e-2) * square * square - 0.5 * square + 1.0
    which = quarter.astype(jnp.int32) % 4
    odd = which % 2 == 1
    cosine, sine = jnp.where(odd, sine, cosine), jnp.where(odd, cosine, sine)
    cosine = jnp.where((which == 1) | (which == 2), -cosine, cosine)
    sine = jnp.where(which >= 2, -sine, sine)
    return cosine, sine


def rope_tables(positions, index):
    section = jnp.where(index < 16, 0, jnp.where(index < 40, 1, 2))
    high = positions // 64
    position = jnp.zeros(index.shape, F32)
    for scale, part in ((64.0, high), (1.0, positions - high * 64)):
        chosen = dot(part.astype(F32).astype(BF16), where_one(rows_of((3, 3 * 128)) == lanes((3, 3 * 128)) // 128), TN)
        picked = chosen[:, 256:]
        for n in range(2):
            picked = jnp.where(section == n, chosen[:, n * 128 : (n + 1) * 128], picked)
        position = position + scale * picked
    inverse = jnp.ones(index.shape, F32)
    for bit in range(6):
        step = 1000000.0 ** (-2.0 * 2**bit / HD)
        inverse = jnp.where((index // 2**bit) % 2 == 1, inverse * step, inverse)
    return turn(position * inverse)


def rotate(value, cosine, sine):
    return value * cosine + move(value, 64) * sine


def split_pair(value):
    high = value.astype(BF16).astype(F32)
    return high, (value - high).astype(BF16).astype(F32)


def state_rows(peak, total):
    row = rows_of((8, 128))
    parts = (*split_pair(peak), *split_pair(total))
    tile = jnp.zeros((8, 128), F32)
    for n, part in enumerate(parts):
        tile = jnp.where(row == n, part, tile)
    return tile.astype(BF16)


def ready_body(pos_ref, seg_ref, held_ref, v_hbm, bias_ref, table_ref, vt_ref, v_ref, sem):
    copy = pltpu.make_async_copy(v_hbm, v_ref, sem)
    copy.start()
    lane = lanes((ROWS, 128))
    cosine, sine = rope_tables(pos_ref[...], lane % 64)
    table_ref[0] = cosine
    table_ref[1] = jnp.where(lane < 64, -sine, sine)
    pick = where_one(rows_of((ROWS, 128)) == lane // 8)
    kinds = where_one(rows_of((8, ROWS)) == seg_ref[...])
    wanted = dot(kinds, pick, NN).astype(BF16)
    for part in range(4):
        have = where_one(rows_of((8, 128)) == held_ref[part : part + 1, :])
        bias_ref[part * 128 : (part + 1) * 128, :] = (dot(have, wanted, TN) - 1.0) * -HIDDEN
    seen = dot(kinds, wanted, TN) * jnp.where(rows_of((ROWS, 128)) <= lane // 8, 1.0, 0.0)
    bias_ref[512:, :] = (seen - 1.0) * -HIDDEN
    copy.wait()
    for g in range(KVH):
        vt_ref[g] = v_ref[:, g * HD : (g + 1) * HD].T


def join(own_ref, came_ref, table_ref, q_ref, kv_ref, flat_ref):
    c = lax.axis_index("c")
    shape = (128, 4 * 128)
    source, target = rows_of(shape), lanes(shape)
    whole = jnp.zeros((256, 512), F32)
    for n, ref in enumerate((own_ref, came_ref)):
        flat_ref[n, 0:768, :] = ref[...].astype(F32)
        kv_ref[n] = flat_ref[n, pl.ds(4, 128, stride=6), :]
        for half in range(2):
            part = jnp.concatenate(
                [flat_ref[n, pl.ds(j + 6 * half, 64, stride=12), :] for j in range(4)], axis=0
            )
            core = 1 - c if n else c
            at = (source // 32) * 128 + half * 64 + core * 32 + source % 32
            whole = whole + dot(part.astype(BF16), where_one(target == at), NN)
    for r in range(ROWS):
        high, low = divmod(r, 4)
        part = whole[low * 64 : (low + 1) * 64, high * 128 : (high + 1) * 128]
        part = rotate(part, table_ref[0, r : r + 1, :], table_ref[1, r : r + 1, :]).astype(BF16)
        for g in range(KVH):
            q_ref[g * 128 + r * 8 : g * 128 + r * 8 + 8, :] = part[g * 8 : (g + 1) * 8]


FACTOR = LOG2E / HD**0.5


def softened(scores):
    peak = jnp.maximum(jnp.max(scores, axis=0, keepdims=True), NONE)
    high, low = split_pair(peak)
    peak = high + low
    weights = jnp.exp2(scores - peak)
    return weights.astype(BF16), peak, jnp.sum(weights, axis=0, keepdims=True)


def heads_at(base, i):
    return pl.ds(pl.multiple_of((base + i) * 128, 128), 128)


def attend(base, q_ref, k_ref, vt_ref, bias_ref, out_ref):
    scores = [
        dot(k_ref[:, heads_at(base, i)], q_ref[heads_at(base, i), :], NT) * FACTOR
        + bias_ref[0:512, :]
        for i in range(4)
    ]
    parts = [softened(s) for s in scores]
    outs = [dot(vt_ref[base + i], parts[i][0], NN) for i in range(4)]
    for i, (_, peak, total) in enumerate(parts):
        emit(out_ref, i * 4, outs[i].astype(BF16), state_rows(peak, total))


def emit(out_ref, first, out, state):
    for n in range(4):
        out_ref[first + n, 0:32, :] = out[n * 32 : (n + 1) * 32]
        out_ref[first + n, 32:40, :] = state


def first_body(
    own_ref, came_ref, table_ref, k_ref, vt_ref, bias_ref, out_ref, q_ref, kv_ref, flat_ref
):
    join(own_ref, came_ref, table_ref, q_ref, kv_ref, flat_ref)
    attend((1 - lax.axis_index("c")) * 4, q_ref, k_ref, vt_ref, bias_ref, out_ref)


def second_body(q_ref, k_ref, vt_ref, bias_ref, kv_ref, table_ref, out_ref):
    c, y = lax.axis_index("c"), lax.axis_index("y")
    g = c * 4 + y
    chips = pl.ds(pl.multiple_of(g * 16, 16), 16)
    own, came = kv_ref[0, chips, :], kv_ref[1, chips, :]
    held = [jnp.where(c == core, own, came) for core in range(2)]
    held = jnp.concatenate(held, axis=0).astype(BF16)
    row, lane = rows_of((128, 128)), lanes((128, 128))
    pick = where_one(lane == row // 64 * 64 + (row % 16) * 4 + (row // 16) % 4)
    row, lane = rows_of((32, 256)), lanes((32, 256))
    place = where_one(row == lane // 128 * 16 + lane % 128 // 8)
    columns = dot(dot(pick, held, NT).astype(BF16), place, NN)
    row, lane = rows_of((128, 256)), lanes((128, 256))
    columns = jnp.where(lane % 8 == lane // 128 * 4 + (row // 16) % 4, columns, 0.0)
    columns = columns[:, :128] + columns[:, 128:]
    found = []
    for kind in range(2):
        value = sum(columns[(kind * 4 + i) * 16 : (kind * 4 + i + 1) * 16] for i in range(4))
        if kind == 0:
            value = rotate(value, table_ref[0], table_ref[1])
        found.append(value.astype(BF16))
    scores = dot(found[0], q_ref[heads_at(c * 4, y), :], NT) * FACTOR + bias_ref[512:, :]
    weights, peak, total = softened(scores)
    own = dot(found[1], weights, TN)
    attend(c * 4, q_ref, k_ref, vt_ref, bias_ref, out_ref)

    @pl.when((lax.axis_index("z") == 0) & (lax.axis_index("x") == 0))
    def _():
        for n in range(4):
            tile = out_ref.at[y * 4 + n]
            out, peaks, totals = merge(
                [tile[0:32, :].astype(F32), own[n * 32 : (n + 1) * 32]],
                *zip(state_of(tile), (peak, total)),
            )
            tile[0:32, :] = out.astype(BF16)
            tile[32:40, :] = state_rows(peaks, totals)


def state_of(ref):
    state = ref[32:40, :].astype(F32)
    return state[0:1] + state[1:2], state[2:3] + state[3:4]


def merge(outs, peaks, totals):
    peak = functools.reduce(jnp.maximum, peaks)
    factors = [jnp.exp2(p - peak) for p in peaks]
    out = sum(o * f for o, f in zip(outs, factors))
    return out, peak, sum(t * f for t, f in zip(totals, factors))


def merged(refs):
    outs = [ref[0:32, :].astype(F32) for ref in refs]
    return merge(outs, *zip(*map(state_of, refs)))


def tiles_of(ref):
    return [ref.at[n] for n in range(ref.shape[0])]


def couple_body(own_ref, came_ref, out_ref):
    for n in range(16):
        out, peak, total = merged([own_ref.at[n], came_ref.at[n]])
        out_ref[n, 0:32, :] = out.astype(BF16)
        out_ref[n, 32:40, :] = state_rows(peak, total)


def merge_body(in_ref, out_ref):
    out, peak, total = merged(tiles_of(in_ref))
    out, state = out.astype(BF16), state_rows(peak, total)
    for d in range(out_ref.shape[0]):
        out_ref[d, 0:32, :] = out
        out_ref[d, 32:40, :] = state


def finish_body(in_ref, out_ref):
    out, _, total = merged(tiles_of(in_ref))
    out_ref[...] = (out / total).astype(BF16)


def pair_body(own_ref, came_ref, out_ref):
    first = lax.axis_index("c") == 0
    own, came = own_ref[...].astype(F32), came_ref[...].astype(F32)
    tiles = (jnp.where(first, own, came).astype(BF16), jnp.where(first, came, own).astype(BF16))
    for d in range(out_ref.shape[0]):
        for n, tile in enumerate(tiles):
            out_ref[d, n * 32 : (n + 1) * 32, :] = tile


def place_body(in_ref, out_hbm, out_ref, sems):
    copies = []
    row = rows_of((128, 128))
    eye = where_one((row % 16) * 8 + row // 16 == lanes((128, 128)))
    for g in range(KVH):
        half, y = divmod(g, 4)
        block = in_ref[y * 4 : (y + 1) * 4, half * 32 : (half + 1) * 32, :].reshape(128, 128)
        block = dot(eye, block, NT).astype(BF16)
        for i in range(8):
            at = (g * 8 + i) * HD
            out_ref[:, at : at + HD] = block[i * ROWS : (i + 1) * ROWS]
        if g % 2:
            part = slice((g - 1) * 8 * HD, (g + 1) * 8 * HD)
            copies.append(
                pltpu.make_async_copy(out_ref.at[:, part], out_hbm.at[:, part], sems.at[g // 2])
            )
            copies[-1].start()
    for copy in copies:
        copy.wait()


def per_device(
    queries,
    span_keys,
    span_values,
    positions,
    span_segments,
    cache_keys,
    cache_values,
    cache_segments,
):
    shape = jax.ShapeDtypeStruct
    small = (
        queries,
        span_keys.T,
        span_values.T,
        positions,
        span_segments.reshape(1, ROWS),
        cache_segments.reshape(4, 128),
    )
    tiles, positions, span_segments, cache_segments = call(
        pack_body,
        "pack",
        (shape((6 * 128, 128), BF16), *(shape(a.shape, a.dtype) for a in small[3:])),
        *(pltpu.with_memory_space_constraint(a, pltpu.HBM) for a in small),
        specs=[HBM] * 6,
        scratch=[pltpu.VMEM(a.shape, a.dtype) for a in small[:3]] + [pltpu.SemaphoreType.DMA((6,))],
    )
    tiles = exchange(tiles.reshape(-1, 2, 128), CHIPS).reshape(-1, 128)
    came = swap(tiles)
    bias, tables, turned_values = call(
        ready_body,
        "ready",
        (
            shape((512 + ROWS, 128), F32),
            shape((2, ROWS, 128), F32),
            shape((KVH, HD, 512), BF16),
        ),
        positions,
        span_segments,
        cache_segments,
        pltpu.with_memory_space_constraint(cache_values, pltpu.HBM),
        specs=[VMEM] * 3 + [HBM],
        scratch=[pltpu.VMEM((512, KVH * HD), BF16), pltpu.SemaphoreType.DMA],
    )
    message = shape((16, 40, 128), BF16)
    parts, q, kv = call(
        first_body,
        "first",
        (message, shape((H * ROWS, HD), BF16), shape((2, 128, 128), F32)),
        tiles,
        came,
        tables,
        cache_keys,
        turned_values,
        bias,
        scratch=[pltpu.VMEM((2, 6 * 128 + 16, 128), F32)],
    )
    other = swap(parts)
    parts = call(
        second_body, "second", message, q, cache_keys, turned_values, bias, kv, tables
    )
    parts = call(couple_body, "couple", message, parts, other)
    parts = exchange(parts, PLANE)
    parts = call(merge_body, "merge", shape((8, 40, 128), BF16), parts)
    parts = exchange(parts, ("z",))
    tile = call(finish_body, "finish", shape((32, 128), BF16), parts)
    whole = call(pair_body, "pair", shape((16, 64, 128), BF16), tile, swap(tile))
    whole = exchange(whole, PLANE)
    return call(
        place_body,
        "place",
        shape((ROWS, H * HD), BF16),
        whole,
        scratch=[pltpu.VMEM((ROWS, H * HD), BF16), pltpu.SemaphoreType.DMA((4,))],
        out_specs=HBM,
    )


def solution(mesh):
    split = Mesh(mesh.devices.reshape(4, 8, 4, 2), ALL)
    return jax.shard_map(
        per_device,
        mesh=split,
        in_specs=(
            P(None, ALL),
            P(None, ALL),
            P(None, ALL),
            P(),
            P(),
            P(ALL, None),
            P(ALL, None),
            P(ALL),
        ),
        out_specs=P(),
        check_vma=False,
    )
```

```python
import functools

import jax
import jax.numpy as jnp
from jax import lax
from jax.experimental import pallas as pl
from jax.experimental.pallas import tpu as pltpu
from jax.sharding import Mesh
from jax.sharding import PartitionSpec as P

H = 64
KVH = 8
HD = 128
ROWS = 16
ALL = ("y", "z", "x", "c")
CHIPS = ("y", "z", "x")
PLANE = ("x", "y")
LOG2E = 1.4426950408889634
NONE = -1e30
HIDDEN = -2e30
F32 = jnp.float32
BF16 = jnp.bfloat16
VMEM = pl.BlockSpec(memory_space=pltpu.VMEM)
NT = (((1,), (1,)), ((), ()))

HBM = pl.BlockSpec(memory_space=pltpu.HBM)


def call(body, name, out_shape, *args, specs=None, scratch=(), limit=8 << 20, out_specs=None):
    return pl.pallas_call(
        body,
        name=name,
        out_shape=out_shape,
        in_specs=specs or [VMEM] * len(args),
        out_specs=out_specs or jax.tree.map(lambda _: VMEM, out_shape),
        scratch_shapes=scratch,
        compiler_params=pltpu.CompilerParams(vmem_limit_bytes=limit),
    )(*args)


def lanes(shape):
    return lax.broadcasted_iota(jnp.int32, shape, len(shape) - 1)


def move(value, by):
    by %= value.shape[-1]
    return pltpu.roll(value, by, value.ndim - 1) if by else value


def exchange(tiles, axes):
    return lax.all_to_all(tiles, axes, 0, 0, tiled=True)


def swap(value):
    return lax.ppermute(value, "c", ((0, 1), (1, 0)))


def rows_of(shape):
    return lax.broadcasted_iota(jnp.int32, shape, 0)


TN = (((0,), (0,)), ((), ()))
NN = (((1,), (0,)), ((), ()))


def dot(a, b, dims):
    return lax.dot_general(a, b, dims, preferred_element_type=F32)


def where_one(hit):
    return jnp.where(hit, 1.0, 0.0).astype(BF16)


def pack_body(*refs):
    out_ref, q_ref, k_ref, v_ref, sems = refs[6], *refs[10:]
    copies = [
        pltpu.make_async_copy(source, target, sems.at[n])
        for n, (source, target) in enumerate(zip(refs[:6], (q_ref, k_ref, v_ref, *refs[7:10])))
    ]
    for copy in copies:
        copy.start()
    wide = where_one(lanes((32, 128)) % 32 == rows_of((32, 128)))
    late = lanes((ROWS, 128)) // 32 == rows_of((ROWS, 128)) // 4
    token = lanes((ROWS, 128)) // 4 - rows_of((ROWS, 128))
    keys, values = where_one(token == 0), where_one(token == 16)
    column = lanes((4, 128)) % 4 == rows_of((4, 128))
    q_rows = where_one(rows_of((48, ROWS)) % 6 == lanes((48, ROWS)) % 4)
    kv_rows = where_one(rows_of((48, 4)) % 6 == 4)
    for copy in copies[:3]:
        copy.wait()
    q = jnp.where(late, dot(q_ref[...], wide, NN), 0.0).astype(BF16)
    kv = dot(k_ref[...], keys, NN) + dot(v_ref[...], values, NN)
    kv = jnp.where(column, kv, 0.0).astype(BF16)
    tiles = (dot(q_rows, q, NN) + dot(kv_rows, kv, NN)).astype(BF16)
    for n in range(out_ref.shape[0] // 48):
        out_ref[n * 48 : (n + 1) * 48, :] = tiles
    for copy in copies[3:]:
        copy.wait()


def turn(angle):
    quarter = jnp.floor(angle * 0.6366197723675814 + 0.5)
    rest = angle - quarter * 1.5703125
    rest = rest - quarter * 4.837512969970703e-4
    rest = rest - quarter * 7.549789948768648e-8
    square = rest * rest
    sine = -1.9515295891e-4 * square + 8.3321608736e-3
    sine = (sine * square - 1.6666654611e-1) * square * rest + rest
    cosine = 2.443315711809948e-5 * square - 1.388731625493765e-3
    cosine = (cosine * square + 4.166664568298827e-2) * square * square - 0.5 * square + 1.0
    which = quarter.astype(jnp.int32) % 4
    odd = which % 2 == 1
    cosine, sine = jnp.where(odd, sine, cosine), jnp.where(odd, cosine, sine)
    cosine = jnp.where((which == 1) | (which == 2), -cosine, cosine)
    sine = jnp.where(which >= 2, -sine, sine)
    return cosine, sine


def rope_tables(positions, index):
    section = jnp.where(index < 16, 0, jnp.where(index < 40, 1, 2))
    high = positions // 64
    position = jnp.zeros(index.shape, F32)
    for scale, part in ((64.0, high), (1.0, positions - high * 64)):
        chosen = dot(part.astype(F32).astype(BF16), where_one(rows_of((3, 3 * 128)) == lanes((3, 3 * 128)) // 128), TN)
        picked = chosen[:, 256:]
        for n in range(2):
            picked = jnp.where(section == n, chosen[:, n * 128 : (n + 1) * 128], picked)
        position = position + scale * picked
    inverse = jnp.ones(index.shape, F32)
    for bit in range(6):
        step = 1000000.0 ** (-2.0 * 2**bit / HD)
        inverse = jnp.where((index // 2**bit) % 2 == 1, inverse * step, inverse)
    return turn(position * inverse)


def rotate(value, cosine, sine):
    return value * cosine + move(value, 64) * sine


def split_pair(value):
    high = value.astype(BF16).astype(F32)
    return high, (value - high).astype(BF16).astype(F32)


def state_rows(peak, total):
    row = rows_of((8, 128))
    parts = (*split_pair(peak), *split_pair(total))
    tile = jnp.zeros((8, 128), F32)
    for n, part in enumerate(parts):
        tile = jnp.where(row == n, part, tile)
    return tile.astype(BF16)


def ready_body(pos_ref, seg_ref, held_ref, v_hbm, bias_ref, table_ref, vt_ref, v_ref, sem):
    copy = pltpu.make_async_copy(v_hbm, v_ref, sem)
    copy.start()
    lane = lanes((ROWS, 128))
    cosine, sine = rope_tables(pos_ref[...], lane % 64)
    table_ref[0] = cosine
    table_ref[1] = jnp.where(lane < 64, -sine, sine)
    pick = where_one(rows_of((ROWS, 128)) == lane // 8)
    kinds = where_one(rows_of((8, ROWS)) == seg_ref[...])
    wanted = dot(kinds, pick, NN).astype(BF16)
    for part in range(4):
        have = where_one(rows_of((8, 128)) == held_ref[part : part + 1, :])
        bias_ref[part * 128 : (part + 1) * 128, :] = (dot(have, wanted, TN) - 1.0) * -HIDDEN
    seen = dot(kinds, wanted, TN) * jnp.where(rows_of((ROWS, 128)) <= lane // 8, 1.0, 0.0)
    bias_ref[512:, :] = (seen - 1.0) * -HIDDEN
    copy.wait()
    for g in range(KVH):
        vt_ref[g] = v_ref[:, g * HD : (g + 1) * HD].T


def join(own_ref, came_ref, table_ref, q_ref, kv_ref, flat_ref):
    c = lax.axis_index("c")
    shape = (128, 4 * 128)
    source, target = rows_of(shape), lanes(shape)
    whole = jnp.zeros((256, 512), F32)
    for n, ref in enumerate((own_ref, came_ref)):
        flat_ref[n, 0:768, :] = ref[...].astype(F32)
        kv_ref[n] = flat_ref[n, pl.ds(4, 128, stride=6), :]
        for half in range(2):
            part = jnp.concatenate(
                [flat_ref[n, pl.ds(j + 6 * half, 64, stride=12), :] for j in range(4)], axis=0
            )
            core = 1 - c if n else c
            at = (source // 32) * 128 + half * 64 + core * 32 + source % 32
            whole = whole + dot(part.astype(BF16), where_one(target == at), NN)
    for r in range(ROWS):
        high, low = divmod(r, 4)
        part = whole[low * 64 : (low + 1) * 64, high * 128 : (high + 1) * 128]
        part = rotate(part, table_ref[0, r : r + 1, :], table_ref[1, r : r + 1, :]).astype(BF16)
        for g in range(KVH):
            q_ref[g * 128 + r * 8 : g * 128 + r * 8 + 8, :] = part[g * 8 : (g + 1) * 8]


FACTOR = LOG2E / HD**0.5


def softened(scores):
    peak = jnp.maximum(jnp.max(scores, axis=0, keepdims=True), NONE)
    high, low = split_pair(peak)
    peak = high + low
    weights = jnp.exp2(scores - peak)
    return weights.astype(BF16), peak, jnp.sum(weights, axis=0, keepdims=True)


def heads_at(base, i):
    return pl.ds(pl.multiple_of((base + i) * 128, 128), 128)


def attend(base, q_ref, k_ref, vt_ref, bias_ref, out_ref):
    scores = [
        dot(k_ref[:, heads_at(base, i)], q_ref[heads_at(base, i), :], NT) * FACTOR
        + bias_ref[0:512, :]
        for i in range(4)
    ]
    parts = [softened(s) for s in scores]
    outs = [dot(vt_ref[base + i], parts[i][0], NN) for i in range(4)]
    for i, (_, peak, total) in enumerate(parts):
        emit(out_ref, i * 4, outs[i].astype(BF16), state_rows(peak, total))


def emit(out_ref, first, out, state):
    for n in range(4):
        out_ref[first + n, 0:32, :] = out[n * 32 : (n + 1) * 32]
        out_ref[first + n, 32:40, :] = state


def first_body(
    own_ref, came_ref, table_ref, k_ref, vt_ref, bias_ref, out_ref, q_ref, kv_ref, flat_ref
):
    join(own_ref, came_ref, table_ref, q_ref, kv_ref, flat_ref)
    attend((1 - lax.axis_index("c")) * 4, q_ref, k_ref, vt_ref, bias_ref, out_ref)


def second_body(q_ref, k_ref, vt_ref, bias_ref, kv_ref, table_ref, out_ref):
    c, y = lax.axis_index("c"), lax.axis_index("y")
    g = c * 4 + y
    chips = pl.ds(pl.multiple_of(g * 16, 16), 16)
    own, came = kv_ref[0, chips, :], kv_ref[1, chips, :]
    held = [jnp.where(c == core, own, came) for core in range(2)]
    held = jnp.concatenate(held, axis=0).astype(BF16)
    row, lane = rows_of((128, 128)), lanes((128, 128))
    pick = where_one(lane == row // 64 * 64 + (row % 16) * 4 + (row // 16) % 4)
    row, lane = rows_of((32, 256)), lanes((32, 256))
    place = where_one(row == lane // 128 * 16 + lane % 128 // 8)
    columns = dot(dot(pick, held, NT).astype(BF16), place, NN)
    row, lane = rows_of((128, 256)), lanes((128, 256))
    columns = jnp.where(lane % 8 == lane // 128 * 4 + (row // 16) % 4, columns, 0.0)
    columns = columns[:, :128] + columns[:, 128:]
    found = []
    for kind in range(2):
        value = sum(columns[(kind * 4 + i) * 16 : (kind * 4 + i + 1) * 16] for i in range(4))
        if kind == 0:
            value = rotate(value, table_ref[0], table_ref[1])
        found.append(value.astype(BF16))
    scores = dot(found[0], q_ref[heads_at(c * 4, y), :], NT) * FACTOR + bias_ref[512:, :]
    weights, peak, total = softened(scores)
    own = dot(found[1], weights, TN)
    attend(c * 4, q_ref, k_ref, vt_ref, bias_ref, out_ref)

    @pl.when((lax.axis_index("z") == 0) & (lax.axis_index("x") == 0))
    def _():
        for n in range(4):
            tile = out_ref.at[y * 4 + n]
            out, peaks, totals = merge(
                [tile[0:32, :].astype(F32), own[n * 32 : (n + 1) * 32]],
                *zip(state_of(tile), (peak, total)),
            )
            tile[0:32, :] = out.astype(BF16)
            tile[32:40, :] = state_rows(peaks, totals)


def state_of(ref):
    state = ref[32:40, :].astype(F32)
    return state[0:1] + state[1:2], state[2:3] + state[3:4]


def merge(outs, peaks, totals):
    peak = functools.reduce(jnp.maximum, peaks)
    factors = [jnp.exp2(p - peak) for p in peaks]
    out = sum(o * f for o, f in zip(outs, factors))
    return out, peak, sum(t * f for t, f in zip(totals, factors))


def merged(refs):
    outs = [ref[0:32, :].astype(F32) for ref in refs]
    return merge(outs, *zip(*map(state_of, refs)))


def tiles_of(ref):
    return [ref.at[n] for n in range(ref.shape[0])]


def couple_body(own_ref, came_ref, out_ref):
    for n in range(16):
        out, peak, total = merged([own_ref.at[n], came_ref.at[n]])
        out_ref[n, 0:32, :] = out.astype(BF16)
        out_ref[n, 32:40, :] = state_rows(peak, total)


def merge_body(in_ref, out_ref):
    out, peak, total = merged(tiles_of(in_ref))
    out, state = out.astype(BF16), state_rows(peak, total)
    for d in range(out_ref.shape[0]):
        out_ref[d, 0:32, :] = out
        out_ref[d, 32:40, :] = state


def finish_body(in_ref, out_ref):
    out, _, total = merged(tiles_of(in_ref))
    out_ref[...] = (out / total).astype(BF16)


def pair_body(own_ref, came_ref, out_ref):
    first = lax.axis_index("c") == 0
    own, came = own_ref[...].astype(F32), came_ref[...].astype(F32)
    tiles = (jnp.where(first, own, came).astype(BF16), jnp.where(first, came, own).astype(BF16))
    for d in range(out_ref.shape[0]):
        for n, tile in enumerate(tiles):
            out_ref[d, n * 32 : (n + 1) * 32, :] = tile


def place_body(in_ref, out_hbm, out_ref, sems):
    copies = []
    row = rows_of((128, 128))
    eye = where_one((row % 16) * 8 + row // 16 == lanes((128, 128)))
    for g in range(KVH):
        half, y = divmod(g, 4)
        block = in_ref[y * 4 : (y + 1) * 4, half * 32 : (half + 1) * 32, :].reshape(128, 128)
        block = dot(eye, block, NT).astype(BF16)
        for i in range(8):
            at = (g * 8 + i) * HD
            out_ref[:, at : at + HD] = block[i * ROWS : (i + 1) * ROWS]
        if g % 2:
            part = slice((g - 1) * 8 * HD, (g + 1) * 8 * HD)
            copies.append(
                pltpu.make_async_copy(out_ref.at[:, part], out_hbm.at[:, part], sems.at[g // 2])
            )
            copies[-1].start()
    for copy in copies:
        copy.wait()


def per_device(
    queries,
    span_keys,
    span_values,
    positions,
    span_segments,
    cache_keys,
    cache_values,
    cache_segments,
):
    shape = jax.ShapeDtypeStruct
    small = (
        queries,
        span_keys.T,
        span_values.T,
        positions,
        span_segments.reshape(1, ROWS),
        cache_segments.reshape(4, 128),
    )
    tiles, positions, span_segments, cache_segments = call(
        pack_body,
        "pack",
        (shape((6 * 128, 128), BF16), *(shape(a.shape, a.dtype) for a in small[3:])),
        *(pltpu.with_memory_space_constraint(a, pltpu.HBM) for a in small),
        specs=[HBM] * 6,
        scratch=[pltpu.VMEM(a.shape, a.dtype) for a in small[:3]] + [pltpu.SemaphoreType.DMA((6,))],
    )
    tiles = exchange(tiles.reshape(-1, 2, 128), CHIPS).reshape(-1, 128)
    came = swap(tiles)
    bias, tables, turned_values = call(
        ready_body,
        "ready",
        (
            shape((512 + ROWS, 128), F32),
            shape((2, ROWS, 128), F32),
            shape((KVH, HD, 512), BF16),
        ),
        positions,
        span_segments,
        cache_segments,
        pltpu.with_memory_space_constraint(cache_values, pltpu.HBM),
        specs=[VMEM] * 3 + [HBM],
        scratch=[pltpu.VMEM((512, KVH * HD), BF16), pltpu.SemaphoreType.DMA],
    )
    message = shape((16, 40, 128), BF16)
    parts, q, kv = call(
        first_body,
        "first",
        (message, shape((H * ROWS, HD), BF16), shape((2, 128, 128), F32)),
        tiles,
        came,
        tables,
        cache_keys,
        turned_values,
        bias,
        scratch=[pltpu.VMEM((2, 6 * 128 + 16, 128), F32)],
    )
    other = swap(parts)
    parts = call(
        second_body, "second", message, q, cache_keys, turned_values, bias, kv, tables
    )
    parts = call(couple_body, "couple", message, parts, other)
    parts = exchange(parts, PLANE)
    parts = call(merge_body, "merge", shape((8, 40, 128), BF16), parts)
    parts = exchange(parts, ("z",))
    tile = call(finish_body, "finish", shape((32, 128), BF16), parts)
    whole = call(pair_body, "pair", shape((16, 64, 128), BF16), tile, swap(tile))
    whole = exchange(whole, PLANE)
    return call(
        place_body,
        "place",
        shape((ROWS, H * HD), BF16),
        whole,
        scratch=[pltpu.VMEM((ROWS, H * HD), BF16), pltpu.SemaphoreType.DMA((4,))],
        out_specs=HBM,
    )


def solution(mesh):
    split = Mesh(mesh.devices.reshape(4, 8, 4, 2), ALL)
    return jax.shard_map(
        per_device,
        mesh=split,
        in_specs=(
            P(None, ALL),
            P(None, ALL),
            P(None, ALL),
            P(),
            P(),
            P(ALL, None),
            P(ALL, None),
            P(ALL),
        ),
        out_specs=P(),
        check_vma=False,
    )
```
